16 devices in a mesh: col: 4 (over z, y), row: 4 (over x, core).
Axes of the slice: x: 2, y: 2, z: 2, core: 2. Of those that a mesh axis runs over, the one named last changes fastest.
Arguments:
- t_amp: float32 [256, 20736], P('row', 'col')
- d_denom: float32 [256, 20736], P('row', 'col')
- v_oovv: bfloat16 [256, 20736], P('row', 'col')
- v_vvvv: bfloat16 [20736, 20736], P('row', 'col')
- v_oooo: bfloat16 [256, 256], replicated
- w_ovov: bfloat16 [2304, 2304], P(None, 'col')
Outputs:
- output: float32 [2304, 2304], P('row', 'col')
All inputs are finite; a program needn't handle non-finite values.
Results may differ from the reference program's by a relative error of at most 0.001.
Values are sent between devices in bfloat16 or wider.
A program may use at most 1 GiB of HBM per device.

```python
import math
import jax
import jax.numpy as jnp
from jax import lax

O = 16
V = 144


def pair_layout(entry_mat):
    entry_four = entry_mat.reshape(O, O, V, V).transpose(0, 2, 1, 3)
    return entry_four.reshape(O * V, O * V)


def setup_inputs(seed: int = 0) -> dict:
    key_list = jax.random.split(jax.random.key(seed), 6)
    amp_scale = 1.5 / math.sqrt(O * V)
    ladder_scale = math.sqrt(O / V)
    hole_scale = math.sqrt(V / O) / 1.5
    t_amp = amp_scale * jax.random.normal(key_list[0], (O * O, V * V), jnp.float32)
    d_denom = -(1.0 + 2.0 * jax.random.uniform(key_list[1], (O * O, V * V), jnp.float32))
    v_oovv = jax.random.normal(key_list[2], (O * O, V * V), jnp.float32).astype(jnp.bfloat16)

    def vvvv_rows(row_block):
        sub_key = jax.random.fold_in(key_list[3], row_block)
        rows_f32 = ladder_scale * jax.random.normal(sub_key, (V, V * V), jnp.float32)
        return rows_f32.astype(jnp.bfloat16)

    v_vvvv = lax.map(vvvv_rows, jnp.arange(V)).reshape(V * V, V * V)
    v_oooo = (hole_scale * jax.random.normal(key_list[4], (O * O, O * O), jnp.float32)).astype(jnp.bfloat16)
    w_ovov = (jax.random.normal(key_list[5], (O * V, O * V), jnp.float32) / 1.5).astype(jnp.bfloat16)
    return {"t_amp": t_amp, "d_denom": d_denom, "v_oovv": v_oovv, "v_vvvv": v_vvvv, "v_oooo": v_oooo, "w_ovov": w_ovov}


def reference(t_amp, d_denom, v_oovv, v_vvvv, v_oooo, w_ovov):
    t_bf = t_amp.astype(jnp.bfloat16)
    r_ladder = jnp.dot(t_bf, v_vvvv, preferred_element_type=jnp.float32)
    x_inter = jnp.dot(v_oovv, t_bf.T, preferred_element_type=jnp.float32)
    w_hole = (v_oooo.astype(jnp.float32) + 0.5 * x_inter).astype(jnp.bfloat16)
    r_hole = jnp.dot(w_hole.T, t_bf, preferred_element_type=jnp.float32)
    entry_sum = v_oovv.astype(jnp.float32) + r_ladder + r_hole
    t_mixed = pair_layout(t_bf)
    r_mixed = jnp.dot(t_mixed, w_ovov, preferred_element_type=jnp.float32)
    return (pair_layout(entry_sum) + r_mixed + r_mixed.T) / pair_layout(d_denom)
```

```python
import functools

import jax
import jax.numpy as jnp
from jax import lax
from jax.experimental import pallas as pl
from jax.experimental.pallas import tpu as pltpu
from jax.sharding import PartitionSpec as P

MESH = pl.DeviceIdType.MESH
F32 = jnp.float32
BF16 = jnp.bfloat16

O = 16
V = 144
RB = 64
CB = 5184
AB = 36
PB = 576
CW = 512
NCH = CB // CW
TW = CB - NCH * CW


def split_cols(load, planes, m):
    for q in range(8 if m < 4 else 4):
        piece = load(m, q)
        base = RB * (8 * m + q)
        planes[0, base : base + RB, :] = piece[:, 0:128]
        planes[1, base : base + RB, 0:16] = piece[:, 128:144]


def take_j(planes, j, base, rows):
    wide = planes[0, pl.ds(base + j, rows, stride=16), :]
    rest = planes[1, pl.ds(base + j, rows, stride=16), :]
    return [wide, rest[:, 0:16]]


def kernel(
    t_hbm, d_hbm, vo_hbm, vv_hbm, oo_ref, w_hbm, out_ref,
    t32, d32, vo, wv, trow, tcol, tlad, planes, tm, r3, pp, pt, pr,
    dsnd, drcv, lsnd, lrcv, planes2, xq, xqr, wt, vbuf, vtail,
    acc, d2r, xsb, xrb, acct, d2t, xst, xrt, r1,
    in_sem, v_sem, row_s, row_r, col_s, col_r, lad_s, lad_r, q_s, q_r,
    d_s, d_r, l_s, l_r, p_s, p_r, dd_s, dd_r, xx_s, xx_r,
):
    r = lax.axis_index("row")
    c = lax.axis_index("col")
    x, k = r // 2, r % 2
    z, y = c // 2, c % 2
    r_k, r_x = 2 * x + 1 - k, 2 * (1 - x) + k
    r_d = 2 * (1 - x) + 1 - k
    c_y, c_z = 2 * z + 1 - y, 2 * (1 - z) + y
    c_d = 2 * (1 - z) + 1 - y
    col_peers = (c_y, c_z, c_d)

    def send(src, dst, ss, rs, row, col):
        return pltpu.make_async_remote_copy(
            src_ref=src, dst_ref=dst, send_sem=ss, recv_sem=rs,
            device_id={"row": row, "col": col}, device_id_type=MESH,
        )

    def load_v(n, slot):
        at = pl.multiple_of(n * CW, CW)
        return pltpu.make_async_copy(vv_hbm.at[:, pl.ds(at, CW)], vbuf.at[slot], v_sem.at[slot])

    load_t = pltpu.make_async_copy(t_hbm, t32, in_sem.at[0])
    load_d = pltpu.make_async_copy(d_hbm, d32, in_sem.at[1])
    load_vo = pltpu.make_async_copy(vo_hbm, vo, in_sem.at[2])
    load_w = pltpu.make_async_copy(w_hbm, wv, in_sem.at[3])
    load_tail = pltpu.make_async_copy(vv_hbm.at[:, pl.ds(NCH * CW, TW)], vtail, in_sem.at[4])
    load_t.start()
    load_w.start()
    load_d.start()
    load_vo.start()
    load_tail.start()
    load_v(0, 0).start()
    load_v(1, 1).start()

    barrier = pltpu.get_barrier_semaphore()
    for rr in range(4):
        for cc in range(4):
            pl.semaphore_signal(barrier, inc=1, device_id={"row": rr, "col": cc}, device_id_type=MESH)

    load_t.wait()
    for m in range(9):
        piece = t32[:, PB * m : PB * m + PB].astype(BF16)
        trow[c, :, PB * m : PB * m + PB] = piece
        tcol[r, :, PB * m : PB * m + PB] = piece
    pl.semaphore_wait(barrier, 16)

    half = RB // 2
    row_copy = (
        send(trow.at[c], trow.at[c], row_s.at[0], row_r.at[0], r, c_y),
        send(trow.at[c], trow.at[c], row_s.at[1], row_r.at[1], r, c_z),
        send(trow.at[c_z, 0:half], trow.at[c_z, 0:half], row_s.at[2], row_r.at[2], r, c_y),
        send(trow.at[c_y, half:RB], trow.at[c_y, half:RB], row_s.at[3], row_r.at[3], r, c_z),
    )
    row_land = (
        send(trow.at[c_y], trow.at[c_y], row_s.at[0], row_r.at[0], r, c_y),
        send(trow.at[c_z], trow.at[c_z], row_s.at[1], row_r.at[1], r, c_z),
        send(trow.at[c_d, 0:half], trow.at[c_d, 0:half], row_s.at[2], row_r.at[2], r, c_y),
        send(trow.at[c_d, half:RB], trow.at[c_d, half:RB], row_s.at[3], row_r.at[3], r, c_z),
    )
    col_copy = (
        send(tcol.at[r], tcol.at[r], col_s.at[0], col_r.at[0], r_x, c),
        send(tcol.at[r], tcol.at[r], col_s.at[1], col_r.at[1], r_k, c),
        send(tcol.at[r_x], tcol.at[r_x], col_s.at[2], col_r.at[2], r_k, c),
    )
    col_land = (
        send(tcol.at[r_x], tcol.at[r_x], col_s.at[0], col_r.at[0], r_x, c),
        send(tcol.at[r_k], tcol.at[r_k], col_s.at[1], col_r.at[1], r_k, c),
        send(tcol.at[r_d], tcol.at[r_d], col_s.at[2], col_r.at[2], r_k, c),
    )
    row_copy[0].start()
    row_copy[1].start()
    col_copy[0].start()
    col_copy[1].start()

    def lad_copy(slot):
        return send(trow.at[slot], tlad.at[r], lad_s.at[slot], lad_r.at[r], slot, c)

    def dispatch(slot):
        @pl.when(slot != r)
        def _():
            lad_copy(slot).start()

        @pl.when(slot == r)
        def _():
            tlad[r] = trow[slot]

    dispatch(c)

    def bf16_piece(slot):
        def load(m, q):
            width = 1152 if m < 4 else 576
            stripe = trow[slot, :, 1152 * m : 1152 * m + width].astype(F32)
            return stripe[:, V * q : V * q + V]

        return load

    load_w.wait()

    def mixed(slot):
        load = bf16_piece(slot)
        for m in range(5):
            split_cols(load, planes, m)
        for h in range(2):
            parts = []
            for j in range(8):
                parts += take_j(planes, 8 * h + j, 0, 4 * AB)
            tm[:, 1152 * h : 1152 * h + 1152] = jnp.concatenate(parts, axis=1).astype(BF16)
        at = pl.multiple_of(slot * V, 8)
        r3[pl.ds(at, V), :] = jnp.dot(tm[...], wv[...], preferred_element_type=F32)

    mixed(c)

    load_d.wait()
    for m in range(5):
        split_cols(lambda m, q: d32[:, 1152 * m + V * q : 1152 * m + V * q + V], planes, m)
    for cc in range(4):
        parts = []
        for j in range(4):
            parts += take_j(planes, 4 * cc + j, 0, 4 * AB)
        dsnd[cc] = jnp.concatenate(parts, axis=1)
    own_rows = pl.ds(pl.multiple_of(c * V, 8), V)
    drcv[own_rows, :] = dsnd[c]

    row_land[1].wait_recv()
    row_copy[2].start()
    dispatch(c_z)
    row_land[0].wait_recv()
    row_copy[3].start()
    dispatch(c_y)
    mixed(c_z)
    mixed(c_y)

    col_land[0].wait_recv()
    col_copy[2].start()

    row_land[2].wait_recv()
    row_land[3].wait_recv()
    dispatch(c_d)
    d_copy = [
        send(dsnd.at[peer], drcv.at[own_rows], d_s.at[q], d_r.at[q], r, peer) for q, peer in enumerate(col_peers)
    ]
    for copy in d_copy:
        copy.start()
    mixed(c_d)

    for b in range(5):
        n = 128 if b < 4 else 64
        planes2[b, :, 0:n] = r3[:, 128 * b : 128 * b + n]
        for i in range(4):
            pp[V * i : V * i + V, 128 * b : 128 * b + n] = planes2[b, pl.ds(i, V, stride=4), :][:, 0:n]
    pt[...] = pp[...].T

    load_vo.wait()
    col_land[1].wait_recv()
    col_land[2].wait_recv()
    xq[...] = lax.dot_general(
        vo[...], tcol[...].reshape(4 * RB, CB), (((1,), (1,)), ((), ())), preferred_element_type=F32
    )
    xqr[c] = xq[...]
    q_copy = [send(xq, xqr.at[c], q_s.at[q], q_r.at[q], r, peer) for q, peer in enumerate(col_peers)]
    for copy in q_copy:
        copy.start()

    p_copy = send(pt, pr, p_s.at[0], p_r.at[0], c, r)

    @pl.when(r != c)
    def _():
        p_copy.start()

    @pl.when(r == c)
    def _():
        pr[...] = pt[...]

    for q, peer in enumerate(col_peers):
        send(xq, xqr.at[peer], q_s.at[q], q_r.at[q], r, peer).wait_recv()
    x_sum = (xqr[0] + xqr[1]) + (xqr[2] + xqr[3])
    w_hole = oo_ref[...].astype(F32) + 0.5 * x_sum
    wt[...] = w_hole.T.astype(BF16)

    for rr in range(4):

        @pl.when(r != rr)
        def _():
            send(trow.at[0], tlad.at[rr], lad_s.at[rr], lad_r.at[rr], rr, c).wait_recv()

    def d2_copy(n):
        return send(acc.at[n, 1 - k], d2r.at[n], dd_s.at[n], dd_r.at[n], r_k, c)

    def xx_copy(n):
        return send(xsb.at[n], xrb.at[n], xx_s.at[n], xx_r.at[n], r_x, c)

    d2_tail = send(acct.at[1 - k], d2t, dd_s.at[NCH], dd_r.at[NCH], r_k, c)
    xx_tail = send(xst, xrt, xx_s.at[NCH], xx_r.at[NCH], r_x, c)

    load_tail.wait()
    part = jnp.dot(tlad[...].reshape(4 * RB, CB), vtail[...], preferred_element_type=F32)
    part = part + jnp.dot(wt[...], trow[c, :, NCH * CW : CB], preferred_element_type=F32)
    for rr in range(4):
        acct[rr % 2, rr // 2] = part[RB * rr : RB * rr + RB]
    d2_tail.start()

    def second(n):
        d2_copy(n).wait_recv()
        xsb[n] = acc[n, k, 1 - x] + d2r[n, 1 - x]
        at = pl.multiple_of(n * CW, CW)
        r1[:, pl.ds(at, CW)] = acc[n, k, x] + d2r[n, x]
        xx_copy(n).start()

    def ladder_step(n, carry):
        slot = n % 2
        load_v(n, slot).wait()
        at = pl.multiple_of(n * CW, CW)
        for h in range(2):
            part = jnp.dot(
                tlad[...].reshape(4 * RB, CB), vbuf[slot, :, 256 * h : 256 * h + 256], preferred_element_type=F32
            )
            part = part + jnp.dot(
                wt[...], trow[c, :, pl.ds(pl.multiple_of(at + 256 * h, 256), 256)], preferred_element_type=F32
            )
            for rr in range(4):
                acc[n, rr % 2, rr // 2, :, 256 * h : 256 * h + 256] = part[RB * rr : RB * rr + RB]
        d2_copy(n).start()

        @pl.when(n + 2 < NCH)
        def _():
            load_v(n + 2, slot).start()

        @pl.when(n == 0)
        def _():
            d2_tail.wait_recv()
            xst[...] = acct[k, 1 - x] + d2t[1 - x]
            r1[:, NCH * CW : CB] = acct[k, x] + d2t[x]
            xx_tail.start()

        @pl.when(n > 0)
        def _():
            second(n - 1)

        return carry

    lax.fori_loop(0, NCH, ladder_step, 0)
    second(NCH - 1)

    l_copy = []
    xx_tail.wait_recv()
    r1[:, NCH * CW : CB] += xrt[...] + vo[:, NCH * CW : CB].astype(F32)
    done = 0
    for m in range(5):
        width = 1152 if m < 4 else 576
        while done < NCH and CW * done < 1152 * m + width:
            xx_copy(done).wait_recv()
            at = CW * done
            r1[:, at : at + CW] += xrb[done] + vo[:, at : at + CW].astype(F32)
            done += 1
        split_cols(lambda m, q: r1[:, 1152 * m + V * q : 1152 * m + V * q + V], planes, m)
        rows = width // V * 4
        first = 32 * m
        for cc in range(4):
            parts = []
            for j in range(4):
                parts += take_j(planes, 4 * cc + j, RB * 8 * m, rows)
            lsnd[cc, first : first + rows, :] = jnp.concatenate(parts, axis=1)
        there = pl.ds(pl.multiple_of(c * V + first, 8), rows)
        lrcv[there, :] = lsnd[c, first : first + rows, :]
        for q, peer in enumerate(col_peers):
            copy = send(
                lsnd.at[peer, first : first + rows], lrcv.at[there], l_s.at[m, q], l_r.at[m, q], r, peer
            )
            copy.start()
            l_copy.append(copy)

    @pl.when(r != c)
    def _():
        p_copy.wait_recv()

    pp[...] = pp[...] + pr[...]
    for q, peer in enumerate(col_peers):
        at = pl.ds(pl.multiple_of(peer * V, 8), V)
        send(dsnd.at[peer], drcv.at[at], d_s.at[q], d_r.at[q], r, peer).wait_recv()
    for m in range(5):
        rows = 32 if m < 4 else 16
        for q, peer in enumerate(col_peers):
            at = pl.ds(pl.multiple_of(peer * V + 32 * m, 8), rows)
            send(
                lsnd.at[peer, 32 * m : 32 * m + rows], lrcv.at[at], l_s.at[m, q], l_r.at[m, q], r, peer
            ).wait_recv()
    for b in range(5):
        n = 128 if b < 4 else 64
        cols = slice(128 * b, 128 * b + n)
        planes[0, 0:PB, 0:n] = lrcv[:, cols]
        planes2[b, :, 0:n] = drcv[:, cols]
        for i in range(4):
            rows = slice(V * i, V * i + V)
            top = planes[0, pl.ds(i, V, stride=4), :][:, 0:n] + pp[rows, cols]
            out_ref[rows, cols] = top / planes2[b, pl.ds(i, V, stride=4), :][:, 0:n]

    for copy in (*row_copy, *col_copy, *q_copy, *d_copy, *l_copy, d2_tail, xx_tail):
        copy.wait_send()
    for slot in range(4):

        @pl.when(slot != r)
        def _():
            lad_copy(slot).wait_send()

    @pl.when(r != c)
    def _():
        p_copy.wait_send()

    def drain(n, carry):
        d2_copy(n).wait_send()
        xx_copy(n).wait_send()
        return carry

    lax.fori_loop(0, NCH, drain, 0)


def solution(mesh):
    vm = pltpu.VMEM
    dma = pltpu.SemaphoreType.DMA
    scratch = [
        vm((RB, CB), F32), vm((RB, CB), F32), vm((RB, CB), BF16), vm((O * V, PB), BF16),
        vm((4, RB, CB), BF16), vm((4, RB, CB), BF16), vm((4, RB, CB), BF16),
        vm((2, AB * RB, 128), F32), vm((V, O * V), BF16),
        vm((PB, PB), F32), vm((PB, PB), F32), vm((PB, PB), F32), vm((PB, PB), F32),
        vm((4, V, PB), F32), vm((PB, PB), F32), vm((4, V, PB), F32), vm((PB, PB), F32),
        vm((5, PB, 128), F32),
        vm((RB, O * O), F32), vm((4, RB, O * O), F32), vm((O * O, RB), BF16),
        vm((2, CB, CW), BF16), vm((CB, TW), BF16),
        vm((NCH, 2, 2, RB, CW), F32), vm((NCH, 2, RB, CW), F32), vm((NCH, RB, CW), F32), vm((NCH, RB, CW), F32),
        vm((2, 2, RB, TW), F32), vm((2, RB, TW), F32), vm((RB, TW), F32), vm((RB, TW), F32),
        vm((RB, CB), F32),
        dma((5,)), dma((2,)), dma((4,)), dma((4,)), dma((3,)), dma((3,)), dma((4,)), dma((4,)), dma((3,)), dma((3,)),
        dma((3,)), dma((3,)), dma((5, 3)), dma((5, 3)), dma((1,)), dma((1,)),
        dma((NCH + 1,)), dma((NCH + 1,)), dma((NCH + 1,)), dma((NCH + 1,)),
    ]
    hbm = pl.BlockSpec(memory_space=pl.ANY)
    vmem = pl.BlockSpec(memory_space=pltpu.VMEM)
    call = pl.pallas_call(
        kernel,
        out_shape=jax.ShapeDtypeStruct((PB, PB), F32),
        in_specs=[hbm, hbm, hbm, hbm, vmem, hbm],
        out_specs=vmem,
        scratch_shapes=scratch,
        compiler_params=pltpu.CompilerParams(
            collective_id=0, has_side_effects=True, vmem_limit_bytes=67_000_000
        ),
        name="sweep",
    )
    return jax.shard_map(
        call,
        mesh=mesh,
        in_specs=(P("row", "col"), P("row", "col"), P("row", "col"), P("row", "col"), P("row", None), P(None, "col")),
        out_specs=P("row", "col"),
        check_vma=False,
    )
```

```python
import functools

import jax
import jax.numpy as jnp
from jax import lax
from jax.experimental import pallas as pl
from jax.experimental.pallas import tpu as pltpu
from jax.sharding import PartitionSpec as P

MESH = pl.DeviceIdType.MESH
F32 = jnp.float32
BF16 = jnp.bfloat16

O = 16
V = 144
RB = 64
CB = 5184
AB = 36
PB = 576
CW = 512
NCH = CB // CW
TW = CB - NCH * CW


def stripe(load, m, q):
    first = 1152 * m + V * q
    low = first // 128 * 128
    high = min(-(-(first + V) // 128) * 128, CB)
    return load(low, high)[:, first - low : first - low + V]


def split_cols(load, planes, m):
    for q in range(8 if m < 4 else 4):
        piece = stripe(load, m, q)
        base = RB * (8 * m + q)
        planes[0, base : base + RB, :] = piece[:, 0:128]
        planes[1, base : base + RB, 0:16] = piece[:, 128:144]


def take_j(planes, j, base, rows):
    wide = planes[0, pl.ds(base + j, rows, stride=16), :]
    rest = planes[1, pl.ds(base + j, rows, stride=16), :]
    return [wide, rest[:, 0:16]]


def kernel(
    t_hbm, d_hbm, vo_hbm, vv_hbm, oo_hbm, w_hbm, out_ref,
    t32, d32, vo, wv, trow, tcol, tlad, planes, tm, r3, pp, pt, pr,
    dsnd, drcv, lsnd, lrcv, planes2, xq, xqr, wt, oo, wblk, wf, vbuf, vtail,
    acc, d2r, xsb, xrb, acct, d2t, xst, xrt, r1,
    in_sem, v_sem, row_s, row_r, col_s, col_r, lad_s, lad_r, q_s, q_r,
    d_s, d_r, l_s, l_r, p_s, p_r, dd_s, dd_r, xx_s, xx_r, w_s, w_r, f_s,
):
    r = lax.axis_index("row")
    c = lax.axis_index("col")
    x, k = r // 2, r % 2
    z, y = c // 2, c % 2
    r_k, r_x = 2 * x + 1 - k, 2 * (1 - x) + k
    r_d = 2 * (1 - x) + 1 - k
    c_y, c_z = 2 * z + 1 - y, 2 * (1 - z) + y
    c_d = 2 * (1 - z) + 1 - y
    col_peers = (c_y, c_z, c_d)

    def send(src, dst, ss, rs, row, col):
        return pltpu.make_async_remote_copy(
            src_ref=src, dst_ref=dst, send_sem=ss, recv_sem=rs,
            device_id={"row": row, "col": col}, device_id_type=MESH,
        )

    def load_v(n, slot):
        at = pl.multiple_of(n * CW, CW)
        return pltpu.make_async_copy(vv_hbm.at[:, pl.ds(at, CW)], vbuf.at[slot], v_sem.at[slot])

    load_t = pltpu.make_async_copy(t_hbm, t32, in_sem.at[0])
    load_d = pltpu.make_async_copy(d_hbm, d32, in_sem.at[1])
    load_vo = pltpu.make_async_copy(vo_hbm, vo, in_sem.at[2])
    load_w = pltpu.make_async_copy(w_hbm, wv, in_sem.at[3])
    load_tail = pltpu.make_async_copy(vv_hbm.at[:, pl.ds(NCH * CW, TW)], vtail, in_sem.at[4])
    load_oo = pltpu.make_async_copy(oo_hbm.at[pl.ds(pl.multiple_of(r * RB, RB), RB)], oo, in_sem.at[5])
    load_t.start()
    load_w.start()
    load_d.start()
    load_vo.start()
    load_tail.start()
    load_oo.start()
    load_v(0, 0).start()
    load_v(1, 1).start()

    barrier = pltpu.get_barrier_semaphore()
    for rr in range(4):
        for cc in range(4):
            pl.semaphore_signal(barrier, inc=1, device_id={"row": rr, "col": cc}, device_id_type=MESH)

    load_t.wait()
    for m in range(9):
        piece = t32[:, PB * m : PB * m + PB].astype(BF16)
        trow[c, :, PB * m : PB * m + PB] = piece
        tcol[r, :, PB * m : PB * m + PB] = piece
    pl.semaphore_wait(barrier, 16)

    half = RB // 2
    row_copy = (
        send(trow.at[c], trow.at[c], row_s.at[0], row_r.at[0], r, c_y),
        send(trow.at[c], trow.at[c], row_s.at[1], row_r.at[1], r, c_z),
        send(trow.at[c_z, 0:half], trow.at[c_z, 0:half], row_s.at[2], row_r.at[2], r, c_y),
        send(trow.at[c_y, half:RB], trow.at[c_y, half:RB], row_s.at[3], row_r.at[3], r, c_z),
    )
    row_land = (
        send(trow.at[c_y], trow.at[c_y], row_s.at[0], row_r.at[0], r, c_y),
        send(trow.at[c_z], trow.at[c_z], row_s.at[1], row_r.at[1], r, c_z),
        send(trow.at[c_d, 0:half], trow.at[c_d, 0:half], row_s.at[2], row_r.at[2], r, c_y),
        send(trow.at[c_d, half:RB], trow.at[c_d, half:RB], row_s.at[3], row_r.at[3], r, c_z),
    )
    col_copy = (
        send(tcol.at[r], tcol.at[r], col_s.at[0], col_r.at[0], r_x, c),
        send(tcol.at[r], tcol.at[r], col_s.at[1], col_r.at[1], r_k, c),
        send(tcol.at[r_x], tcol.at[r_x], col_s.at[2], col_r.at[2], r_k, c),
    )
    col_land = (
        send(tcol.at[r_x], tcol.at[r_x], col_s.at[0], col_r.at[0], r_x, c),
        send(tcol.at[r_k], tcol.at[r_k], col_s.at[1], col_r.at[1], r_k, c),
        send(tcol.at[r_d], tcol.at[r_d], col_s.at[2], col_r.at[2], r_k, c),
    )
    row_copy[0].start()
    row_copy[1].start()

    @pl.when(x == z)
    def _():
        col_copy[0].start()

    col_copy[1].start()

    def lad_copy(slot):
        return send(trow.at[slot], tlad.at[r], lad_s.at[slot], lad_r.at[r], slot, c)

    def dispatch(slot):
        @pl.when(slot != r)
        def _():
            lad_copy(slot).start()

        @pl.when(slot == r)
        def _():
            tlad[r] = trow[slot]

    dispatch(c)

    load_w.wait()

    def mixed(slot):
        for m in range(5):
            split_cols(lambda lo, hi: trow[slot, :, lo:hi].astype(F32), planes, m)
        for h in range(2):
            parts = []
            for j in range(8):
                parts += take_j(planes, 8 * h + j, 0, 4 * AB)
            tm[:, 1152 * h : 1152 * h + 1152] = jnp.concatenate(parts, axis=1).astype(BF16)
        at = pl.multiple_of(slot * V, 8)
        r3[pl.ds(at, V), :] = lax.dot_general(
            tm[...], wv[...], (((1,), (1,)), ((), ())), preferred_element_type=F32
        )

    mixed(c)

    load_d.wait()
    for m in range(5):
        split_cols(lambda lo, hi: d32[:, lo:hi], planes, m)
    for cc in range(4):
        parts = []
        for j in range(4):
            parts += take_j(planes, 4 * cc + j, 0, 4 * AB)
        dsnd[cc] = jnp.concatenate(parts, axis=1)
    own_rows = pl.ds(pl.multiple_of(c * V, 8), V)
    drcv[own_rows, :] = dsnd[c]

    row_land[1].wait_recv()
    row_copy[2].start()
    dispatch(c_z)
    row_land[0].wait_recv()
    row_copy[3].start()
    dispatch(c_y)
    mixed(c_z)
    mixed(c_y)

    @pl.when(x != z)
    def _():
        col_land[0].wait_recv()
        col_copy[2].start()

    row_land[2].wait_recv()
    row_land[3].wait_recv()
    dispatch(c_d)
    d_copy = [
        send(dsnd.at[peer], drcv.at[own_rows], d_s.at[q], d_r.at[q], r, peer) for q, peer in enumerate(col_peers)
    ]
    for copy in d_copy:
        copy.start()
    mixed(c_d)

    for b in range(5):
        n = 128 if b < 4 else 64
        planes2[b, :, 0:n] = r3[:, 128 * b : 128 * b + n]
        for i in range(4):
            pp[V * i : V * i + V, 128 * b : 128 * b + n] = planes2[b, pl.ds(i, V, stride=4), :][:, 0:n]
    pt[...] = pp[...].T

    p_copy = send(pt, pr, p_s.at[0], p_r.at[0], c, r)

    @pl.when(r != c)
    def _():
        p_copy.start()

    @pl.when(r == c)
    def _():
        pr[...] = pt[...]

    for rr in range(4):

        @pl.when(r != rr)
        def _():
            send(trow.at[0], tlad.at[rr], lad_s.at[rr], lad_r.at[rr], rr, c).wait_recv()

    fwd = (
        send(tlad.at[r_d], tcol.at[r_d], f_s.at[0], col_r.at[0], r_k, c),
        send(tlad.at[r_x], tcol.at[r_x], f_s.at[1], col_r.at[2], r_k, c),
    )

    @pl.when(r == c)
    def _():
        for copy in fwd:
            copy.start()
        tcol[r_d] = tlad[r_d]
        tcol[r_x] = tlad[r_x]

    q_copy = [send(xq, xqr.at[c], q_s.at[q], q_r.at[q], r, peer) for q, peer in enumerate(col_peers)]

    def hole_x():
        load_vo.wait()
        col_land[1].wait_recv()

        @pl.when(jnp.logical_and(x == z, r != c))
        def _():
            col_land[0].wait_recv()

        @pl.when(r != c)
        def _():
            col_land[2].wait_recv()

        xq[...] = lax.dot_general(
            vo[...], tcol[...].reshape(4 * RB, CB), (((1,), (1,)), ((), ())), preferred_element_type=F32
        )
        xqr[c] = xq[...]
        for copy in q_copy:
            copy.start()

    def w_copy(rr):
        return send(wt.at[RB * rr : RB * rr + RB], wblk.at[r], w_s.at[rr], w_r.at[r], rr, c)

    def hole_w():
        load_oo.wait()
        for q, peer in enumerate(col_peers):
            send(xq, xqr.at[peer], q_s.at[q], q_r.at[q], r, peer).wait_recv()
        x_sum = (xqr[0] + xqr[1]) + (xqr[2] + xqr[3])
        w_hole = oo[...].astype(F32) + 0.5 * x_sum
        wt[...] = w_hole.T.astype(BF16)
        wblk[r] = wt[pl.ds(pl.multiple_of(r * RB, RB), RB), :]
        for rr in range(4):

            @pl.when(r != rr)
            def _():
                w_copy(rr).start()

    def d2_copy(n):
        return send(acc.at[n, 1 - k], d2r.at[n], dd_s.at[n], dd_r.at[n], r_k, c)

    def xx_copy(n):
        return send(xsb.at[n], xrb.at[n], xx_s.at[n], xx_r.at[n], r_x, c)

    d2_tail = send(acct.at[1 - k], d2t, dd_s.at[NCH], dd_r.at[NCH], r_k, c)
    xx_tail = send(xst, xrt, xx_s.at[NCH], xx_r.at[NCH], r_x, c)

    load_tail.wait()
    part = jnp.dot(tlad[...].reshape(4 * RB, CB), vtail[...], preferred_element_type=F32)
    for rr in range(4):
        acct[rr % 2, rr // 2] = part[RB * rr : RB * rr + RB]
    d2_tail.start()

    def second(n):
        d2_copy(n).wait_recv()
        xsb[n] = acc[n, k, 1 - x] + d2r[n, 1 - x]
        at = pl.multiple_of(n * CW, CW)
        r1[:, pl.ds(at, CW)] = acc[n, k, x] + d2r[n, x]
        xx_copy(n).start()

    def ladder_step(n, carry):
        slot = n % 2
        load_v(n, slot).wait()
        for h in range(2):
            part = jnp.dot(
                tlad[...].reshape(4 * RB, CB), vbuf[slot, :, 256 * h : 256 * h + 256], preferred_element_type=F32
            )
            for rr in range(4):
                acc[n, rr % 2, rr // 2, :, 256 * h : 256 * h + 256] = part[RB * rr : RB * rr + RB]
        d2_copy(n).start()

        @pl.when(n + 2 < NCH)
        def _():
            load_v(n + 2, slot).start()

        @pl.when(n == 0)
        def _():
            d2_tail.wait_recv()
            xst[...] = acct[k, 1 - x] + d2t[1 - x]
            r1[:, NCH * CW : CB] = acct[k, x] + d2t[x]
            xx_tail.start()

        @pl.when(n > 0)
        def _():
            second(n - 1)

        @pl.when(n == 2)
        def _():
            hole_x()

        @pl.when(n == 5)
        def _():
            hole_w()

        return carry

    lax.fori_loop(0, NCH, ladder_step, 0)
    second(NCH - 1)

    l_copy = []
    for rr in range(4):

        @pl.when(r != rr)
        def _():
            send(wt.at[0:RB], wblk.at[rr], w_s.at[rr], w_r.at[rr], rr, c).wait_recv()

    wf[...] = jnp.concatenate([wblk[rr].astype(F32) for rr in range(4)], axis=1).astype(BF16)

    def close(lo, hi, landed):
        hole = jnp.dot(wf[...], tcol[:, :, lo:hi].reshape(4 * RB, hi - lo), preferred_element_type=F32)
        r1[:, lo:hi] = r1[:, lo:hi] + landed + hole + vo[:, lo:hi].astype(F32)

    xx_tail.wait_recv()
    close(NCH * CW, CB, xrt[...])
    done = 0
    for m in range(5):
        width = 1152 if m < 4 else 576
        while done < NCH and CW * done < 1152 * m + width:
            xx_copy(done).wait_recv()
            close(CW * done, CW * done + CW, xrb[done])
            done += 1
        split_cols(lambda lo, hi: r1[:, lo:hi], planes, m)
        rows = width // V * 4
        first = 32 * m
        for cc in range(4):
            parts = []
            for j in range(4):
                parts += take_j(planes, 4 * cc + j, RB * 8 * m, rows)
            lsnd[cc, first : first + rows, :] = jnp.concatenate(parts, axis=1)
        there = pl.ds(pl.multiple_of(c * V + first, 8), rows)
        lrcv[there, :] = lsnd[c, first : first + rows, :]
        for q, peer in enumerate(col_peers):
            copy = send(
                lsnd.at[peer, first : first + rows], lrcv.at[there], l_s.at[m, q], l_r.at[m, q], r, peer
            )
            copy.start()
            l_copy.append(copy)

    @pl.when(r != c)
    def _():
        p_copy.wait_recv()

    pp[...] = pp[...] + pr[...]
    for q, peer in enumerate(col_peers):
        at = pl.ds(pl.multiple_of(peer * V, 8), V)
        send(dsnd.at[peer], drcv.at[at], d_s.at[q], d_r.at[q], r, peer).wait_recv()
    for m in range(5):
        rows = 32 if m < 4 else 16
        for q, peer in enumerate(col_peers):
            at = pl.ds(pl.multiple_of(peer * V + 32 * m, 8), rows)
            send(
                lsnd.at[peer, 32 * m : 32 * m + rows], lrcv.at[at], l_s.at[m, q], l_r.at[m, q], r, peer
            ).wait_recv()
    for b in range(5):
        n = 128 if b < 4 else 64
        cols = slice(128 * b, 128 * b + n)
        planes[0, 0:PB, 0:n] = lrcv[:, cols]
        planes2[b, :, 0:n] = drcv[:, cols]
        for i in range(4):
            rows = slice(V * i, V * i + V)
            top = planes[0, pl.ds(i, V, stride=4), :][:, 0:n] + pp[rows, cols]
            out_ref[rows, cols] = top / planes2[b, pl.ds(i, V, stride=4), :][:, 0:n]

    for copy in (*row_copy, col_copy[1], *q_copy, *d_copy, *l_copy, d2_tail, xx_tail):
        copy.wait_send()

    @pl.when(x == z)
    def _():
        col_copy[0].wait_send()

    @pl.when(x != z)
    def _():
        col_copy[2].wait_send()

    @pl.when(r == c)
    def _():
        for copy in fwd:
            copy.wait_send()

    for slot in range(4):

        @pl.when(slot != r)
        def _():
            lad_copy(slot).wait_send()
            w_copy(slot).wait_send()

    @pl.when(r != c)
    def _():
        p_copy.wait_send()

    def drain(n, carry):
        d2_copy(n).wait_send()
        xx_copy(n).wait_send()
        return carry

    lax.fori_loop(0, NCH, drain, 0)


def solution(mesh):
    vm = pltpu.VMEM
    dma = pltpu.SemaphoreType.DMA
    scratch = [
        vm((RB, CB), F32), vm((RB, CB), F32), vm((RB, CB), BF16), vm((PB, O * V), BF16),
        vm((4, RB, CB), BF16), vm((4, RB, CB), BF16), vm((4, RB, CB), BF16),
        vm((2, AB * RB, 128), F32), vm((V, O * V), BF16),
        vm((PB, PB), F32), vm((PB, PB), F32), vm((PB, PB), F32), vm((PB, PB), F32),
        vm((4, V, PB), F32), vm((PB, PB), F32), vm((4, V, PB), F32), vm((PB, PB), F32),
        vm((5, PB, 128), F32),
        vm((RB, O * O), F32), vm((4, RB, O * O), F32), vm((O * O, RB), BF16), vm((RB, O * O), BF16), vm((4, RB, RB), BF16), vm((RB, O * O), BF16),
        vm((2, CB, CW), BF16), vm((CB, TW), BF16),
        vm((NCH, 2, 2, RB, CW), F32), vm((NCH, 2, RB, CW), F32), vm((NCH, RB, CW), F32), vm((NCH, RB, CW), F32),
        vm((2, 2, RB, TW), F32), vm((2, RB, TW), F32), vm((RB, TW), F32), vm((RB, TW), F32),
        vm((RB, CB), F32),
        dma((6,)), dma((2,)), dma((4,)), dma((4,)), dma((3,)), dma((3,)), dma((4,)), dma((4,)), dma((3,)), dma((3,)),
        dma((3,)), dma((3,)), dma((5, 3)), dma((5, 3)), dma((1,)), dma((1,)),
        dma((NCH + 1,)), dma((NCH + 1,)), dma((NCH + 1,)), dma((NCH + 1,)), dma((4,)), dma((4,)), dma((2,)),
    ]
    hbm = pl.BlockSpec(memory_space=pl.ANY)
    vmem = pl.BlockSpec(memory_space=pltpu.VMEM)
    call = pl.pallas_call(
        kernel,
        out_shape=jax.ShapeDtypeStruct((PB, PB), F32),
        in_specs=[hbm] * 6,
        out_specs=vmem,
        scratch_shapes=scratch,
        compiler_params=pltpu.CompilerParams(
            collective_id=0, has_side_effects=True, vmem_limit_bytes=67_000_000
        ),
        name="sweep",
    )
    def local_sweep(t_blk, d_blk, voovv_blk, vvvvv_blk, oooo, w_blk):
        return call(t_blk, d_blk, voovv_blk, vvvvv_blk, oooo, w_blk.T)

    return jax.shard_map(
        local_sweep,
        mesh=mesh,
        in_specs=(P("row", "col"), P("row", "col"), P("row", "col"), P("row", "col"), P(None, None), P(None, "col")),
        out_specs=P("row", "col"),
        check_vma=False,
    )
```

```python
import functools

import jax
import jax.numpy as jnp
from jax import lax
from jax.experimental import pallas as pl
from jax.experimental.pallas import tpu as pltpu
from jax.sharding import PartitionSpec as P

MESH = pl.DeviceIdType.MESH
F32 = jnp.float32
BF16 = jnp.bfloat16

O = 16
V = 144
RB = 64
CB = 5184
AB = 36
PB = 576
CW = 512
NCH = CB // CW
TW = CB - NCH * CW


def stripe(load, m, q):
    first = 1152 * m + V * q
    low = first // 128 * 128
    high = min(-(-(first + V) // 128) * 128, CB)
    return load(low, high)[:, first - low : first - low + V]


def split_cols(load, planes, m):
    for q in range(8 if m < 4 else 4):
        piece = stripe(load, m, q)
        base = RB * (8 * m + q)
        planes[0, base : base + RB, :] = piece[:, 0:128]
        planes[1, base : base + RB, 0:16] = piece[:, 128:144]


def take_j(planes, j, base, rows):
    wide = planes[0, pl.ds(base + j, rows, stride=16), :]
    rest = planes[1, pl.ds(base + j, rows, stride=16), :]
    return [wide, rest[:, 0:16]]


def kernel(
    t_hbm, d_hbm, vo_hbm, vv_hbm, oo_hbm, w_hbm, out_ref,
    t32, d32, vo, wv, trow, tcol, tlad, planes, tm, r3, pp, pt, pr,
    dsnd, drcv, lsnd, lrcv, planes2, prel, xq, xqr, wt, oo, wblk, wf, vbuf, vtail,
    acc, d2r, xsb, xrb, acct, d2t, xst, xrt, r1,
    in_sem, v_sem, row_s, row_r, col_s, col_r, lad_s, lad_r, q_s, q_r,
    d_s, d_r, l_s, l_r, p_s, p_r, fw_s, dd_s, dd_r, xx_s, xx_r, w_s, w_r, f_s,
):
    r = lax.axis_index("row")
    c = lax.axis_index("col")
    x, k = r // 2, r % 2
    z, y = c // 2, c % 2
    r_k, r_x = 2 * x + 1 - k, 2 * (1 - x) + k
    r_d = 2 * (1 - x) + 1 - k
    c_y, c_z = 2 * z + 1 - y, 2 * (1 - z) + y
    c_d = 2 * (1 - z) + 1 - y
    col_peers = (c_y, c_z, c_d)

    def send(src, dst, ss, rs, row, col):
        return pltpu.make_async_remote_copy(
            src_ref=src, dst_ref=dst, send_sem=ss, recv_sem=rs,
            device_id={"row": row, "col": col}, device_id_type=MESH,
        )

    def load_v(n, slot):
        at = pl.multiple_of(n * CW, CW)
        return pltpu.make_async_copy(vv_hbm.at[:, pl.ds(at, CW)], vbuf.at[slot], v_sem.at[slot])

    load_t = pltpu.make_async_copy(t_hbm, t32, in_sem.at[0])
    load_d = pltpu.make_async_copy(d_hbm, d32, in_sem.at[1])
    load_vo = pltpu.make_async_copy(vo_hbm, vo, in_sem.at[2])
    load_w = pltpu.make_async_copy(w_hbm, wv, in_sem.at[3])
    load_tail = pltpu.make_async_copy(vv_hbm.at[:, pl.ds(NCH * CW, TW)], vtail, in_sem.at[4])
    load_oo = pltpu.make_async_copy(oo_hbm.at[pl.ds(pl.multiple_of(r * RB, RB), RB)], oo, in_sem.at[5])
    load_t.start()
    load_w.start()
    load_d.start()
    load_vo.start()
    load_tail.start()
    load_oo.start()
    load_v(0, 0).start()
    load_v(1, 1).start()

    barrier = pltpu.get_barrier_semaphore()
    for rr in range(4):
        for cc in range(4):
            pl.semaphore_signal(barrier, inc=1, device_id={"row": rr, "col": cc}, device_id_type=MESH)

    load_t.wait()
    for m in range(9):
        piece = t32[:, PB * m : PB * m + PB].astype(BF16)
        trow[c, :, PB * m : PB * m + PB] = piece
        tcol[r, :, PB * m : PB * m + PB] = piece
    pl.semaphore_wait(barrier, 16)

    half = RB // 2
    halves = (slice(0, half), slice(half, RB))

    def row_copy(way, h):
        block, peer = ((c, c_y), (c, c_z), ((c_z, c_y), (c_y, c_z))[h])[way]
        piece = trow.at[block, halves[h]]
        return send(piece, piece, row_s.at[way, h], row_r.at[way, h], r, peer)

    def row_wait(way, h):
        piece = trow.at[(c_y, c_z, c_d)[way], halves[h]]
        send(piece, piece, row_s.at[way, h], row_r.at[way, h], r, c_y).wait_recv()

    def col_piece(h):
        piece = tcol.at[r, halves[h]]
        return send(piece, piece, col_s.at[h], col_r.at[h], r_x, c)

    col_pair = send(tcol.at[r], tcol.at[r], col_s.at[2], col_r.at[2], r_k, c)
    col_relay = send(tcol.at[r_x], tcol.at[r_x], col_s.at[3], col_r.at[3], r_k, c)

    def lad_copy(slot, h):
        return send(trow.at[slot, halves[h]], tlad.at[r, halves[h]], lad_s.at[slot, h], lad_r.at[r, h], slot, c)

    def dispatch(slot, h):
        @pl.when(slot != r)
        def _():
            lad_copy(slot, h).start()

        @pl.when(slot == r)
        def _():
            tlad[r, halves[h]] = trow[slot, halves[h]]

    @pl.when(x == z)
    def _():
        col_piece(0).start()

    for h in range(2):
        row_copy(0, h).start()
        row_copy(1, h).start()
        dispatch(c, h)
    col_pair.start()

    load_w.wait()

    def mixed(slot):
        for m in range(5):
            split_cols(lambda lo, hi: trow[slot, :, lo:hi].astype(F32), planes, m)
        for h in range(2):
            parts = []
            for j in range(8):
                parts += take_j(planes, 8 * h + j, 0, 4 * AB)
            tm[:, 1152 * h : 1152 * h + 1152] = jnp.concatenate(parts, axis=1).astype(BF16)
        at = pl.multiple_of(slot * V, 8)
        r3[pl.ds(at, V), :] = lax.dot_general(
            tm[...], wv[...], (((1,), (1,)), ((), ())), preferred_element_type=F32
        )

    mixed(c)

    row_wait(1, 0)
    row_copy(2, 0).start()
    dispatch(c_z, 0)
    row_wait(0, 0)
    dispatch(c_y, 0)

    load_d.wait()
    for m in range(5):
        split_cols(lambda lo, hi: d32[:, lo:hi], planes, m)
    for cc in range(4):
        parts = []
        for j in range(4):
            parts += take_j(planes, 4 * cc + j, 0, 4 * AB)
        dsnd[cc] = jnp.concatenate(parts, axis=1)
    own_rows = pl.ds(pl.multiple_of(c * V, 8), V)
    drcv[own_rows, :] = dsnd[c]

    row_wait(1, 1)
    dispatch(c_z, 1)
    row_wait(0, 1)
    row_copy(2, 1).start()
    dispatch(c_y, 1)
    mixed(c_z)
    row_wait(2, 0)
    row_wait(2, 1)

    @pl.when(x != z)
    def _():
        dispatch(c_d, 0)
        dispatch(c_d, 1)

    @pl.when(x == z)
    def _():
        col_piece(1).start()

    mixed(c_y)
    mixed(c_d)
    d_copy = [
        send(dsnd.at[peer], drcv.at[own_rows], d_s.at[q], d_r.at[q], r, peer) for q, peer in enumerate(col_peers)
    ]

    for b in range(5):
        n = 128 if b < 4 else 64
        planes2[b, :, 0:n] = r3[:, 128 * b : 128 * b + n]
        for i in range(4):
            pp[V * i : V * i + V, 128 * b : 128 * b + n] = planes2[b, pl.ds(i, V, stride=4), :][:, 0:n]
    pt[...] = pp[...].T

    top, low = slice(0, PB // 2), slice(PB // 2, PB)
    p_copy = send(pt, pr, p_s.at[0], p_r.at[0], c, r)
    p_out = (
        send(pt.at[top], prel.at[0], p_s.at[1], p_r.at[1], r_x, c),
        send(pt.at[low], prel.at[1], p_s.at[2], p_r.at[2], r, c_z),
    )
    p_on = (
        send(prel.at[0], pr.at[top], p_s.at[3], p_r.at[3], c, r_x),
        send(prel.at[1], pr.at[low], p_s.at[4], p_r.at[4], c_z, r),
    )

    @pl.when(jnp.logical_and(x == z, r != c))
    def _():
        p_copy.start()

    @pl.when(r == c)
    def _():
        pr[...] = pt[...]

    @pl.when(x != z)
    def _():
        p_out[1].start()
        p_out[0].start()

    def lad_wait(slot, h):
        send(trow.at[0, halves[h]], tlad.at[slot, halves[h]], lad_s.at[slot, h], lad_r.at[slot, h], r, c).wait_recv()

    def lad_forward(slot, h):
        piece = tlad.at[slot, halves[h]]
        return send(piece, piece, fw_s.at[slot, h], lad_r.at[slot, h], r, c_y)

    gives = jnp.logical_and(x != z, k == y)
    for h in range(2):
        lad_wait(r_k, h)
    for h in range(2):
        for slot in (r_x, r_d):
            lad_wait(slot, h)

            @pl.when(gives)
            def _():
                lad_forward(slot, h).start()

    fwd = (
        send(tlad.at[r_d], tcol.at[r_d], f_s.at[0], col_r.at[4], r_k, c),
        send(tlad.at[r_x], tcol.at[r_x], f_s.at[1], col_r.at[3], r_k, c),
    )

    @pl.when(r == c)
    def _():
        for copy in fwd:
            copy.start()
        tcol[r_d] = tlad[r_d]
        tcol[r_x] = tlad[r_x]

    q_copy = [send(xq, xqr.at[c], q_s.at[q], q_r.at[q], r, peer) for q, peer in enumerate(col_peers)]

    def hole_x():
        load_vo.wait()
        send(tcol.at[r_k], tcol.at[r_k], col_s.at[2], col_r.at[2], r_k, c).wait_recv()

        @pl.when(jnp.logical_and(x == z, r != c))
        def _():
            send(tcol.at[r_x], tcol.at[r_x], f_s.at[0], col_r.at[4], r_k, c).wait_recv()

        @pl.when(r != c)
        def _():
            send(tcol.at[r_d], tcol.at[r_d], col_s.at[3], col_r.at[3], r_k, c).wait_recv()

        xq[...] = lax.dot_general(
            vo[...], tcol[...].reshape(4 * RB, CB), (((1,), (1,)), ((), ())), preferred_element_type=F32
        )
        xqr[c] = xq[...]
        for copy in q_copy:
            copy.start()

    def w_copy(rr):
        return send(wt.at[RB * rr : RB * rr + RB], wblk.at[r], w_s.at[rr], w_r.at[r], rr, c)

    def hole_w():
        load_oo.wait()
        for q, peer in enumerate(col_peers):
            send(xq, xqr.at[peer], q_s.at[q], q_r.at[q], r, peer).wait_recv()
        x_sum = (xqr[0] + xqr[1]) + (xqr[2] + xqr[3])
        w_hole = oo[...].astype(F32) + 0.5 * x_sum
        wt[...] = w_hole.T.astype(BF16)
        wblk[r] = wt[pl.ds(pl.multiple_of(r * RB, RB), RB), :]
        for rr in range(4):

            @pl.when(r != rr)
            def _():
                w_copy(rr).start()

    def d2_copy(n):
        return send(acc.at[n, 1 - k], d2r.at[n], dd_s.at[n], dd_r.at[n], r_k, c)

    def xx_copy(n):
        return send(xsb.at[n], xrb.at[n], xx_s.at[n], xx_r.at[n], r_x, c)

    d2_tail = send(acct.at[1 - k], d2t, dd_s.at[NCH], dd_r.at[NCH], r_k, c)
    xx_tail = send(xst, xrt, xx_s.at[NCH], xx_r.at[NCH], r_x, c)

    load_tail.wait()
    part = jnp.dot(tlad[...].reshape(4 * RB, CB), vtail[...], preferred_element_type=F32)
    for rr in range(4):
        acct[rr % 2, rr // 2] = part[RB * rr : RB * rr + RB]
    d2_tail.start()

    def second(n):
        d2_copy(n).wait_recv()
        xsb[n] = acc[n, k, 1 - x] + d2r[n, 1 - x]
        at = pl.multiple_of(n * CW, CW)
        r1[:, pl.ds(at, CW)] = acc[n, k, x] + d2r[n, x]
        xx_copy(n).start()

    def ladder_step(n, carry):
        slot = n % 2
        load_v(n, slot).wait()
        for h in range(2):
            part = jnp.dot(
                tlad[...].reshape(4 * RB, CB), vbuf[slot, :, 256 * h : 256 * h + 256], preferred_element_type=F32
            )
            for rr in range(4):
                acc[n, rr % 2, rr // 2, :, 256 * h : 256 * h + 256] = part[RB * rr : RB * rr + RB]
        d2_copy(n).start()

        @pl.when(n + 2 < NCH)
        def _():
            load_v(n + 2, slot).start()

        @pl.when(n == 0)
        def _():
            d2_tail.wait_recv()
            xst[...] = acct[k, 1 - x] + d2t[1 - x]
            r1[:, NCH * CW : CB] = acct[k, x] + d2t[x]
            xx_tail.start()

        @pl.when(n > 0)
        def _():
            second(n - 1)

        @pl.when(n == 0)
        def _():
            for copy in d_copy:
                copy.start()

        @pl.when(jnp.logical_and(n == 2, x != z))
        def _():
            for h in range(2):
                piece = tcol.at[r_x, halves[h]]
                send(piece, piece, col_s.at[h], col_r.at[h], r_x, c).wait_recv()
            col_relay.start()

        @pl.when(n == 3)
        def _():
            hole_x()

        @pl.when(jnp.logical_and(n == 4, x == z))
        def _():
            for copy, on in zip(p_out, p_on):
                copy.wait_recv()
                on.start()

        @pl.when(n == 6)
        def _():
            hole_w()

        return carry

    lax.fori_loop(0, NCH, ladder_step, 0)
    second(NCH - 1)

    l_copy = []
    for rr in range(4):

        @pl.when(r != rr)
        def _():
            send(wt.at[0:RB], wblk.at[rr], w_s.at[rr], w_r.at[rr], rr, c).wait_recv()

    wf[...] = jnp.concatenate([wblk[rr].astype(F32) for rr in range(4)], axis=1).astype(BF16)

    def close(lo, hi, landed):
        hole = jnp.dot(wf[...], tcol[:, :, lo:hi].reshape(4 * RB, hi - lo), preferred_element_type=F32)
        r1[:, lo:hi] = r1[:, lo:hi] + landed + hole + vo[:, lo:hi].astype(F32)

    xx_tail.wait_recv()
    close(NCH * CW, CB, xrt[...])
    done = 0
    for m in range(5):
        width = 1152 if m < 4 else 576
        while done < NCH and CW * done < 1152 * m + width:
            xx_copy(done).wait_recv()
            close(CW * done, CW * done + CW, xrb[done])
            done += 1
        split_cols(lambda lo, hi: r1[:, lo:hi], planes, m)
        rows = width // V * 4
        first = 32 * m
        for cc in range(4):
            parts = []
            for j in range(4):
                parts += take_j(planes, 4 * cc + j, RB * 8 * m, rows)
            lsnd[cc, first : first + rows, :] = jnp.concatenate(parts, axis=1)
        there = pl.ds(pl.multiple_of(c * V + first, 8), rows)
        lrcv[there, :] = lsnd[c, first : first + rows, :]
        for q, peer in enumerate(col_peers):
            copy = send(
                lsnd.at[peer, first : first + rows], lrcv.at[there], l_s.at[m, q], l_r.at[m, q], r, peer
            )
            copy.start()
            l_copy.append(copy)

    @pl.when(jnp.logical_and(x == z, r != c))
    def _():
        p_copy.wait_recv()

    @pl.when(x != z)
    def _():
        for copy in p_on:
            copy.wait_recv()

    pp[...] = pp[...] + pr[...]
    for q, peer in enumerate(col_peers):
        at = pl.ds(pl.multiple_of(peer * V, 8), V)
        send(dsnd.at[peer], drcv.at[at], d_s.at[q], d_r.at[q], r, peer).wait_recv()
    for m in range(5):
        rows = 32 if m < 4 else 16
        for q, peer in enumerate(col_peers):
            at = pl.ds(pl.multiple_of(peer * V + 32 * m, 8), rows)
            send(
                lsnd.at[peer, 32 * m : 32 * m + rows], lrcv.at[at], l_s.at[m, q], l_r.at[m, q], r, peer
            ).wait_recv()
    for b in range(5):
        n = 128 if b < 4 else 64
        cols = slice(128 * b, 128 * b + n)
        planes[0, 0:PB, 0:n] = lrcv[:, cols]
        planes2[b, :, 0:n] = drcv[:, cols]
        for i in range(4):
            rows = slice(V * i, V * i + V)
            top = planes[0, pl.ds(i, V, stride=4), :][:, 0:n] + pp[rows, cols]
            out_ref[rows, cols] = top / planes2[b, pl.ds(i, V, stride=4), :][:, 0:n]

    for copy in (col_pair, *q_copy, *d_copy, *l_copy, d2_tail, xx_tail):
        copy.wait_send()
    for way in range(3):
        for h in range(2):
            row_copy(way, h).wait_send()

    @pl.when(x == z)
    def _():
        for h in range(2):
            col_piece(h).wait_send()
        for copy in p_on:
            copy.wait_send()

    @pl.when(jnp.logical_and(x == z, r != c))
    def _():
        p_copy.wait_send()

    @pl.when(x != z)
    def _():
        col_relay.wait_send()
        for copy in p_out:
            copy.wait_send()

    @pl.when(r == c)
    def _():
        for copy in fwd:
            copy.wait_send()

    @pl.when(gives)
    def _():
        for h in range(2):
            for slot in (r_x, r_d):
                lad_forward(slot, h).wait_send()

    for slot in range(4):

        @pl.when(slot != r)
        def _():
            w_copy(slot).wait_send()

        @pl.when(jnp.logical_and(slot != r, jnp.logical_or(slot != c_d, x != z)))
        def _():
            for h in range(2):
                lad_copy(slot, h).wait_send()

    def drain(n, carry):
        d2_copy(n).wait_send()
        xx_copy(n).wait_send()
        return carry

    lax.fori_loop(0, NCH, drain, 0)


def solution(mesh):
    vm = pltpu.VMEM
    dma = pltpu.SemaphoreType.DMA
    scratch = [
        vm((RB, CB), F32), vm((RB, CB), F32), vm((RB, CB), BF16), vm((PB, O * V), BF16),
        vm((4, RB, CB), BF16), vm((4, RB, CB), BF16), vm((4, RB, CB), BF16),
        vm((2, AB * RB, 128), F32), vm((V, O * V), BF16),
        vm((PB, PB), F32), vm((PB, PB), F32), vm((PB, PB), F32), vm((PB, PB), F32),
        vm((4, V, PB), F32), vm((PB, PB), F32), vm((4, V, PB), F32), vm((PB, PB), F32),
        vm((5, PB, 128), F32), vm((2, PB // 2, PB), F32),
        vm((RB, O * O), F32), vm((4, RB, O * O), F32), vm((O * O, RB), BF16), vm((RB, O * O), BF16), vm((4, RB, RB), BF16), vm((RB, O * O), BF16),
        vm((2, CB, CW), BF16), vm((CB, TW), BF16),
        vm((NCH, 2, 2, RB, CW), F32), vm((NCH, 2, RB, CW), F32), vm((NCH, RB, CW), F32), vm((NCH, RB, CW), F32),
        vm((2, 2, RB, TW), F32), vm((2, RB, TW), F32), vm((RB, TW), F32), vm((RB, TW), F32),
        vm((RB, CB), F32),
        dma((6,)), dma((2,)), dma((3, 2)), dma((3, 2)), dma((5,)), dma((5,)), dma((4, 2)), dma((4, 2)),
        dma((3,)), dma((3,)), dma((3,)), dma((3,)), dma((5, 3)), dma((5, 3)), dma((5,)), dma((5,)), dma((4, 2)),
        dma((NCH + 1,)), dma((NCH + 1,)), dma((NCH + 1,)), dma((NCH + 1,)), dma((4,)), dma((4,)), dma((2,)),
    ]
    hbm = pl.BlockSpec(memory_space=pl.ANY)
    vmem = pl.BlockSpec(memory_space=pltpu.VMEM)
    call = pl.pallas_call(
        kernel,
        out_shape=jax.ShapeDtypeStruct((PB, PB), F32),
        in_specs=[hbm] * 6,
        out_specs=vmem,
        scratch_shapes=scratch,
        compiler_params=pltpu.CompilerParams(
            collective_id=0, has_side_effects=True, vmem_limit_bytes=67_000_000
        ),
        name="sweep",
    )
    def local_sweep(t_blk, d_blk, voovv_blk, vvvvv_blk, oooo, w_blk):
        return call(t_blk, d_blk, voovv_blk, vvvvv_blk, oooo, w_blk.T)

    return jax.shard_map(
        local_sweep,
        mesh=mesh,
        in_specs=(P("row", "col"), P("row", "col"), P("row", "col"), P("row", "col"), P(None, None), P(None, "col")),
        out_specs=P("row", "col"),
        check_vma=False,
    )
```

```python
import functools

import jax
import jax.numpy as jnp
from jax import lax
from jax.experimental import pallas as pl
from jax.experimental.pallas import tpu as pltpu
from jax.sharding import PartitionSpec as P

MESH = pl.DeviceIdType.MESH
scope = jax.named_scope
F32 = jnp.float32
BF16 = jnp.bfloat16

O = 16
V = 144
RB = 64
CB = 5184
AB = 36
PB = 576
CW = 512
NCH = CB // CW
TW = CB - NCH * CW


def stripe(load, m, q):
    first = 1152 * m + V * q
    low = first // 128 * 128
    high = min(-(-(first + V) // 128) * 128, CB)
    return load(low, high)[:, first - low : first - low + V]


def split_cols(load, planes, m):
    for q in range(8 if m < 4 else 4):
        piece = stripe(load, m, q)
        base = RB * (8 * m + q)
        planes[0, base : base + RB, :] = piece[:, 0:128]
        planes[1, base : base + RB, 0:16] = piece[:, 128:144]


def take_j(planes, j, base, rows):
    wide = planes[0, pl.ds(base + j, rows, stride=16), :]
    rest = planes[1, pl.ds(base + j, rows, stride=16), :]
    return [wide, rest[:, 0:16]]


def kernel(
    t_hbm, d_hbm, vo_hbm, vv_hbm, oo_hbm, w_hbm, out_ref,
    t32, d32, vo, wv, trow, tcol, tlad, planes, tm, r3, pp, pt, pr,
    dsnd, drcv, lsnd, lrcv, planes2, prel, xq, xqr, wt, oo, wblk, wf, vbuf, vtail,
    acc, d2r, xsb, xrb, acct, d2t, xst, xrt, r1,
    in_sem, v_sem, row_s, row_r, col_s, col_r, lad_s, lad_r, q_s, q_r,
    d_s, d_r, l_s, l_r, p_s, p_r, fw_s, dd_s, dd_r, xx_s, xx_r, w_s, w_r, f_s,
):
    r = lax.axis_index("row")
    c = lax.axis_index("col")
    x, k = r // 2, r % 2
    z, y = c // 2, c % 2
    r_k, r_x = 2 * x + 1 - k, 2 * (1 - x) + k
    r_d = 2 * (1 - x) + 1 - k
    c_y, c_z = 2 * z + 1 - y, 2 * (1 - z) + y
    c_d = 2 * (1 - z) + 1 - y
    col_peers = (c_y, c_z, c_d)

    def send(src, dst, ss, rs, row, col):
        return pltpu.make_async_remote_copy(
            src_ref=src, dst_ref=dst, send_sem=ss, recv_sem=rs,
            device_id={"row": row, "col": col}, device_id_type=MESH,
        )

    def load_v(n, slot):
        at = pl.multiple_of(n * CW, CW)
        return pltpu.make_async_copy(vv_hbm.at[:, pl.ds(at, CW)], vbuf.at[slot], v_sem.at[slot])

    load_t = pltpu.make_async_copy(t_hbm, t32, in_sem.at[0])
    load_d = pltpu.make_async_copy(d_hbm, d32, in_sem.at[1])
    load_vo = pltpu.make_async_copy(vo_hbm, vo, in_sem.at[2])
    load_w = pltpu.make_async_copy(w_hbm, wv, in_sem.at[3])
    load_tail = pltpu.make_async_copy(vv_hbm.at[:, pl.ds(NCH * CW, TW)], vtail, in_sem.at[4])
    load_oo = pltpu.make_async_copy(oo_hbm.at[pl.ds(pl.multiple_of(r * RB, RB), RB)], oo, in_sem.at[5])
    load_t.start()
    load_w.start()
    load_d.start()
    load_vo.start()
    load_tail.start()
    load_oo.start()
    load_v(0, 0).start()
    load_v(1, 1).start()

    barrier = pltpu.get_barrier_semaphore()
    for rr in range(4):
        for cc in range(4):
            pl.semaphore_signal(barrier, inc=1, device_id={"row": rr, "col": cc}, device_id_type=MESH)

    with scope("wait_t"):
        load_t.wait()
    for m in range(9):
        piece = t32[:, PB * m : PB * m + PB].astype(BF16)
        trow[c, :, PB * m : PB * m + PB] = piece
        tcol[r, :, PB * m : PB * m + PB] = piece
    with scope("barrier"):
        pl.semaphore_wait(barrier, 16)

    half = RB // 2
    halves = (slice(0, half), slice(half, RB))

    def row_copy(way, h):
        block, peer = ((c, c_y), (c, c_z), ((c_z, c_y), (c_y, c_z))[h])[way]
        piece = trow.at[block, halves[h]]
        return send(piece, piece, row_s.at[way, h], row_r.at[way, h], r, peer)

    def row_wait(way, h):
        piece = trow.at[(c_y, c_z, c_d)[way], halves[h]]
        send(piece, piece, row_s.at[way, h], row_r.at[way, h], r, c_y).wait_recv()

    def col_piece(h):
        piece = tcol.at[r, halves[h]]
        return send(piece, piece, col_s.at[h], col_r.at[h], r_x, c)

    col_pair = send(tcol.at[r], tcol.at[r], col_s.at[2], col_r.at[2], r_k, c)
    col_relay = send(tcol.at[r_x], tcol.at[r_x], col_s.at[3], col_r.at[3], r_k, c)

    def lad_copy(slot, h):
        return send(trow.at[slot, halves[h]], tlad.at[r, halves[h]], lad_s.at[slot, h], lad_r.at[r, h], slot, c)

    def dispatch(slot, h):
        @pl.when(slot != r)
        def _():
            lad_copy(slot, h).start()

        @pl.when(slot == r)
        def _():
            tlad[r, halves[h]] = trow[slot, halves[h]]

    def lad_wait(slot, h):
        send(trow.at[0, halves[h]], tlad.at[slot, halves[h]], lad_s.at[slot, h], lad_r.at[slot, h], r, c).wait_recv()

    def lad_forward(slot, h):
        piece = tlad.at[slot, halves[h]]
        return send(piece, piece, fw_s.at[slot, h], lad_r.at[slot, h], r, c_y)

    gives = jnp.logical_and(x != z, k == y)

    def forward(h):
        @pl.when(gives)
        def _():
            for slot in (r_x, r_d):
                with scope("lad_f"):
                    lad_wait(slot, h)
                lad_forward(slot, h).start()

    @pl.when(x == z)
    def _():
        col_piece(0).start()

    for h in range(2):
        row_copy(0, h).start()
        row_copy(1, h).start()
        dispatch(c, h)
    col_pair.start()

    with scope("wait_w"):
        load_w.wait()

    def mixed(slot):
        for m in range(5):
            split_cols(lambda lo, hi: trow[slot, :, lo:hi].astype(F32), planes, m)
        for h in range(2):
            parts = []
            for j in range(8):
                parts += take_j(planes, 8 * h + j, 0, 4 * AB)
            tm[:, 1152 * h : 1152 * h + 1152] = jnp.concatenate(parts, axis=1).astype(BF16)
        at = pl.multiple_of(slot * V, 8)
        r3[pl.ds(at, V), :] = lax.dot_general(
            tm[...], wv[...], (((1,), (1,)), ((), ())), preferred_element_type=F32
        )

    with scope("mixed_c"):
        mixed(c)

    with scope("row10"):
        row_wait(1, 0)
    row_copy(2, 0).start()
    dispatch(c_z, 0)
    with scope("row00"):
        row_wait(0, 0)
    dispatch(c_y, 0)

    load_d.wait()
    for m in range(5):
        split_cols(lambda lo, hi: d32[:, lo:hi], planes, m)
    for cc in range(4):
        parts = []
        for j in range(4):
            parts += take_j(planes, 4 * cc + j, 0, 4 * AB)
        dsnd[cc] = jnp.concatenate(parts, axis=1)
    own_rows = pl.ds(pl.multiple_of(c * V, 8), V)
    drcv[own_rows, :] = dsnd[c]

    with scope("row11"):
        row_wait(1, 1)
    dispatch(c_z, 1)
    with scope("row01"):
        row_wait(0, 1)
    row_copy(2, 1).start()
    dispatch(c_y, 1)
    forward(0)
    with scope("mixed_c_z"):
        mixed(c_z)
    with scope("row20"):
        row_wait(2, 0)
    with scope("row21"):
        row_wait(2, 1)

    @pl.when(x != z)
    def _():
        dispatch(c_d, 0)
        dispatch(c_d, 1)

    @pl.when(x == z)
    def _():
        col_piece(1).start()

    forward(1)
    with scope("mixed_c_y"):
        mixed(c_y)
    with scope("mixed_c_d"):
        mixed(c_d)
    d_copy = [
        send(dsnd.at[peer], drcv.at[own_rows], d_s.at[q], d_r.at[q], r, peer) for q, peer in enumerate(col_peers)
    ]

    for b in range(5):
        n = 128 if b < 4 else 64
        planes2[b, :, 0:n] = r3[:, 128 * b : 128 * b + n]
        for i in range(4):
            pp[V * i : V * i + V, 128 * b : 128 * b + n] = planes2[b, pl.ds(i, V, stride=4), :][:, 0:n]
    pt[...] = pp[...].T

    top, low = slice(0, PB // 2), slice(PB // 2, PB)
    p_copy = send(pt, pr, p_s.at[0], p_r.at[0], c, r)
    p_out = (
        send(pt.at[top], prel.at[0], p_s.at[1], p_r.at[1], r_x, c),
        send(pt.at[low], prel.at[1], p_s.at[2], p_r.at[2], r, c_z),
    )
    p_on = (
        send(prel.at[0], pr.at[top], p_s.at[3], p_r.at[3], c, r_x),
        send(prel.at[1], pr.at[low], p_s.at[4], p_r.at[4], c_z, r),
    )

    @pl.when(jnp.logical_and(x == z, r != c))
    def _():
        p_copy.start()

    @pl.when(r == c)
    def _():
        pr[...] = pt[...]

    @pl.when(x != z)
    def _():
        p_out[1].start()
        p_out[0].start()

    q_copy = [send(xq, xqr.at[c], q_s.at[q], q_r.at[q], r, peer) for q, peer in enumerate(col_peers)]

    def hole_x():
        load_vo.wait()
        send(tcol.at[r_k], tcol.at[r_k], col_s.at[2], col_r.at[2], r_k, c).wait_recv()

        @pl.when(jnp.logical_and(x == z, r != c))
        def _():
            send(tcol.at[r_x], tcol.at[r_x], f_s.at[0], col_r.at[4], r_k, c).wait_recv()

        @pl.when(r != c)
        def _():
            send(tcol.at[r_d], tcol.at[r_d], col_s.at[3], col_r.at[3], r_k, c).wait_recv()

        xq[...] = lax.dot_general(
            vo[...], tcol[...].reshape(4 * RB, CB), (((1,), (1,)), ((), ())), preferred_element_type=F32
        )
        xqr[c] = xq[...]
        for copy in q_copy:
            copy.start()

    @pl.when(x != z)
    def _():
        with scope("col"):
            for h in range(2):
                piece = tcol.at[r_x, halves[h]]
                send(piece, piece, col_s.at[h], col_r.at[h], r_x, c).wait_recv()
        col_relay.start()
        with scope("hole_x"):
            hole_x()
        for copy in d_copy:
            copy.start()

    @pl.when(jnp.logical_not(gives))
    def _():
        for h in range(2):
            for slot in (r_x, r_d):
                with scope("lad"):
                    lad_wait(slot, h)

    for h in range(2):
        with scope("lad_k"):
            lad_wait(r_k, h)

    fwd = (
        send(tlad.at[r_d], tcol.at[r_d], f_s.at[0], col_r.at[4], r_k, c),
        send(tlad.at[r_x], tcol.at[r_x], f_s.at[1], col_r.at[3], r_k, c),
    )

    @pl.when(r == c)
    def _():
        for copy in fwd:
            copy.start()
        tcol[r_d] = tlad[r_d]
        tcol[r_x] = tlad[r_x]

    def w_copy(rr):
        return send(wt.at[RB * rr : RB * rr + RB], wblk.at[r], w_s.at[rr], w_r.at[r], rr, c)

    def hole_w():
        load_oo.wait()
        for q, peer in enumerate(col_peers):
            send(xq, xqr.at[peer], q_s.at[q], q_r.at[q], r, peer).wait_recv()
        x_sum = (xqr[0] + xqr[1]) + (xqr[2] + xqr[3])
        w_hole = oo[...].astype(F32) + 0.5 * x_sum
        wt[...] = w_hole.T.astype(BF16)
        wblk[r] = wt[pl.ds(pl.multiple_of(r * RB, RB), RB), :]
        for rr in range(4):

            @pl.when(r != rr)
            def _():
                w_copy(rr).start()

    def d2_copy(n):
        return send(acc.at[n, 1 - k], d2r.at[n], dd_s.at[n], dd_r.at[n], r_k, c)

    def xx_copy(n):
        return send(xsb.at[n], xrb.at[n], xx_s.at[n], xx_r.at[n], r_x, c)

    d2_tail = send(acct.at[1 - k], d2t, dd_s.at[NCH], dd_r.at[NCH], r_k, c)
    xx_tail = send(xst, xrt, xx_s.at[NCH], xx_r.at[NCH], r_x, c)

    def gather_w():
        with scope("w_in"):
            for rr in range(4):

                @pl.when(r != rr)
                def _():
                    send(wt.at[0:RB], wblk.at[rr], w_s.at[rr], w_r.at[rr], rr, c).wait_recv()

        wf[...] = jnp.concatenate([wblk[rr].astype(F32) for rr in range(4)], axis=1).astype(BF16)

    def close(lo, hi, landed):
        hole = jnp.dot(wf[...], tcol[:, :, lo:hi].reshape(4 * RB, hi - lo), preferred_element_type=F32)
        r1[:, lo:hi] = r1[:, lo:hi] + landed + hole + vo[:, lo:hi].astype(F32)

    def stripe_rows(m):
        return 32 if m < 4 else 16

    def l_copy(m, q):
        rows = stripe_rows(m)
        there = pl.ds(pl.multiple_of(c * V + 32 * m, 8), rows)
        peer = col_peers[q]
        return send(
            lsnd.at[peer, 32 * m : 32 * m + rows], lrcv.at[there], l_s.at[m, q], l_r.at[m, q], r, peer
        )

    def stripe_out(m):
        for n in ((0, 1, 2), (3, 4), (5, 6), (7, 8), (9,))[m]:
            with scope("sum"):
                xx_copy(n).wait_recv()
            close(CW * n, CW * n + CW, xrb[n])
        if m == 4:
            xx_tail.wait_recv()
            close(NCH * CW, CB, xrt[...])
        split_cols(lambda lo, hi: r1[:, lo:hi], planes, m)
        first, rows = 32 * m, stripe_rows(m)
        for cc in range(4):
            parts = []
            for j in range(4):
                parts += take_j(planes, 4 * cc + j, RB * 8 * m, rows)
            lsnd[cc, first : first + rows, :] = jnp.concatenate(parts, axis=1)
        there = pl.ds(pl.multiple_of(c * V + first, 8), rows)
        lrcv[there, :] = lsnd[c, first : first + rows, :]
        for q in range(3):
            l_copy(m, q).start()

    load_tail.wait()
    part = jnp.dot(tlad[...].reshape(4 * RB, CB), vtail[...], preferred_element_type=F32)
    for rr in range(4):
        acct[rr % 2, rr // 2] = part[RB * rr : RB * rr + RB]
    d2_tail.start()

    def second(n):
        with scope("pair"):
            d2_copy(n).wait_recv()
        xsb[n] = acc[n, k, 1 - x] + d2r[n, 1 - x]
        at = pl.multiple_of(n * CW, CW)
        r1[:, pl.ds(at, CW)] = acc[n, k, x] + d2r[n, x]
        xx_copy(n).start()

    def ladder_step(n, carry):
        slot = n % 2
        with scope("wait_v"):
            load_v(n, slot).wait()
        with scope("dot"):
            for h in range(2):
                part = jnp.dot(
                    tlad[...].reshape(4 * RB, CB), vbuf[slot, :, 256 * h : 256 * h + 256], preferred_element_type=F32
                )
                for rr in range(4):
                    acc[n, rr % 2, rr // 2, :, 256 * h : 256 * h + 256] = part[RB * rr : RB * rr + RB]
        d2_copy(n).start()

        @pl.when(n + 2 < NCH)
        def _():
            load_v(n + 2, slot).start()

        @pl.when(n == 0)
        def _():
            d2_tail.wait_recv()
            xst[...] = acct[k, 1 - x] + d2t[1 - x]
            r1[:, NCH * CW : CB] = acct[k, x] + d2t[x]
            xx_tail.start()

        @pl.when(n > 0)
        def _():
            second(n - 1)

        @pl.when(jnp.logical_and(n == 1, x == z))
        def _():
            with scope("hole_x"):
                hole_x()
            for copy in d_copy:
                copy.start()

        @pl.when(jnp.logical_and(n == 4, x == z))
        def _():
            for copy, on in zip(p_out, p_on):
                with scope("relay"):
                    copy.wait_recv()
                on.start()

        @pl.when(n == jnp.where(x == z, 6, 1))
        def _():
            with scope("hole_w"):
                hole_w()

        @pl.when(n == 7)
        def _():
            gather_w()
            stripe_out(0)

        @pl.when(n == 9)
        def _():
            stripe_out(1)

        return carry

    lax.fori_loop(0, NCH, ladder_step, 0)
    second(NCH - 1)

    for m in range(2, 5):
        stripe_out(m)

    with scope("mirror"):

        @pl.when(jnp.logical_and(x == z, r != c))
        def _():
            p_copy.wait_recv()

        @pl.when(x != z)
        def _():
            for copy in p_on:
                copy.wait_recv()

    pp[...] = pp[...] + pr[...]
    for q, peer in enumerate(col_peers):
        at = pl.ds(pl.multiple_of(peer * V, 8), V)
        with scope("denom"):
            send(dsnd.at[peer], drcv.at[at], d_s.at[q], d_r.at[q], r, peer).wait_recv()
    for m in range(5):
        rows = 32 if m < 4 else 16
        for q, peer in enumerate(col_peers):
            at = pl.ds(pl.multiple_of(peer * V + 32 * m, 8), rows)
            with scope("regroup"):
                send(
                    lsnd.at[peer, 32 * m : 32 * m + rows], lrcv.at[at], l_s.at[m, q], l_r.at[m, q], r, peer
                ).wait_recv()
    for b in range(5):
        n = 128 if b < 4 else 64
        cols = slice(128 * b, 128 * b + n)
        planes[0, 0:PB, 0:n] = lrcv[:, cols]
        planes2[b, :, 0:n] = drcv[:, cols]
        for i in range(4):
            rows = slice(V * i, V * i + V)
            top = planes[0, pl.ds(i, V, stride=4), :][:, 0:n] + pp[rows, cols]
            out_ref[rows, cols] = top / planes2[b, pl.ds(i, V, stride=4), :][:, 0:n]

    for copy in (col_pair, *q_copy, *d_copy, d2_tail, xx_tail):
        copy.wait_send()
    for m in range(5):
        for q in range(3):
            l_copy(m, q).wait_send()
    for way in range(3):
        for h in range(2):
            row_copy(way, h).wait_send()

    @pl.when(x == z)
    def _():
        for h in range(2):
            col_piece(h).wait_send()
        for copy in p_on:
            copy.wait_send()

    @pl.when(jnp.logical_and(x == z, r != c))
    def _():
        p_copy.wait_send()

    @pl.when(x != z)
    def _():
        col_relay.wait_send()
        for copy in p_out:
            copy.wait_send()

    @pl.when(r == c)
    def _():
        for copy in fwd:
            copy.wait_send()

    @pl.when(gives)
    def _():
        for h in range(2):
            for slot in (r_x, r_d):
                lad_forward(slot, h).wait_send()

    for slot in range(4):

        @pl.when(slot != r)
        def _():
            w_copy(slot).wait_send()

        @pl.when(jnp.logical_and(slot != r, jnp.logical_or(slot != c_d, x != z)))
        def _():
            for h in range(2):
                lad_copy(slot, h).wait_send()

    def drain(n, carry):
        d2_copy(n).wait_send()
        xx_copy(n).wait_send()
        return carry

    lax.fori_loop(0, NCH, drain, 0)


def solution(mesh):
    vm = pltpu.VMEM
    dma = pltpu.SemaphoreType.DMA
    scratch = [
        vm((RB, CB), F32), vm((RB, CB), F32), vm((RB, CB), BF16), vm((PB, O * V), BF16),
        vm((4, RB, CB), BF16), vm((4, RB, CB), BF16), vm((4, RB, CB), BF16),
        vm((2, AB * RB, 128), F32), vm((V, O * V), BF16),
        vm((PB, PB), F32), vm((PB, PB), F32), vm((PB, PB), F32), vm((PB, PB), F32),
        vm((4, V, PB), F32), vm((PB, PB), F32), vm((4, V, PB), F32), vm((PB, PB), F32),
        vm((5, PB, 128), F32), vm((2, PB // 2, PB), F32),
        vm((RB, O * O), F32), vm((4, RB, O * O), F32), vm((O * O, RB), BF16), vm((RB, O * O), BF16), vm((4, RB, RB), BF16), vm((RB, O * O), BF16),
        vm((2, CB, CW), BF16), vm((CB, TW), BF16),
        vm((NCH, 2, 2, RB, CW), F32), vm((NCH, 2, RB, CW), F32), vm((NCH, RB, CW), F32), vm((NCH, RB, CW), F32),
        vm((2, 2, RB, TW), F32), vm((2, RB, TW), F32), vm((RB, TW), F32), vm((RB, TW), F32),
        vm((RB, CB), F32),
        dma((6,)), dma((2,)), dma((3, 2)), dma((3, 2)), dma((5,)), dma((5,)), dma((4, 2)), dma((4, 2)),
        dma((3,)), dma((3,)), dma((3,)), dma((3,)), dma((5, 3)), dma((5, 3)), dma((5,)), dma((5,)), dma((4, 2)),
        dma((NCH + 1,)), dma((NCH + 1,)), dma((NCH + 1,)), dma((NCH + 1,)), dma((4,)), dma((4,)), dma((2,)),
    ]
    hbm = pl.BlockSpec(memory_space=pl.ANY)
    vmem = pl.BlockSpec(memory_space=pltpu.VMEM)
    call = pl.pallas_call(
        kernel,
        out_shape=jax.ShapeDtypeStruct((PB, PB), F32),
        in_specs=[hbm] * 6,
        out_specs=vmem,
        scratch_shapes=scratch,
        compiler_params=pltpu.CompilerParams(
            collective_id=0, has_side_effects=True, vmem_limit_bytes=67_000_000
        ),
        name="sweep",
    )
    def local_sweep(t_blk, d_blk, voovv_blk, vvvvv_blk, oooo, w_blk):
        return call(t_blk, d_blk, voovv_blk, vvvvv_blk, oooo, w_blk.T)

    return jax.shard_map(
        local_sweep,
        mesh=mesh,
        in_specs=(P("row", "col"), P("row", "col"), P("row", "col"), P("row", "col"), P(None, None), P(None, "col")),
        out_specs=P("row", "col"),
        check_vma=False,
    )
```

```python
import functools

import jax
import jax.numpy as jnp
from jax import lax
from jax.experimental import pallas as pl
from jax.experimental.pallas import tpu as pltpu
from jax.sharding import PartitionSpec as P

MESH = pl.DeviceIdType.MESH
scope = jax.named_scope
F32 = jnp.float32
BF16 = jnp.bfloat16

O = 16
V = 144
RB = 64
CB = 5184
AB = 36
PB = 576
CW = 512
NCH = CB // CW
TW = CB - NCH * CW


def stripe(load, m, q):
    first = 1152 * m + V * q
    low = first // 128 * 128
    high = min(-(-(first + V) // 128) * 128, CB)
    return load(low, high)[:, first - low : first - low + V]


def split_cols(load, planes, m):
    for q in range(8 if m < 4 else 4):
        piece = stripe(load, m, q)
        base = RB * (8 * m + q)
        planes[0, base : base + RB, :] = piece[:, 0:128]
        planes[1, base : base + RB, 0:16] = piece[:, 128:144]


def take_j(planes, j, base, rows):
    wide = planes[0, pl.ds(base + j, rows, stride=16), :]
    rest = planes[1, pl.ds(base + j, rows, stride=16), :]
    return [wide, rest[:, 0:16]]


def kernel(
    t_hbm, d_hbm, vo_hbm, vv_hbm, oo_hbm, w_hbm, out_ref,
    t32, d32, vo, wv, trow, tcol, tlad, planes, tm, r3, pp, pt, pr,
    dsnd, drcv, lsnd, lrcv, planes2, prel, xq, xqr, wt, oo, wblk, wf, vbuf, vtail,
    acc, d2r, xsb, xrb, acct, d2t, xst, xrt, r1,
    in_sem, v_sem, row_s, row_r, col_s, col_r, lad_s, lad_r, q_s, q_r,
    d_s, d_r, l_s, l_r, p_s, p_r, fw_s, dd_s, dd_r, xx_s, xx_r, w_s, w_r, f_s,
):
    r = lax.axis_index("row")
    c = lax.axis_index("col")
    x, k = r // 2, r % 2
    z, y = c // 2, c % 2
    r_k, r_x = 2 * x + 1 - k, 2 * (1 - x) + k
    r_d = 2 * (1 - x) + 1 - k
    c_y, c_z = 2 * z + 1 - y, 2 * (1 - z) + y
    c_d = 2 * (1 - z) + 1 - y
    col_peers = (c_y, c_z, c_d)

    def send(src, dst, ss, rs, row, col):
        return pltpu.make_async_remote_copy(
            src_ref=src, dst_ref=dst, send_sem=ss, recv_sem=rs,
            device_id={"row": row, "col": col}, device_id_type=MESH,
        )

    def load_v(n, slot):
        at = pl.multiple_of(n * CW, CW)
        return pltpu.make_async_copy(vv_hbm.at[:, pl.ds(at, CW)], vbuf.at[slot], v_sem.at[slot])

    load_t = pltpu.make_async_copy(t_hbm, t32, in_sem.at[0])
    load_d = pltpu.make_async_copy(d_hbm, d32, in_sem.at[1])
    load_vo = pltpu.make_async_copy(vo_hbm, vo, in_sem.at[2])
    load_w = pltpu.make_async_copy(w_hbm, wv, in_sem.at[3])
    load_tail = pltpu.make_async_copy(vv_hbm.at[:, pl.ds(NCH * CW, TW)], vtail, in_sem.at[4])
    load_oo = pltpu.make_async_copy(oo_hbm.at[pl.ds(pl.multiple_of(r * RB, RB), RB)], oo, in_sem.at[5])
    load_t.start()
    load_w.start()
    load_d.start()
    load_vo.start()
    load_tail.start()
    load_oo.start()
    load_v(0, 0).start()
    load_v(1, 1).start()

    barrier = pltpu.get_barrier_semaphore()
    for rr in range(4):
        for cc in range(4):
            pl.semaphore_signal(barrier, inc=1, device_id={"row": rr, "col": cc}, device_id_type=MESH)

    with scope("wait_t"):
        load_t.wait()
    for m in range(9):
        piece = t32[:, PB * m : PB * m + PB].astype(BF16)
        trow[c, :, PB * m : PB * m + PB] = piece
        tcol[r, :, PB * m : PB * m + PB] = piece
    with scope("barrier"):
        pl.semaphore_wait(barrier, 16)

    half = RB // 2
    halves = (slice(0, half), slice(half, RB))

    def row_copy(way, h):
        block, peer = ((c, c_y), (c, c_z), ((c_z, c_y), (c_y, c_z))[h])[way]
        piece = trow.at[block, halves[h]]
        return send(piece, piece, row_s.at[way, h], row_r.at[way, h], r, peer)

    def row_wait(way, h):
        piece = trow.at[(c_y, c_z, c_d)[way], halves[h]]
        send(piece, piece, row_s.at[way, h], row_r.at[way, h], r, c_y).wait_recv()

    def col_piece(h):
        piece = tcol.at[r, halves[h]]
        return send(piece, piece, col_s.at[h], col_r.at[h], r_x, c)

    col_pair = send(tcol.at[r], tcol.at[r], col_s.at[2], col_r.at[2], r_k, c)
    col_relay = send(tcol.at[r_x], tcol.at[r_x], col_s.at[3], col_r.at[3], r_k, c)

    def lad_copy(slot, h):
        return send(trow.at[slot, halves[h]], tlad.at[r, halves[h]], lad_s.at[slot, h], lad_r.at[r, h], slot, c)

    def dispatch(slot, h):
        @pl.when(slot != r)
        def _():
            lad_copy(slot, h).start()

        @pl.when(slot == r)
        def _():
            tlad[r, halves[h]] = trow[slot, halves[h]]

    def lad_wait(slot, h):
        send(trow.at[0, halves[h]], tlad.at[slot, halves[h]], lad_s.at[slot, h], lad_r.at[slot, h], r, c).wait_recv()

    def lad_forward(slot, h):
        piece = tlad.at[slot, halves[h]]
        return send(piece, piece, fw_s.at[slot, h], lad_r.at[slot, h], r, c_y)

    gives = jnp.logical_and(x != z, k == y)

    def forward(h):
        @pl.when(gives)
        def _():
            for slot in (r_x, r_d):
                with scope("lad_f"):
                    lad_wait(slot, h)
                lad_forward(slot, h).start()

    @pl.when(x == z)
    def _():
        col_piece(0).start()

    for h in range(2):
        row_copy(0, h).start()
        row_copy(1, h).start()
        dispatch(c, h)
    col_pair.start()

    with scope("wait_w"):
        load_w.wait()

    def mixed(slot):
        for m in range(5):
            split_cols(lambda lo, hi: trow[slot, :, lo:hi].astype(F32), planes, m)
        for h in range(2):
            parts = []
            for j in range(8):
                parts += take_j(planes, 8 * h + j, 0, 4 * AB)
            tm[:, 1152 * h : 1152 * h + 1152] = jnp.concatenate(parts, axis=1).astype(BF16)
        at = pl.multiple_of(slot * V, 8)
        r3[pl.ds(at, V), :] = lax.dot_general(
            tm[...], wv[...], (((1,), (1,)), ((), ())), preferred_element_type=F32
        )

    with scope("mixed_c"):
        mixed(c)

    with scope("row10"):
        row_wait(1, 0)
    row_copy(2, 0).start()
    dispatch(c_z, 0)
    with scope("row00"):
        row_wait(0, 0)
    dispatch(c_y, 0)

    load_d.wait()
    for m in range(5):
        split_cols(lambda lo, hi: d32[:, lo:hi], planes, m)
    for cc in range(4):
        parts = []
        for j in range(4):
            parts += take_j(planes, 4 * cc + j, 0, 4 * AB)
        dsnd[cc] = jnp.concatenate(parts, axis=1)
    own_rows = pl.ds(pl.multiple_of(c * V, 8), V)
    drcv[own_rows, :] = dsnd[c]

    with scope("row11"):
        row_wait(1, 1)
    dispatch(c_z, 1)
    with scope("row01"):
        row_wait(0, 1)
    row_copy(2, 1).start()
    dispatch(c_y, 1)
    forward(0)
    with scope("mixed_c_z"):
        mixed(c_z)
    with scope("row20"):
        row_wait(2, 0)
    with scope("row21"):
        row_wait(2, 1)

    @pl.when(x != z)
    def _():
        dispatch(c_d, 0)
        dispatch(c_d, 1)

    @pl.when(x == z)
    def _():
        col_piece(1).start()

    forward(1)
    with scope("mixed_c_y"):
        mixed(c_y)
    with scope("mixed_c_d"):
        mixed(c_d)
    d_copy = [
        send(dsnd.at[peer], drcv.at[own_rows], d_s.at[q], d_r.at[q], r, peer) for q, peer in enumerate(col_peers)
    ]

    for b in range(5):
        n = 128 if b < 4 else 64
        planes2[b, :, 0:n] = r3[:, 128 * b : 128 * b + n]
        for i in range(4):
            pp[V * i : V * i + V, 128 * b : 128 * b + n] = planes2[b, pl.ds(i, V, stride=4), :][:, 0:n]
    pt[...] = pp[...].T

    top, low = slice(0, PB // 2), slice(PB // 2, PB)
    p_copy = send(pt, pr, p_s.at[0], p_r.at[0], c, r)
    p_out = (
        send(pt.at[top], prel.at[0], p_s.at[1], p_r.at[1], r_x, c),
        send(pt.at[low], prel.at[1], p_s.at[2], p_r.at[2], r, c_z),
    )
    p_on = (
        send(prel.at[0], pr.at[top], p_s.at[3], p_r.at[3], c, r_x),
        send(prel.at[1], pr.at[low], p_s.at[4], p_r.at[4], c_z, r),
    )

    @pl.when(jnp.logical_and(x == z, r != c))
    def _():
        p_copy.start()

    @pl.when(r == c)
    def _():
        pr[...] = pt[...]

    @pl.when(x != z)
    def _():
        p_out[1].start()
        p_out[0].start()

    q_copy = [send(xq, xqr.at[c], q_s.at[q], q_r.at[q], r, peer) for q, peer in enumerate(col_peers)]

    def hole_x():
        load_vo.wait()
        send(tcol.at[r_k], tcol.at[r_k], col_s.at[2], col_r.at[2], r_k, c).wait_recv()

        @pl.when(jnp.logical_and(x == z, r != c))
        def _():
            send(tcol.at[r_x], tcol.at[r_x], f_s.at[0], col_r.at[4], r_k, c).wait_recv()

        @pl.when(r != c)
        def _():
            send(tcol.at[r_d], tcol.at[r_d], col_s.at[3], col_r.at[3], r_k, c).wait_recv()

        xq[...] = lax.dot_general(
            vo[...], tcol[...].reshape(4 * RB, CB), (((1,), (1,)), ((), ())), preferred_element_type=F32
        )
        xqr[c] = xq[...]
        for copy in q_copy:
            copy.start()

    @pl.when(x != z)
    def _():
        with scope("col"):
            for h in range(2):
                piece = tcol.at[r_x, halves[h]]
                send(piece, piece, col_s.at[h], col_r.at[h], r_x, c).wait_recv()
        col_relay.start()
        with scope("hole_x"):
            hole_x()

    @pl.when(jnp.logical_not(gives))
    def _():
        for h in range(2):
            for slot in (r_x, r_d):
                with scope("lad"):
                    lad_wait(slot, h)

    for h in range(2):
        with scope("lad_k"):
            lad_wait(r_k, h)

    fwd = (
        send(tlad.at[r_d], tcol.at[r_d], f_s.at[0], col_r.at[4], r_k, c),
        send(tlad.at[r_x], tcol.at[r_x], f_s.at[1], col_r.at[3], r_k, c),
    )

    @pl.when(r == c)
    def _():
        for copy in fwd:
            copy.start()
        tcol[r_d] = tlad[r_d]
        tcol[r_x] = tlad[r_x]

    def w_copy(rr):
        return send(wt.at[RB * rr : RB * rr + RB], wblk.at[r], w_s.at[rr], w_r.at[r], rr, c)

    def hole_w():
        load_oo.wait()
        for q, peer in enumerate(col_peers):
            send(xq, xqr.at[peer], q_s.at[q], q_r.at[q], r, peer).wait_recv()
        x_sum = (xqr[0] + xqr[1]) + (xqr[2] + xqr[3])
        w_hole = oo[...].astype(F32) + 0.5 * x_sum
        wt[...] = w_hole.T.astype(BF16)
        wblk[r] = wt[pl.ds(pl.multiple_of(r * RB, RB), RB), :]
        for rr in range(4):

            @pl.when(r != rr)
            def _():
                w_copy(rr).start()

    def d2_copy(n):
        return send(acc.at[n, 1 - k], d2r.at[n], dd_s.at[n], dd_r.at[n], r_k, c)

    def xx_copy(n):
        return send(xsb.at[n], xrb.at[n], xx_s.at[n], xx_r.at[n], r_x, c)

    d2_tail = send(acct.at[1 - k], d2t, dd_s.at[NCH], dd_r.at[NCH], r_k, c)
    xx_tail = send(xst, xrt, xx_s.at[NCH], xx_r.at[NCH], r_x, c)

    def gather_w():
        with scope("w_in"):
            for rr in range(4):

                @pl.when(r != rr)
                def _():
                    send(wt.at[0:RB], wblk.at[rr], w_s.at[rr], w_r.at[rr], rr, c).wait_recv()

        wf[...] = jnp.concatenate([wblk[rr].astype(F32) for rr in range(4)], axis=1).astype(BF16)

    def close(lo, hi, landed):
        hole = jnp.dot(wf[...], tcol[:, :, lo:hi].reshape(4 * RB, hi - lo), preferred_element_type=F32)
        r1[:, lo:hi] = r1[:, lo:hi] + landed + hole + vo[:, lo:hi].astype(F32)

    def stripe_rows(m):
        return 32 if m < 4 else 16

    def l_copy(m, q):
        rows = stripe_rows(m)
        there = pl.ds(pl.multiple_of(c * V + 32 * m, 8), rows)
        peer = col_peers[q]
        return send(
            lsnd.at[peer, 32 * m : 32 * m + rows], lrcv.at[there], l_s.at[m, q], l_r.at[m, q], r, peer
        )

    def stripe_out(m):
        for n in ((0, 1, 2), (3, 4), (5, 6), (7, 8), (9,))[m]:
            with scope("sum"):
                xx_copy(n).wait_recv()
            close(CW * n, CW * n + CW, xrb[n])
        if m == 4:
            xx_tail.wait_recv()
            close(NCH * CW, CB, xrt[...])
        split_cols(lambda lo, hi: r1[:, lo:hi], planes, m)
        first, rows = 32 * m, stripe_rows(m)
        for cc in range(4):
            parts = []
            for j in range(4):
                parts += take_j(planes, 4 * cc + j, RB * 8 * m, rows)
            lsnd[cc, first : first + rows, :] = jnp.concatenate(parts, axis=1)
        there = pl.ds(pl.multiple_of(c * V + first, 8), rows)
        lrcv[there, :] = lsnd[c, first : first + rows, :]
        for q in range(3):
            l_copy(m, q).start()

    load_tail.wait()
    part = jnp.dot(tlad[...].reshape(4 * RB, CB), vtail[...], preferred_element_type=F32)
    for rr in range(4):
        acct[rr % 2, rr // 2] = part[RB * rr : RB * rr + RB]
    d2_tail.start()

    def second(n):
        with scope("pair"):
            d2_copy(n).wait_recv()
        xsb[n] = acc[n, k, 1 - x] + d2r[n, 1 - x]
        at = pl.multiple_of(n * CW, CW)
        r1[:, pl.ds(at, CW)] = acc[n, k, x] + d2r[n, x]
        xx_copy(n).start()

    def ladder_step(n, carry):
        slot = n % 2
        with scope("wait_v"):
            load_v(n, slot).wait()
        with scope("dot"):
            for h in range(2):
                part = jnp.dot(
                    tlad[...].reshape(4 * RB, CB), vbuf[slot, :, 256 * h : 256 * h + 256], preferred_element_type=F32
                )
                for rr in range(4):
                    acc[n, rr % 2, rr // 2, :, 256 * h : 256 * h + 256] = part[RB * rr : RB * rr + RB]
        d2_copy(n).start()

        @pl.when(n + 2 < NCH)
        def _():
            load_v(n + 2, slot).start()

        @pl.when(n == 0)
        def _():
            d2_tail.wait_recv()
            xst[...] = acct[k, 1 - x] + d2t[1 - x]
            r1[:, NCH * CW : CB] = acct[k, x] + d2t[x]
            xx_tail.start()

        @pl.when(n > 0)
        def _():
            second(n - 1)

        @pl.when(jnp.logical_and(n == 1, x == z))
        def _():
            with scope("hole_x"):
                hole_x()
            for copy in d_copy:
                copy.start()

        @pl.when(jnp.logical_and(n == 4, x != z))
        def _():
            for copy in d_copy:
                copy.start()

        @pl.when(n == jnp.where(x == z, 8, 6))
        def _():
            with scope("hole_w"):
                hole_w()

        @pl.when(jnp.logical_and(n == 9, x != z))
        def _():
            gather_w()
            stripe_out(0)
            stripe_out(1)

        return carry

    lax.fori_loop(0, NCH, ladder_step, 0)
    second(NCH - 1)

    @pl.when(x == z)
    def _():
        for copy, on in zip(p_out, p_on):
            with scope("relay"):
                copy.wait_recv()
            on.start()
        gather_w()
        stripe_out(0)
        stripe_out(1)

    for m in range(2, 5):
        stripe_out(m)

    with scope("mirror"):

        @pl.when(jnp.logical_and(x == z, r != c))
        def _():
            p_copy.wait_recv()

        @pl.when(x != z)
        def _():
            for copy in p_on:
                copy.wait_recv()

    pp[...] = pp[...] + pr[...]
    for q, peer in enumerate(col_peers):
        at = pl.ds(pl.multiple_of(peer * V, 8), V)
        with scope("denom"):
            send(dsnd.at[peer], drcv.at[at], d_s.at[q], d_r.at[q], r, peer).wait_recv()
    for m in range(5):
        rows = 32 if m < 4 else 16
        for q, peer in enumerate(col_peers):
            at = pl.ds(pl.multiple_of(peer * V + 32 * m, 8), rows)
            with scope("regroup"):
                send(
                    lsnd.at[peer, 32 * m : 32 * m + rows], lrcv.at[at], l_s.at[m, q], l_r.at[m, q], r, peer
                ).wait_recv()
    for b in range(5):
        n = 128 if b < 4 else 64
        cols = slice(128 * b, 128 * b + n)
        planes[0, 0:PB, 0:n] = lrcv[:, cols]
        planes2[b, :, 0:n] = drcv[:, cols]
        for i in range(4):
            rows = slice(V * i, V * i + V)
            top = planes[0, pl.ds(i, V, stride=4), :][:, 0:n] + pp[rows, cols]
            out_ref[rows, cols] = top / planes2[b, pl.ds(i, V, stride=4), :][:, 0:n]

    for copy in (col_pair, *q_copy, *d_copy, d2_tail, xx_tail):
        copy.wait_send()
    for m in range(5):
        for q in range(3):
            l_copy(m, q).wait_send()
    for way in range(3):
        for h in range(2):
            row_copy(way, h).wait_send()

    @pl.when(x == z)
    def _():
        for h in range(2):
            col_piece(h).wait_send()
        for copy in p_on:
            copy.wait_send()

    @pl.when(jnp.logical_and(x == z, r != c))
    def _():
        p_copy.wait_send()

    @pl.when(x != z)
    def _():
        col_relay.wait_send()
        for copy in p_out:
            copy.wait_send()

    @pl.when(r == c)
    def _():
        for copy in fwd:
            copy.wait_send()

    @pl.when(gives)
    def _():
        for h in range(2):
            for slot in (r_x, r_d):
                lad_forward(slot, h).wait_send()

    for slot in range(4):

        @pl.when(slot != r)
        def _():
            w_copy(slot).wait_send()

        @pl.when(jnp.logical_and(slot != r, jnp.logical_or(slot != c_d, x != z)))
        def _():
            for h in range(2):
                lad_copy(slot, h).wait_send()

    def drain(n, carry):
        d2_copy(n).wait_send()
        xx_copy(n).wait_send()
        return carry

    lax.fori_loop(0, NCH, drain, 0)


def solution(mesh):
    vm = pltpu.VMEM
    dma = pltpu.SemaphoreType.DMA
    scratch = [
        vm((RB, CB), F32), vm((RB, CB), F32), vm((RB, CB), BF16), vm((PB, O * V), BF16),
        vm((4, RB, CB), BF16), vm((4, RB, CB), BF16), vm((4, RB, CB), BF16),
        vm((2, AB * RB, 128), F32), vm((V, O * V), BF16),
        vm((PB, PB), F32), vm((PB, PB), F32), vm((PB, PB), F32), vm((PB, PB), F32),
        vm((4, V, PB), F32), vm((PB, PB), F32), vm((4, V, PB), F32), vm((PB, PB), F32),
        vm((5, PB, 128), F32), vm((2, PB // 2, PB), F32),
        vm((RB, O * O), F32), vm((4, RB, O * O), F32), vm((O * O, RB), BF16), vm((RB, O * O), BF16), vm((4, RB, RB), BF16), vm((RB, O * O), BF16),
        vm((2, CB, CW), BF16), vm((CB, TW), BF16),
        vm((NCH, 2, 2, RB, CW), F32), vm((NCH, 2, RB, CW), F32), vm((NCH, RB, CW), F32), vm((NCH, RB, CW), F32),
        vm((2, 2, RB, TW), F32), vm((2, RB, TW), F32), vm((RB, TW), F32), vm((RB, TW), F32),
        vm((RB, CB), F32),
        dma((6,)), dma((2,)), dma((3, 2)), dma((3, 2)), dma((5,)), dma((5,)), dma((4, 2)), dma((4, 2)),
        dma((3,)), dma((3,)), dma((3,)), dma((3,)), dma((5, 3)), dma((5, 3)), dma((5,)), dma((5,)), dma((4, 2)),
        dma((NCH + 1,)), dma((NCH + 1,)), dma((NCH + 1,)), dma((NCH + 1,)), dma((4,)), dma((4,)), dma((2,)),
    ]
    hbm = pl.BlockSpec(memory_space=pl.ANY)
    vmem = pl.BlockSpec(memory_space=pltpu.VMEM)
    call = pl.pallas_call(
        kernel,
        out_shape=jax.ShapeDtypeStruct((PB, PB), F32),
        in_specs=[hbm] * 6,
        out_specs=vmem,
        scratch_shapes=scratch,
        compiler_params=pltpu.CompilerParams(
            collective_id=0, has_side_effects=True, vmem_limit_bytes=67_000_000
        ),
        name="sweep",
    )
    def local_sweep(t_blk, d_blk, voovv_blk, vvvvv_blk, oooo, w_blk):
        return call(t_blk, d_blk, voovv_blk, vvvvv_blk, oooo, w_blk.T)

    return jax.shard_map(
        local_sweep,
        mesh=mesh,
        in_specs=(P("row", "col"), P("row", "col"), P("row", "col"), P("row", "col"), P(None, None), P(None, "col")),
        out_specs=P("row", "col"),
        check_vma=False,
    )
```

```python
import functools

import jax
import jax.numpy as jnp
from jax import lax
from jax.experimental import pallas as pl
from jax.experimental.pallas import tpu as pltpu
from jax.sharding import PartitionSpec as P

MESH = pl.DeviceIdType.MESH
scope = jax.named_scope
F32 = jnp.float32
BF16 = jnp.bfloat16

O = 16
V = 144
RB = 64
CB = 5184
AB = 36
PB = 576
CW = 512
NCH = CB // CW
TW = CB - NCH * CW


def stripe(load, m, q):
    first = 1152 * m + V * q
    low = first // 128 * 128
    high = min(-(-(first + V) // 128) * 128, CB)
    return load(low, high)[:, first - low : first - low + V]


def split_cols(load, planes, m):
    for q in range(8 if m < 4 else 4):
        piece = stripe(load, m, q)
        base = RB * (8 * m + q)
        planes[0, base : base + RB, :] = piece[:, 0:128]
        planes[1, base : base + RB, 0:16] = piece[:, 128:144]


def take_j(planes, j, base, rows):
    wide = planes[0, pl.ds(base + j, rows, stride=16), :]
    rest = planes[1, pl.ds(base + j, rows, stride=16), :]
    return [wide, rest[:, 0:16]]


def kernel(
    t_hbm, d_hbm, vo_hbm, vv_hbm, oo_hbm, w_hbm, out_ref,
    t32, d32, vo, wv, trow, tcol, tlad, planes, tm, r3, pp, pt, pr,
    dsnd, drcv, lsnd, lrcv, planes2, prel, xq, xqr, wt, oo, wblk, wf, vbuf, vtail,
    acc, d2r, xsb, xrb, acct, d2t, xst, xrt, r1,
    in_sem, v_sem, row_s, row_r, col_s, col_r, lad_s, lad_r, q_s, q_r,
    d_s, d_r, l_s, l_r, p_s, p_r, fw_s, dd_s, dd_r, xx_s, xx_r, w_s, w_r, f_s,
):
    r = lax.axis_index("row")
    c = lax.axis_index("col")
    x, k = r // 2, r % 2
    z, y = c // 2, c % 2
    r_k, r_x = 2 * x + 1 - k, 2 * (1 - x) + k
    r_d = 2 * (1 - x) + 1 - k
    c_y, c_z = 2 * z + 1 - y, 2 * (1 - z) + y
    c_d = 2 * (1 - z) + 1 - y
    col_peers = (c_y, c_z, c_d)

    def send(src, dst, ss, rs, row, col):
        return pltpu.make_async_remote_copy(
            src_ref=src, dst_ref=dst, send_sem=ss, recv_sem=rs,
            device_id={"row": row, "col": col}, device_id_type=MESH,
        )

    def load_v(n, slot):
        at = pl.multiple_of(n * CW, CW)
        return pltpu.make_async_copy(vv_hbm.at[:, pl.ds(at, CW)], vbuf.at[slot], v_sem.at[slot])

    load_t = pltpu.make_async_copy(t_hbm, t32, in_sem.at[0])
    load_d = pltpu.make_async_copy(d_hbm, d32, in_sem.at[1])
    load_vo = pltpu.make_async_copy(vo_hbm, vo, in_sem.at[2])
    load_w = pltpu.make_async_copy(w_hbm, wv, in_sem.at[3])
    load_tail = pltpu.make_async_copy(vv_hbm.at[:, pl.ds(NCH * CW, TW)], vtail, in_sem.at[4])
    load_oo = pltpu.make_async_copy(oo_hbm.at[pl.ds(pl.multiple_of(r * RB, RB), RB)], oo, in_sem.at[5])
    load_t.start()
    load_w.start()
    load_d.start()
    load_vo.start()
    load_tail.start()
    load_oo.start()
    load_v(0, 0).start()
    load_v(1, 1).start()

    barrier = pltpu.get_barrier_semaphore()
    for rr in range(4):
        for cc in range(4):
            pl.semaphore_signal(barrier, inc=1, device_id={"row": rr, "col": cc}, device_id_type=MESH)

    with scope("wait_t"):
        load_t.wait()
    for m in range(9):
        piece = t32[:, PB * m : PB * m + PB].astype(BF16)
        trow[c, :, PB * m : PB * m + PB] = piece
        tcol[r, :, PB * m : PB * m + PB] = piece
    with scope("barrier"):
        pl.semaphore_wait(barrier, 16)

    half = RB // 2
    halves = (slice(0, half), slice(half, RB))

    def row_copy(way, h):
        block, peer = ((c, c_y), (c, c_z), ((c_z, c_y), (c_y, c_z))[h])[way]
        piece = trow.at[block, halves[h]]
        return send(piece, piece, row_s.at[way, h], row_r.at[way, h], r, peer)

    def row_wait(way, h):
        piece = trow.at[(c_y, c_z, c_d)[way], halves[h]]
        send(piece, piece, row_s.at[way, h], row_r.at[way, h], r, c_y).wait_recv()

    def col_piece(h):
        piece = tcol.at[r, halves[h]]
        return send(piece, piece, col_s.at[h], col_r.at[h], r_x, c)

    col_pair = send(tcol.at[r], tcol.at[r], col_s.at[2], col_r.at[2], r_k, c)
    col_relay = send(tcol.at[r_x], tcol.at[r_x], col_s.at[3], col_r.at[3], r_k, c)

    def lad_copy(slot, h):
        return send(trow.at[slot, halves[h]], tlad.at[r, halves[h]], lad_s.at[slot, h], lad_r.at[r, h], slot, c)

    def dispatch(slot, h):
        @pl.when(slot != r)
        def _():
            lad_copy(slot, h).start()

        @pl.when(slot == r)
        def _():
            tlad[r, halves[h]] = trow[slot, halves[h]]

    def lad_wait(slot, h):
        send(trow.at[0, halves[h]], tlad.at[slot, halves[h]], lad_s.at[slot, h], lad_r.at[slot, h], r, c).wait_recv()

    def lad_forward(slot, h):
        piece = tlad.at[slot, halves[h]]
        return send(piece, piece, fw_s.at[slot, h], lad_r.at[slot, h], r, c_y)

    gives = jnp.logical_and(x != z, k == y)

    def forward(h):
        @pl.when(gives)
        def _():
            for slot in (r_x, r_d):
                with scope("lad_f"):
                    lad_wait(slot, h)
                lad_forward(slot, h).start()

    @pl.when(x == z)
    def _():
        col_piece(0).start()

    for h in range(2):
        row_copy(0, h).start()
        row_copy(1, h).start()
        dispatch(c, h)
    col_pair.start()

    with scope("wait_w"):
        load_w.wait()

    def mixed(slot):
        for m in range(5):
            split_cols(lambda lo, hi: trow[slot, :, lo:hi].astype(F32), planes, m)
        for h in range(2):
            parts = []
            for j in range(8):
                parts += take_j(planes, 8 * h + j, 0, 4 * AB)
            tm[:, 1152 * h : 1152 * h + 1152] = jnp.concatenate(parts, axis=1).astype(BF16)
        at = pl.multiple_of(slot * V, 8)
        r3[pl.ds(at, V), :] = lax.dot_general(
            tm[...], wv[...], (((1,), (1,)), ((), ())), preferred_element_type=F32
        )

    with scope("mixed_c"):
        mixed(c)

    with scope("row10"):
        row_wait(1, 0)
    row_copy(2, 0).start()
    dispatch(c_z, 0)
    with scope("row00"):
        row_wait(0, 0)
    dispatch(c_y, 0)

    load_d.wait()
    for m in range(5):
        split_cols(lambda lo, hi: d32[:, lo:hi], planes, m)
    for cc in range(4):
        parts = []
        for j in range(4):
            parts += take_j(planes, 4 * cc + j, 0, 4 * AB)
        dsnd[cc] = jnp.concatenate(parts, axis=1)
    own_rows = pl.ds(pl.multiple_of(c * V, 8), V)
    drcv[own_rows, :] = dsnd[c]

    with scope("row11"):
        row_wait(1, 1)
    dispatch(c_z, 1)
    with scope("row01"):
        row_wait(0, 1)
    row_copy(2, 1).start()
    dispatch(c_y, 1)
    d_copy = [
        send(dsnd.at[peer], drcv.at[own_rows], d_s.at[q], d_r.at[q], r, peer) for q, peer in enumerate(col_peers)
    ]

    d_copy[1].start()

    @pl.when(x == z)
    def _():
        d_copy[0].start()
        d_copy[2].start()

    forward(0)
    with scope("mixed_c_z"):
        mixed(c_z)
    with scope("row20"):
        row_wait(2, 0)
    with scope("row21"):
        row_wait(2, 1)

    @pl.when(x != z)
    def _():
        dispatch(c_d, 0)
        dispatch(c_d, 1)

    @pl.when(x == z)
    def _():
        col_piece(1).start()

    forward(1)
    with scope("mixed_c_y"):
        mixed(c_y)
    with scope("mixed_c_d"):
        mixed(c_d)
    for b in range(5):
        n = 128 if b < 4 else 64
        planes2[b, :, 0:n] = r3[:, 128 * b : 128 * b + n]
        for i in range(4):
            pp[V * i : V * i + V, 128 * b : 128 * b + n] = planes2[b, pl.ds(i, V, stride=4), :][:, 0:n]
    pt[...] = pp[...].T

    p_copy = send(pt, pr, p_s.at[0], p_r.at[0], c, r)
    p_out, p_on = [], []
    for q in range(4):
        piece = slice(V * q, V * q + V)
        via, to = ((r_x, c), (c, r_x)) if q < 2 else ((r, c_z), (c_z, r))
        p_out.append(send(pt.at[piece], prel.at[q], p_s.at[1 + q], p_r.at[1 + q], *via))
        p_on.append(send(prel.at[q], pr.at[piece], p_s.at[5 + q], p_r.at[5 + q], *to))

    @pl.when(jnp.logical_and(x == z, r != c))
    def _():
        p_copy.start()

    @pl.when(r == c)
    def _():
        pr[...] = pt[...]

    @pl.when(x != z)
    def _():
        for q in (2, 0, 1):
            p_out[q].start()

    q_copy = [send(xq, xqr.at[c], q_s.at[q], q_r.at[q], r, peer) for q, peer in enumerate(col_peers)]

    def hole_x():
        load_vo.wait()
        send(tcol.at[r_k], tcol.at[r_k], col_s.at[2], col_r.at[2], r_k, c).wait_recv()

        @pl.when(jnp.logical_and(x == z, r != c))
        def _():
            send(tcol.at[r_x], tcol.at[r_x], f_s.at[0], col_r.at[4], r_k, c).wait_recv()

        @pl.when(r != c)
        def _():
            send(tcol.at[r_d], tcol.at[r_d], col_s.at[3], col_r.at[3], r_k, c).wait_recv()

        xq[...] = lax.dot_general(
            vo[...], tcol[...].reshape(4 * RB, CB), (((1,), (1,)), ((), ())), preferred_element_type=F32
        )
        xqr[c] = xq[...]
        for copy in q_copy:
            copy.start()

    @pl.when(x != z)
    def _():
        with scope("col"):
            for h in range(2):
                piece = tcol.at[r_x, halves[h]]
                send(piece, piece, col_s.at[h], col_r.at[h], r_x, c).wait_recv()
        col_relay.start()
        with scope("hole_x"):
            hole_x()
        p_out[3].start()

    @pl.when(jnp.logical_not(gives))
    def _():
        for h in range(2):
            for slot in (r_x, r_d):
                with scope("lad"):
                    lad_wait(slot, h)

    for h in range(2):
        with scope("lad_k"):
            lad_wait(r_k, h)

    fwd = (
        send(tlad.at[r_d], tcol.at[r_d], f_s.at[0], col_r.at[4], r_k, c),
        send(tlad.at[r_x], tcol.at[r_x], f_s.at[1], col_r.at[3], r_k, c),
    )

    @pl.when(r == c)
    def _():
        for copy in fwd:
            copy.start()
        tcol[r_d] = tlad[r_d]
        tcol[r_x] = tlad[r_x]

    def w_copy(rr):
        return send(wt.at[RB * rr : RB * rr + RB], wblk.at[r], w_s.at[rr], w_r.at[r], rr, c)

    def hole_w():
        load_oo.wait()
        for q, peer in enumerate(col_peers):
            send(xq, xqr.at[peer], q_s.at[q], q_r.at[q], r, peer).wait_recv()
        x_sum = (xqr[0] + xqr[1]) + (xqr[2] + xqr[3])
        w_hole = oo[...].astype(F32) + 0.5 * x_sum
        wt[...] = w_hole.T.astype(BF16)
        wblk[r] = wt[pl.ds(pl.multiple_of(r * RB, RB), RB), :]
        for rr in range(4):

            @pl.when(r != rr)
            def _():
                w_copy(rr).start()

    def d2_copy(n):
        return send(acc.at[n, 1 - k], d2r.at[n], dd_s.at[n], dd_r.at[n], r_k, c)

    def xx_copy(n):
        return send(xsb.at[n], xrb.at[n], xx_s.at[n], xx_r.at[n], r_x, c)

    d2_tail = send(acct.at[1 - k], d2t, dd_s.at[NCH], dd_r.at[NCH], r_k, c)
    xx_tail = send(xst, xrt, xx_s.at[NCH], xx_r.at[NCH], r_x, c)

    def gather_w():
        with scope("w_in"):
            for rr in range(4):

                @pl.when(r != rr)
                def _():
                    send(wt.at[0:RB], wblk.at[rr], w_s.at[rr], w_r.at[rr], rr, c).wait_recv()

        wf[...] = jnp.concatenate([wblk[rr].astype(F32) for rr in range(4)], axis=1).astype(BF16)

    def close(lo, hi, landed):
        hole = jnp.dot(wf[...], tcol[:, :, lo:hi].reshape(4 * RB, hi - lo), preferred_element_type=F32)
        r1[:, lo:hi] = r1[:, lo:hi] + landed + hole + vo[:, lo:hi].astype(F32)

    def stripe_rows(m):
        return 32 if m < 4 else 16

    def l_copy(m, q):
        rows = stripe_rows(m)
        there = pl.ds(pl.multiple_of(c * V + 32 * m, 8), rows)
        peer = col_peers[q]
        return send(
            lsnd.at[peer, 32 * m : 32 * m + rows], lrcv.at[there], l_s.at[m, q], l_r.at[m, q], r, peer
        )

    def stripe_out(m):
        for n in ((0, 1, 2), (3, 4), (5, 6), (7, 8), (9,))[m]:
            with scope("sum"):
                xx_copy(n).wait_recv()
            close(CW * n, CW * n + CW, xrb[n])
        if m == 4:
            xx_tail.wait_recv()
            close(NCH * CW, CB, xrt[...])
        split_cols(lambda lo, hi: r1[:, lo:hi], planes, m)
        first, rows = 32 * m, stripe_rows(m)
        for cc in range(4):
            parts = []
            for j in range(4):
                parts += take_j(planes, 4 * cc + j, RB * 8 * m, rows)
            lsnd[cc, first : first + rows, :] = jnp.concatenate(parts, axis=1)
        there = pl.ds(pl.multiple_of(c * V + first, 8), rows)
        lrcv[there, :] = lsnd[c, first : first + rows, :]
        for q in range(3):
            l_copy(m, q).start()

    load_tail.wait()
    part = jnp.dot(tlad[...].reshape(4 * RB, CB), vtail[...], preferred_element_type=F32)
    for rr in range(4):
        acct[rr % 2, rr // 2] = part[RB * rr : RB * rr + RB]
    d2_tail.start()

    def second(n):
        with scope("pair"):
            d2_copy(n).wait_recv()
        xsb[n] = acc[n, k, 1 - x] + d2r[n, 1 - x]
        at = pl.multiple_of(n * CW, CW)
        r1[:, pl.ds(at, CW)] = acc[n, k, x] + d2r[n, x]
        xx_copy(n).start()

    def ladder_step(n, carry):
        slot = n % 2
        with scope("wait_v"):
            load_v(n, slot).wait()
        with scope("dot"):
            for h in range(2):
                part = jnp.dot(
                    tlad[...].reshape(4 * RB, CB), vbuf[slot, :, 256 * h : 256 * h + 256], preferred_element_type=F32
                )
                for rr in range(4):
                    acc[n, rr % 2, rr // 2, :, 256 * h : 256 * h + 256] = part[RB * rr : RB * rr + RB]
        d2_copy(n).start()

        @pl.when(n + 2 < NCH)
        def _():
            load_v(n + 2, slot).start()

        @pl.when(n == 0)
        def _():
            d2_tail.wait_recv()
            xst[...] = acct[k, 1 - x] + d2t[1 - x]
            r1[:, NCH * CW : CB] = acct[k, x] + d2t[x]
            xx_tail.start()

        @pl.when(n > 0)
        def _():
            second(n - 1)

        @pl.when(jnp.logical_and(n == 1, x == z))
        def _():
            with scope("hole_x"):
                hole_x()

        @pl.when(jnp.logical_and(n == 1, x != z))
        def _():
            d_copy[0].start()
            d_copy[2].start()

        def relay(*quarters):
            for q in quarters:
                with scope("relay"):
                    p_out[q].wait_recv()
                p_on[q].start()

        @pl.when(jnp.logical_and(n == 3, x == z))
        def _():
            relay(0, 2)

        @pl.when(jnp.logical_and(n == 7, x == z))
        def _():
            relay(1, 3)

        @pl.when(n == jnp.where(x == z, 6, 4))
        def _():
            with scope("hole_w"):
                hole_w()

        @pl.when(jnp.logical_and(n == 9, x != z))
        def _():
            gather_w()
            stripe_out(0)
            stripe_out(1)

        return carry

    lax.fori_loop(0, NCH, ladder_step, 0)
    second(NCH - 1)

    @pl.when(x == z)
    def _():
        gather_w()
        stripe_out(0)
        stripe_out(1)

    for m in range(2, 5):
        stripe_out(m)

    with scope("mirror"):

        @pl.when(jnp.logical_and(x == z, r != c))
        def _():
            p_copy.wait_recv()

        @pl.when(x != z)
        def _():
            for copy in p_on:
                copy.wait_recv()

    pp[...] = pp[...] + pr[...]
    for q, peer in enumerate(col_peers):
        at = pl.ds(pl.multiple_of(peer * V, 8), V)
        with scope("denom"):
            send(dsnd.at[peer], drcv.at[at], d_s.at[q], d_r.at[q], r, peer).wait_recv()
    for m in range(5):
        rows = 32 if m < 4 else 16
        for q, peer in enumerate(col_peers):
            at = pl.ds(pl.multiple_of(peer * V + 32 * m, 8), rows)
            with scope("regroup"):
                send(
                    lsnd.at[peer, 32 * m : 32 * m + rows], lrcv.at[at], l_s.at[m, q], l_r.at[m, q], r, peer
                ).wait_recv()
    for b in range(5):
        n = 128 if b < 4 else 64
        cols = slice(128 * b, 128 * b + n)
        planes[0, 0:PB, 0:n] = lrcv[:, cols]
        planes2[b, :, 0:n] = drcv[:, cols]
        for i in range(4):
            rows = slice(V * i, V * i + V)
            top = planes[0, pl.ds(i, V, stride=4), :][:, 0:n] + pp[rows, cols]
            out_ref[rows, cols] = top / planes2[b, pl.ds(i, V, stride=4), :][:, 0:n]

    for copy in (col_pair, *q_copy, *d_copy, d2_tail, xx_tail):
        copy.wait_send()
    for m in range(5):
        for q in range(3):
            l_copy(m, q).wait_send()
    for way in range(3):
        for h in range(2):
            row_copy(way, h).wait_send()

    @pl.when(x == z)
    def _():
        for h in range(2):
            col_piece(h).wait_send()
        for copy in p_on:
            copy.wait_send()

    @pl.when(jnp.logical_and(x == z, r != c))
    def _():
        p_copy.wait_send()

    @pl.when(x != z)
    def _():
        col_relay.wait_send()
        for copy in p_out:
            copy.wait_send()

    @pl.when(r == c)
    def _():
        for copy in fwd:
            copy.wait_send()

    @pl.when(gives)
    def _():
        for h in range(2):
            for slot in (r_x, r_d):
                lad_forward(slot, h).wait_send()

    for slot in range(4):

        @pl.when(slot != r)
        def _():
            w_copy(slot).wait_send()

        @pl.when(jnp.logical_and(slot != r, jnp.logical_or(slot != c_d, x != z)))
        def _():
            for h in range(2):
                lad_copy(slot, h).wait_send()

    def drain(n, carry):
        d2_copy(n).wait_send()
        xx_copy(n).wait_send()
        return carry

    lax.fori_loop(0, NCH, drain, 0)


def solution(mesh):
    vm = pltpu.VMEM
    dma = pltpu.SemaphoreType.DMA
    scratch = [
        vm((RB, CB), F32), vm((RB, CB), F32), vm((RB, CB), BF16), vm((PB, O * V), BF16),
        vm((4, RB, CB), BF16), vm((4, RB, CB), BF16), vm((4, RB, CB), BF16),
        vm((2, AB * RB, 128), F32), vm((V, O * V), BF16),
        vm((PB, PB), F32), vm((PB, PB), F32), vm((PB, PB), F32), vm((PB, PB), F32),
        vm((4, V, PB), F32), vm((PB, PB), F32), vm((4, V, PB), F32), vm((PB, PB), F32),
        vm((5, PB, 128), F32), vm((4, V, PB), F32),
        vm((RB, O * O), F32), vm((4, RB, O * O), F32), vm((O * O, RB), BF16), vm((RB, O * O), BF16), vm((4, RB, RB), BF16), vm((RB, O * O), BF16),
        vm((2, CB, CW), BF16), vm((CB, TW), BF16),
        vm((NCH, 2, 2, RB, CW), F32), vm((NCH, 2, RB, CW), F32), vm((NCH, RB, CW), F32), vm((NCH, RB, CW), F32),
        vm((2, 2, RB, TW), F32), vm((2, RB, TW), F32), vm((RB, TW), F32), vm((RB, TW), F32),
        vm((RB, CB), F32),
        dma((6,)), dma((2,)), dma((3, 2)), dma((3, 2)), dma((5,)), dma((5,)), dma((4, 2)), dma((4, 2)),
        dma((3,)), dma((3,)), dma((3,)), dma((3,)), dma((5, 3)), dma((5, 3)), dma((9,)), dma((9,)), dma((4, 2)),
        dma((NCH + 1,)), dma((NCH + 1,)), dma((NCH + 1,)), dma((NCH + 1,)), dma((4,)), dma((4,)), dma((2,)),
    ]
    hbm = pl.BlockSpec(memory_space=pl.ANY)
    vmem = pl.BlockSpec(memory_space=pltpu.VMEM)
    call = pl.pallas_call(
        kernel,
        out_shape=jax.ShapeDtypeStruct((PB, PB), F32),
        in_specs=[hbm] * 6,
        out_specs=vmem,
        scratch_shapes=scratch,
        compiler_params=pltpu.CompilerParams(
            collective_id=0, has_side_effects=True, vmem_limit_bytes=67_000_000
        ),
        name="sweep",
    )
    def local_sweep(t_blk, d_blk, voovv_blk, vvvvv_blk, oooo, w_blk):
        return call(t_blk, d_blk, voovv_blk, vvvvv_blk, oooo, w_blk.T)

    return jax.shard_map(
        local_sweep,
        mesh=mesh,
        in_specs=(P("row", "col"), P("row", "col"), P("row", "col"), P("row", "col"), P(None, None), P(None, "col")),
        out_specs=P("row", "col"),
        check_vma=False,
    )
```

```python
import functools

import jax
import jax.numpy as jnp
from jax import lax
from jax.experimental import pallas as pl
from jax.experimental.pallas import tpu as pltpu
from jax.sharding import PartitionSpec as P

MESH = pl.DeviceIdType.MESH
scope = jax.named_scope
F32 = jnp.float32
BF16 = jnp.bfloat16

O = 16
V = 144
RB = 64
CB = 5184
AB = 36
PB = 576
CW = 512
NCH = CB // CW
TW = CB - NCH * CW


def stripe(load, m, q):
    first = 1152 * m + V * q
    low = first // 128 * 128
    high = min(-(-(first + V) // 128) * 128, CB)
    return load(low, high)[:, first - low : first - low + V]


def split_cols(load, planes, m):
    for q in range(8 if m < 4 else 4):
        piece = stripe(load, m, q)
        base = RB * (8 * m + q)
        planes[0, base : base + RB, :] = piece[:, 0:128]
        planes[1, base : base + RB, 0:16] = piece[:, 128:144]


def take_j(planes, j, base, rows):
    wide = planes[0, pl.ds(base + j, rows, stride=16), :]
    rest = planes[1, pl.ds(base + j, rows, stride=16), :]
    return [wide, rest[:, 0:16]]


def kernel(
    t_hbm, d_hbm, vo_hbm, vv_hbm, oo_hbm, w_hbm, out_ref,
    t32, d32, vo, wv, trow, tcol, tlad, planes, tm, r3, pp, pt, pr,
    dsnd, drcv, lsnd, lrcv, planes2, prel, xq, xqr, wt, oo, wblk, wf, vbuf, vtail,
    acc, d2r, xsb, xrb, acct, d2t, xst, xrt, r1,
    in_sem, v_sem, row_s, row_r, col_s, col_r, lad_s, lad_r, q_s, q_r,
    d_s, d_r, l_s, l_r, p_s, p_r, fw_s, dd_s, dd_r, xx_s, xx_r, w_s, w_r, f_s,
):
    r = lax.axis_index("row")
    c = lax.axis_index("col")
    x, k = r // 2, r % 2
    z, y = c // 2, c % 2
    r_k, r_x = 2 * x + 1 - k, 2 * (1 - x) + k
    r_d = 2 * (1 - x) + 1 - k
    c_y, c_z = 2 * z + 1 - y, 2 * (1 - z) + y
    c_d = 2 * (1 - z) + 1 - y
    col_peers = (c_y, c_z, c_d)

    def send(src, dst, ss, rs, row, col):
        return pltpu.make_async_remote_copy(
            src_ref=src, dst_ref=dst, send_sem=ss, recv_sem=rs,
            device_id={"row": row, "col": col}, device_id_type=MESH,
        )

    def load_v(n, slot):
        at = pl.multiple_of(n * CW, CW)
        return pltpu.make_async_copy(vv_hbm.at[:, pl.ds(at, CW)], vbuf.at[slot], v_sem.at[slot])

    load_t = pltpu.make_async_copy(t_hbm, t32, in_sem.at[0])
    load_d = pltpu.make_async_copy(d_hbm, d32, in_sem.at[1])
    load_vo = pltpu.make_async_copy(vo_hbm, vo, in_sem.at[2])
    load_w = pltpu.make_async_copy(w_hbm, wv, in_sem.at[3])
    load_tail = pltpu.make_async_copy(vv_hbm.at[:, pl.ds(NCH * CW, TW)], vtail, in_sem.at[4])
    load_oo = pltpu.make_async_copy(oo_hbm.at[pl.ds(pl.multiple_of(r * RB, RB), RB)], oo, in_sem.at[5])
    load_t.start()
    load_w.start()
    load_d.start()
    load_vo.start()
    load_tail.start()
    load_oo.start()
    load_v(0, 0).start()
    load_v(1, 1).start()

    barrier = pltpu.get_barrier_semaphore()
    for rr in range(4):
        for cc in range(4):
            pl.semaphore_signal(barrier, inc=1, device_id={"row": rr, "col": cc}, device_id_type=MESH)

    with scope("wait_t"):
        load_t.wait()
    for m in range(9):
        piece = t32[:, PB * m : PB * m + PB].astype(BF16)
        trow[c, :, PB * m : PB * m + PB] = piece
        tcol[r, :, PB * m : PB * m + PB] = piece
    with scope("barrier"):
        pl.semaphore_wait(barrier, 16)

    half = RB // 2
    halves = (slice(0, half), slice(half, RB))

    def row_copy(way, h):
        block, peer = ((c, c_y), (c, c_z), ((c_z, c_y), (c_y, c_z))[h])[way]
        piece = trow.at[block, halves[h]]
        return send(piece, piece, row_s.at[way, h], row_r.at[way, h], r, peer)

    def row_wait(way, h):
        piece = trow.at[(c_y, c_z, c_d)[way], halves[h]]
        send(piece, piece, row_s.at[way, h], row_r.at[way, h], r, c_y).wait_recv()

    def col_piece(h):
        piece = tcol.at[r, halves[h]]
        return send(piece, piece, col_s.at[h], col_r.at[h], r_x, c)

    col_pair = send(tcol.at[r], tcol.at[r], col_s.at[2], col_r.at[2], r_k, c)
    col_relay = send(tcol.at[r_x], tcol.at[r_x], col_s.at[3], col_r.at[3], r_k, c)

    def lad_copy(slot, h):
        return send(trow.at[slot, halves[h]], tlad.at[r, halves[h]], lad_s.at[slot, h], lad_r.at[r, h], slot, c)

    def dispatch(slot, h):
        @pl.when(slot != r)
        def _():
            lad_copy(slot, h).start()

        @pl.when(slot == r)
        def _():
            tlad[r, halves[h]] = trow[slot, halves[h]]

    def lad_wait(slot, h):
        send(trow.at[0, halves[h]], tlad.at[slot, halves[h]], lad_s.at[slot, h], lad_r.at[slot, h], r, c).wait_recv()

    def lad_forward(slot, h):
        piece = tlad.at[slot, halves[h]]
        return send(piece, piece, fw_s.at[slot, h], lad_r.at[slot, h], r, c_y)

    gives = jnp.logical_and(x != z, k == y)

    def forward(h):
        @pl.when(gives)
        def _():
            for slot in (r_x, r_d):
                with scope("lad_f"):
                    lad_wait(slot, h)
                lad_forward(slot, h).start()

    @pl.when(x == z)
    def _():
        col_piece(0).start()

    for h in range(2):
        row_copy(0, h).start()
        row_copy(1, h).start()
        dispatch(c, h)
    col_pair.start()

    with scope("wait_w"):
        load_w.wait()

    def mixed(slot):
        for m in range(5):
            split_cols(lambda lo, hi: trow[slot, :, lo:hi].astype(F32), planes, m)
        for h in range(2):
            parts = []
            for j in range(8):
                parts += take_j(planes, 8 * h + j, 0, 4 * AB)
            tm[:, 1152 * h : 1152 * h + 1152] = jnp.concatenate(parts, axis=1).astype(BF16)
        at = pl.multiple_of(slot * V, 8)
        r3[pl.ds(at, V), :] = lax.dot_general(
            tm[...], wv[...], (((1,), (1,)), ((), ())), preferred_element_type=F32
        )

    with scope("mixed_c"):
        mixed(c)

    with scope("row10"):
        row_wait(1, 0)
    row_copy(2, 0).start()
    dispatch(c_z, 0)
    with scope("row00"):
        row_wait(0, 0)
    dispatch(c_y, 0)

    load_d.wait()
    for m in range(5):
        split_cols(lambda lo, hi: d32[:, lo:hi], planes, m)
    for cc in range(4):
        parts = []
        for j in range(4):
            parts += take_j(planes, 4 * cc + j, 0, 4 * AB)
        dsnd[cc] = jnp.concatenate(parts, axis=1)
    own_rows = pl.ds(pl.multiple_of(c * V, 8), V)
    drcv[own_rows, :] = dsnd[c]

    with scope("row11"):
        row_wait(1, 1)
    dispatch(c_z, 1)
    with scope("row01"):
        row_wait(0, 1)
    row_copy(2, 1).start()
    dispatch(c_y, 1)
    d_copy = [
        send(dsnd.at[peer], drcv.at[own_rows], d_s.at[q], d_r.at[q], r, peer) for q, peer in enumerate(col_peers)
    ]

    d_copy[1].start()

    @pl.when(x == z)
    def _():
        d_copy[0].start()
        d_copy[2].start()

    forward(0)
    with scope("mixed_c_z"):
        mixed(c_z)
    with scope("row20"):
        row_wait(2, 0)
    with scope("row21"):
        row_wait(2, 1)

    @pl.when(x != z)
    def _():
        dispatch(c_d, 0)
        dispatch(c_d, 1)

    @pl.when(x == z)
    def _():
        col_piece(1).start()

    forward(1)
    with scope("mixed_c_y"):
        mixed(c_y)
    with scope("mixed_c_d"):
        mixed(c_d)
    for b in range(5):
        n = 128 if b < 4 else 64
        planes2[b, :, 0:n] = r3[:, 128 * b : 128 * b + n]
        for i in range(4):
            pp[V * i : V * i + V, 128 * b : 128 * b + n] = planes2[b, pl.ds(i, V, stride=4), :][:, 0:n]
    pt[...] = pp[...].T

    p_copy = send(pt, pr, p_s.at[0], p_r.at[0], c, r)
    p_out, p_on = [], []
    for q in range(4):
        piece = slice(V * q, V * q + V)
        via, to = ((r_x, c), (c, r_x)) if q < 2 else ((r, c_z), (c_z, r))
        p_out.append(send(pt.at[piece], prel.at[q], p_s.at[1 + q], p_r.at[1 + q], *via))
        p_on.append(send(prel.at[q], pr.at[piece], p_s.at[5 + q], p_r.at[5 + q], *to))

    @pl.when(r == c)
    def _():
        pr[...] = pt[...]

    @pl.when(x != z)
    def _():
        for q in (2, 0, 1):
            p_out[q].start()

    q_copy = [send(xq, xqr.at[c], q_s.at[q], q_r.at[q], r, peer) for q, peer in enumerate(col_peers)]

    def hole_x():
        load_vo.wait()
        send(tcol.at[r_k], tcol.at[r_k], col_s.at[2], col_r.at[2], r_k, c).wait_recv()

        @pl.when(jnp.logical_and(x == z, r != c))
        def _():
            send(tcol.at[r_x], tcol.at[r_x], f_s.at[0], col_r.at[4], r_k, c).wait_recv()

        @pl.when(r != c)
        def _():
            send(tcol.at[r_d], tcol.at[r_d], col_s.at[3], col_r.at[3], r_k, c).wait_recv()

        xq[...] = lax.dot_general(
            vo[...], tcol[...].reshape(4 * RB, CB), (((1,), (1,)), ((), ())), preferred_element_type=F32
        )
        xqr[c] = xq[...]
        for copy in q_copy:
            copy.start()

    @pl.when(x != z)
    def _():
        with scope("col"):
            for h in range(2):
                piece = tcol.at[r_x, halves[h]]
                send(piece, piece, col_s.at[h], col_r.at[h], r_x, c).wait_recv()
        col_relay.start()
        with scope("hole_x"):
            hole_x()
        p_out[3].start()

    @pl.when(jnp.logical_not(gives))
    def _():
        for h in range(2):
            for slot in (r_x, r_d):
                with scope("lad"):
                    lad_wait(slot, h)

    for h in range(2):
        with scope("lad_k"):
            lad_wait(r_k, h)

    fwd = (
        send(tlad.at[r_d], tcol.at[r_d], f_s.at[0], col_r.at[4], r_k, c),
        send(tlad.at[r_x], tcol.at[r_x], f_s.at[1], col_r.at[3], r_k, c),
    )

    @pl.when(r == c)
    def _():
        for copy in fwd:
            copy.start()
        tcol[r_d] = tlad[r_d]
        tcol[r_x] = tlad[r_x]

    def w_copy(rr):
        return send(wt.at[RB * rr : RB * rr + RB], wblk.at[r], w_s.at[rr], w_r.at[r], rr, c)

    def hole_w():
        load_oo.wait()
        for q, peer in enumerate(col_peers):
            send(xq, xqr.at[peer], q_s.at[q], q_r.at[q], r, peer).wait_recv()
        x_sum = (xqr[0] + xqr[1]) + (xqr[2] + xqr[3])
        w_hole = oo[...].astype(F32) + 0.5 * x_sum
        wt[...] = w_hole.T.astype(BF16)
        wblk[r] = wt[pl.ds(pl.multiple_of(r * RB, RB), RB), :]
        for rr in range(4):

            @pl.when(r != rr)
            def _():
                w_copy(rr).start()

    def d2_copy(n):
        return send(acc.at[n, 1 - k], d2r.at[n], dd_s.at[n], dd_r.at[n], r_k, c)

    def xx_copy(n):
        return send(xsb.at[n], xrb.at[n], xx_s.at[n], xx_r.at[n], r_x, c)

    d2_tail = send(acct.at[1 - k], d2t, dd_s.at[NCH], dd_r.at[NCH], r_k, c)
    xx_tail = send(xst, xrt, xx_s.at[NCH], xx_r.at[NCH], r_x, c)

    def gather_w():
        with scope("w_in"):
            for rr in range(4):

                @pl.when(r != rr)
                def _():
                    send(wt.at[0:RB], wblk.at[rr], w_s.at[rr], w_r.at[rr], rr, c).wait_recv()

        wf[...] = jnp.concatenate([wblk[rr].astype(F32) for rr in range(4)], axis=1).astype(BF16)

    def close(lo, hi, landed):
        hole = jnp.dot(wf[...], tcol[:, :, lo:hi].reshape(4 * RB, hi - lo), preferred_element_type=F32)
        r1[:, lo:hi] = r1[:, lo:hi] + landed + hole + vo[:, lo:hi].astype(F32)

    def stripe_rows(m):
        return 32 if m < 4 else 16

    def l_copy(m, q):
        rows = stripe_rows(m)
        there = pl.ds(pl.multiple_of(c * V + 32 * m, 8), rows)
        peer = col_peers[q]
        return send(
            lsnd.at[peer, 32 * m : 32 * m + rows], lrcv.at[there], l_s.at[m, q], l_r.at[m, q], r, peer
        )

    def stripe_out(m):
        for n in ((0, 1, 2), (3, 4), (5, 6), (7, 8), (9,))[m]:
            with scope("sum"):
                xx_copy(n).wait_recv()
            close(CW * n, CW * n + CW, xrb[n])
        if m == 4:
            xx_tail.wait_recv()
            close(NCH * CW, CB, xrt[...])
        split_cols(lambda lo, hi: r1[:, lo:hi], planes, m)
        first, rows = 32 * m, stripe_rows(m)
        for cc in range(4):
            parts = []
            for j in range(4):
                parts += take_j(planes, 4 * cc + j, RB * 8 * m, rows)
            lsnd[cc, first : first + rows, :] = jnp.concatenate(parts, axis=1)
        there = pl.ds(pl.multiple_of(c * V + first, 8), rows)
        lrcv[there, :] = lsnd[c, first : first + rows, :]
        for q in range(3):
            l_copy(m, q).start()

    load_tail.wait()
    part = jnp.dot(tlad[...].reshape(4 * RB, CB), vtail[...], preferred_element_type=F32)
    for rr in range(4):
        acct[rr % 2, rr // 2] = part[RB * rr : RB * rr + RB]
    d2_tail.start()

    def second(n):
        with scope("pair"):
            d2_copy(n).wait_recv()
        xsb[n] = acc[n, k, 1 - x] + d2r[n, 1 - x]
        at = pl.multiple_of(n * CW, CW)
        r1[:, pl.ds(at, CW)] = acc[n, k, x] + d2r[n, x]
        xx_copy(n).start()

    def ladder_step(n, carry):
        slot = n % 2
        with scope("wait_v"):
            load_v(n, slot).wait()
        with scope("dot"):
            for h in range(2):
                part = jnp.dot(
                    tlad[...].reshape(4 * RB, CB), vbuf[slot, :, 256 * h : 256 * h + 256], preferred_element_type=F32
                )
                for rr in range(4):
                    acc[n, rr % 2, rr // 2, :, 256 * h : 256 * h + 256] = part[RB * rr : RB * rr + RB]
        d2_copy(n).start()

        @pl.when(n + 2 < NCH)
        def _():
            load_v(n + 2, slot).start()

        @pl.when(n == 0)
        def _():
            d2_tail.wait_recv()
            xst[...] = acct[k, 1 - x] + d2t[1 - x]
            r1[:, NCH * CW : CB] = acct[k, x] + d2t[x]
            xx_tail.start()

        @pl.when(n > 0)
        def _():
            second(n - 1)

        @pl.when(jnp.logical_and(n == 1, x == z))
        def _():
            with scope("hole_x"):
                hole_x()

            @pl.when(r != c)
            def _():
                p_copy.start()

        @pl.when(jnp.logical_and(n == 1, x != z))
        def _():
            d_copy[0].start()
            d_copy[2].start()

        def relay(*quarters):
            for q in quarters:
                with scope("relay"):
                    p_out[q].wait_recv()
                p_on[q].start()

        @pl.when(jnp.logical_and(n == 3, x == z))
        def _():
            relay(0, 2)

        @pl.when(jnp.logical_and(n == 7, x == z))
        def _():
            relay(1, 3)

        @pl.when(n == jnp.where(x == z, 6, 4))
        def _():
            with scope("hole_w"):
                hole_w()

        @pl.when(jnp.logical_and(n == 9, x != z))
        def _():
            gather_w()
            stripe_out(0)
            stripe_out(1)

        return carry

    lax.fori_loop(0, NCH, ladder_step, 0)
    second(NCH - 1)

    @pl.when(x == z)
    def _():
        gather_w()
        stripe_out(0)
        stripe_out(1)

    for m in range(2, 5):
        stripe_out(m)

    with scope("mirror"):

        @pl.when(jnp.logical_and(x == z, r != c))
        def _():
            p_copy.wait_recv()

        @pl.when(x != z)
        def _():
            for copy in p_on:
                copy.wait_recv()

    pp[...] = pp[...] + pr[...]
    for q, peer in enumerate(col_peers):
        at = pl.ds(pl.multiple_of(peer * V, 8), V)
        with scope("denom"):
            send(dsnd.at[peer], drcv.at[at], d_s.at[q], d_r.at[q], r, peer).wait_recv()
    for b in range(5):
        n = 128 if b < 4 else 64
        cols = slice(128 * b, 128 * b + n)
        planes2[b, :, 0:n] = drcv[:, cols]
        for i in range(4):
            r3[V * i : V * i + V, cols] = planes2[b, pl.ds(i, V, stride=4), :][:, 0:n]

    for m in range(5):
        rows = stripe_rows(m)
        for q, peer in enumerate(col_peers):
            at = pl.ds(pl.multiple_of(peer * V + 32 * m, 8), rows)
            with scope("regroup"):
                send(
                    lsnd.at[peer, 32 * m : 32 * m + rows], lrcv.at[at], l_s.at[m, q], l_r.at[m, q], r, peer
                ).wait_recv()
        for cc in range(4):
            for b in range(5):
                n = 128 if b < 4 else 64
                cols = slice(128 * b, 128 * b + n)
                base = V * cc + 32 * m
                planes2[b, base : base + rows, 0:n] = lrcv[base : base + rows, cols]
                for i in range(4):
                    first = V * i + AB * cc + 8 * m
                    there = slice(first, first + rows // 4)
                    part = planes2[b, pl.ds(base + i, rows // 4, stride=4), :][:, 0:n]
                    out_ref[there, cols] = (part + pp[there, cols]) / r3[there, cols]

    for copy in (col_pair, *q_copy, *d_copy, d2_tail, xx_tail):
        copy.wait_send()
    for m in range(5):
        for q in range(3):
            l_copy(m, q).wait_send()
    for way in range(3):
        for h in range(2):
            row_copy(way, h).wait_send()

    @pl.when(x == z)
    def _():
        for h in range(2):
            col_piece(h).wait_send()
        for copy in p_on:
            copy.wait_send()

    @pl.when(jnp.logical_and(x == z, r != c))
    def _():
        p_copy.wait_send()

    @pl.when(x != z)
    def _():
        col_relay.wait_send()
        for copy in p_out:
            copy.wait_send()

    @pl.when(r == c)
    def _():
        for copy in fwd:
            copy.wait_send()

    @pl.when(gives)
    def _():
        for h in range(2):
            for slot in (r_x, r_d):
                lad_forward(slot, h).wait_send()

    for slot in range(4):

        @pl.when(slot != r)
        def _():
            w_copy(slot).wait_send()

        @pl.when(jnp.logical_and(slot != r, jnp.logical_or(slot != c_d, x != z)))
        def _():
            for h in range(2):
                lad_copy(slot, h).wait_send()

    def drain(n, carry):
        d2_copy(n).wait_send()
        xx_copy(n).wait_send()
        return carry

    lax.fori_loop(0, NCH, drain, 0)


def solution(mesh):
    vm = pltpu.VMEM
    dma = pltpu.SemaphoreType.DMA
    scratch = [
        vm((RB, CB), F32), vm((RB, CB), F32), vm((RB, CB), BF16), vm((PB, O * V), BF16),
        vm((4, RB, CB), BF16), vm((4, RB, CB), BF16), vm((4, RB, CB), BF16),
        vm((2, AB * RB, 128), F32), vm((V, O * V), BF16),
        vm((PB, PB), F32), vm((PB, PB), F32), vm((PB, PB), F32), vm((PB, PB), F32),
        vm((4, V, PB), F32), vm((PB, PB), F32), vm((4, V, PB), F32), vm((PB, PB), F32),
        vm((5, PB, 128), F32), vm((4, V, PB), F32),
        vm((RB, O * O), F32), vm((4, RB, O * O), F32), vm((O * O, RB), BF16), vm((RB, O * O), BF16), vm((4, RB, RB), BF16), vm((RB, O * O), BF16),
        vm((2, CB, CW), BF16), vm((CB, TW), BF16),
        vm((NCH, 2, 2, RB, CW), F32), vm((NCH, 2, RB, CW), F32), vm((NCH, RB, CW), F32), vm((NCH, RB, CW), F32),
        vm((2, 2, RB, TW), F32), vm((2, RB, TW), F32), vm((RB, TW), F32), vm((RB, TW), F32),
        vm((RB, CB), F32),
        dma((6,)), dma((2,)), dma((3, 2)), dma((3, 2)), dma((5,)), dma((5,)), dma((4, 2)), dma((4, 2)),
        dma((3,)), dma((3,)), dma((3,)), dma((3,)), dma((5, 3)), dma((5, 3)), dma((9,)), dma((9,)), dma((4, 2)),
        dma((NCH + 1,)), dma((NCH + 1,)), dma((NCH + 1,)), dma((NCH + 1,)), dma((4,)), dma((4,)), dma((2,)),
    ]
    hbm = pl.BlockSpec(memory_space=pl.ANY)
    vmem = pl.BlockSpec(memory_space=pltpu.VMEM)
    call = pl.pallas_call(
        kernel,
        out_shape=jax.ShapeDtypeStruct((PB, PB), F32),
        in_specs=[hbm] * 6,
        out_specs=vmem,
        scratch_shapes=scratch,
        compiler_params=pltpu.CompilerParams(
            collective_id=0, has_side_effects=True, vmem_limit_bytes=67_000_000
        ),
        name="sweep",
    )
    def local_sweep(t_blk, d_blk, voovv_blk, vvvvv_blk, oooo, w_blk):
        return call(t_blk, d_blk, voovv_blk, vvvvv_blk, oooo, w_blk.T)

    return jax.shard_map(
        local_sweep,
        mesh=mesh,
        in_specs=(P("row", "col"), P("row", "col"), P("row", "col"), P("row", "col"), P(None, None), P(None, "col")),
        out_specs=P("row", "col"),
        check_vma=False,
    )
```

```python
import functools

import jax
import jax.numpy as jnp
from jax import lax
from jax.experimental import pallas as pl
from jax.experimental.pallas import tpu as pltpu
from jax.sharding import PartitionSpec as P

MESH = pl.DeviceIdType.MESH
scope = jax.named_scope
F32 = jnp.float32
BF16 = jnp.bfloat16

O = 16
V = 144
RB = 64
CB = 5184
AB = 36
PQ = 648
PB = 576
CW = 512
NCH = CB // CW
TW = CB - NCH * CW


def stripe(load, m, q):
    first = 1152 * m + V * q
    low = first // 128 * 128
    high = min(-(-(first + V) // 128) * 128, CB)
    return load(low, high)[:, first - low : first - low + V]


def split_cols(load, planes, m):
    for q in range(8 if m < 4 else 4):
        piece = stripe(load, m, q)
        base = RB * (8 * m + q)
        planes[0, base : base + RB, :] = piece[:, 0:128]
        planes[1, base : base + RB, 0:16] = piece[:, 128:144]


def take_j(planes, j, base, rows):
    wide = planes[0, pl.ds(base + j, rows, stride=16), :]
    rest = planes[1, pl.ds(base + j, rows, stride=16), :]
    return [wide, rest[:, 0:16]]


def pack(put, rows, wide):
    for b in range(4):
        put(rows * b, rows, slice(0, 128), wide[:, 128 * b : 128 * b + 128])
    put(4 * rows, rows // 2, slice(0, 64), wide[: rows // 2, 512:576])
    put(4 * rows, rows // 2, slice(64, 128), wide[rows // 2 :, 512:576])


def kernel(
    t_hbm, d_hbm, vo_hbm, vv_hbm, oo_hbm, w_hbm, out_ref,
    t32, d32, vo, wv, trow, tcol, tlad, planes, tm, r3, pp, pt, pr,
    dsnd, drcv, lsnd, lrcv, planes2, prel, xq, xqr, wt, oo, wblk, wf, vbuf, vtail,
    acc, d2r, xsb, xrb, acct, d2t, xst, xrt, r1,
    in_sem, v_sem, row_s, row_r, col_s, col_r, lad_s, lad_r, q_s, q_r,
    d_s, d_r, l_s, l_r, p_s, p_r, fw_s, dd_s, dd_r, xx_s, xx_r, w_s, w_r, f_s,
):
    r = lax.axis_index("row")
    c = lax.axis_index("col")
    x, k = r // 2, r % 2
    z, y = c // 2, c % 2
    r_k, r_x = 2 * x + 1 - k, 2 * (1 - x) + k
    r_d = 2 * (1 - x) + 1 - k
    c_y, c_z = 2 * z + 1 - y, 2 * (1 - z) + y
    c_d = 2 * (1 - z) + 1 - y
    col_peers = (c_y, c_z, c_d)

    def send(src, dst, ss, rs, row, col):
        return pltpu.make_async_remote_copy(
            src_ref=src, dst_ref=dst, send_sem=ss, recv_sem=rs,
            device_id={"row": row, "col": col}, device_id_type=MESH,
        )

    def load_v(n, slot):
        at = pl.multiple_of(n * CW, CW)
        return pltpu.make_async_copy(vv_hbm.at[:, pl.ds(at, CW)], vbuf.at[slot], v_sem.at[slot])

    load_t = pltpu.make_async_copy(t_hbm, t32, in_sem.at[0])
    load_d = pltpu.make_async_copy(d_hbm, d32, in_sem.at[1])
    load_vo = pltpu.make_async_copy(vo_hbm, vo, in_sem.at[2])
    load_w = pltpu.make_async_copy(w_hbm, wv, in_sem.at[3])
    load_tail = pltpu.make_async_copy(vv_hbm.at[:, pl.ds(NCH * CW, TW)], vtail, in_sem.at[4])
    load_oo = pltpu.make_async_copy(oo_hbm.at[pl.ds(pl.multiple_of(r * RB, RB), RB)], oo, in_sem.at[5])
    load_t.start()
    load_w.start()
    load_d.start()
    load_vo.start()
    load_tail.start()
    load_oo.start()
    load_v(0, 0).start()
    load_v(1, 1).start()

    barrier = pltpu.get_barrier_semaphore()
    for rr in range(4):
        for cc in range(4):
            pl.semaphore_signal(barrier, inc=1, device_id={"row": rr, "col": cc}, device_id_type=MESH)

    with scope("wait_t"):
        load_t.wait()
    for m in range(9):
        piece = t32[:, PB * m : PB * m + PB].astype(BF16)
        trow[c, :, PB * m : PB * m + PB] = piece
        tcol[r, :, PB * m : PB * m + PB] = piece
    with scope("barrier"):
        pl.semaphore_wait(barrier, 16)

    half = RB // 2
    halves = (slice(0, half), slice(half, RB))

    def row_copy(way, h):
        block, peer = ((c, c_y), (c, c_z), ((c_z, c_y), (c_y, c_z))[h])[way]
        piece = trow.at[block, halves[h]]
        return send(piece, piece, row_s.at[way, h], row_r.at[way, h], r, peer)

    def row_wait(way, h):
        piece = trow.at[(c_y, c_z, c_d)[way], halves[h]]
        send(piece, piece, row_s.at[way, h], row_r.at[way, h], r, c_y).wait_recv()

    def col_piece(h):
        piece = tcol.at[r, halves[h]]
        return send(piece, piece, col_s.at[h], col_r.at[h], r_x, c)

    col_pair = send(tcol.at[r], tcol.at[r], col_s.at[2], col_r.at[2], r_k, c)
    col_relay = send(tcol.at[r_x], tcol.at[r_x], col_s.at[3], col_r.at[3], r_k, c)

    def lad_copy(slot, h):
        return send(trow.at[slot, halves[h]], tlad.at[r, halves[h]], lad_s.at[slot, h], lad_r.at[r, h], slot, c)

    def dispatch(slot, h):
        @pl.when(slot != r)
        def _():
            lad_copy(slot, h).start()

        @pl.when(slot == r)
        def _():
            tlad[r, halves[h]] = trow[slot, halves[h]]

    def lad_wait(slot, h):
        send(trow.at[0, halves[h]], tlad.at[slot, halves[h]], lad_s.at[slot, h], lad_r.at[slot, h], r, c).wait_recv()

    def lad_forward(slot, h):
        piece = tlad.at[slot, halves[h]]
        return send(piece, piece, fw_s.at[slot, h], lad_r.at[slot, h], r, c_y)

    gives = jnp.logical_and(x != z, k == y)

    def forward(h):
        @pl.when(gives)
        def _():
            for slot in (r_x, r_d):
                with scope("lad_f"):
                    lad_wait(slot, h)
                lad_forward(slot, h).start()

    @pl.when(x == z)
    def _():
        col_piece(0).start()

    for h in range(2):
        row_copy(0, h).start()
        row_copy(1, h).start()
        dispatch(c, h)
    col_pair.start()

    with scope("wait_w"):
        load_w.wait()

    def mixed(slot):
        for m in range(5):
            split_cols(lambda lo, hi: trow[slot, :, lo:hi].astype(F32), planes, m)
        for h in range(2):
            parts = []
            for j in range(8):
                parts += take_j(planes, 8 * h + j, 0, 4 * AB)
            tm[:, 1152 * h : 1152 * h + 1152] = jnp.concatenate(parts, axis=1).astype(BF16)
        at = pl.multiple_of(slot * V, 8)
        r3[pl.ds(at, V), :] = lax.dot_general(
            tm[...], wv[...], (((1,), (1,)), ((), ())), preferred_element_type=F32
        )

    with scope("mixed_c"):
        mixed(c)

    with scope("row10"):
        row_wait(1, 0)
    row_copy(2, 0).start()
    dispatch(c_z, 0)
    with scope("row00"):
        row_wait(0, 0)
    dispatch(c_y, 0)

    load_d.wait()
    for m in range(5):
        split_cols(lambda lo, hi: d32[:, lo:hi], planes, m)
    for cc in range(4):
        parts = []
        for j in range(4):
            parts += take_j(planes, 4 * cc + j, 0, 4 * AB)
        def put_d(at, rows, lanes, value):
            dsnd[cc, at : at + rows, lanes] = value

        pack(put_d, V, jnp.concatenate(parts, axis=1))
    drcv[c] = dsnd[c]

    with scope("row11"):
        row_wait(1, 1)
    dispatch(c_z, 1)
    with scope("row01"):
        row_wait(0, 1)
    row_copy(2, 1).start()
    dispatch(c_y, 1)
    d_copy = [
        send(dsnd.at[peer], drcv.at[c], d_s.at[q], d_r.at[q], r, peer) for q, peer in enumerate(col_peers)
    ]

    d_copy[1].start()

    @pl.when(x == z)
    def _():
        d_copy[0].start()
        d_copy[2].start()

    forward(0)
    with scope("mixed_c_z"):
        mixed(c_z)
    with scope("row20"):
        row_wait(2, 0)
    with scope("row21"):
        row_wait(2, 1)

    @pl.when(x != z)
    def _():
        dispatch(c_d, 0)
        dispatch(c_d, 1)

    @pl.when(x == z)
    def _():
        col_piece(1).start()

    forward(1)
    with scope("mixed_c_y"):
        mixed(c_y)
    with scope("mixed_c_d"):
        mixed(c_d)
    for b in range(5):
        n = 128 if b < 4 else 64
        planes2[b, :, 0:n] = r3[:, 128 * b : 128 * b + n]
        for i in range(4):
            pp[V * i : V * i + V, 128 * b : 128 * b + n] = planes2[b, pl.ds(i, V, stride=4), :][:, 0:n]

    def put_p(at, count, lanes, value):
        pt[at : at + count, lanes] = value

    pack(put_p, PB, pp[...].T)

    p_copy = send(pt, pr, p_s.at[0], p_r.at[0], c, r)
    p_out, p_on = [], []
    for q in range(4):
        piece = slice(PQ * q, PQ * q + PQ)
        via, to = ((r_x, c), (c, r_x)) if q < 2 else ((r, c_z), (c_z, r))
        p_out.append(send(pt.at[piece], prel.at[q], p_s.at[1 + q], p_r.at[1 + q], *via))
        p_on.append(send(prel.at[q], pr.at[piece], p_s.at[5 + q], p_r.at[5 + q], *to))

    @pl.when(r == c)
    def _():
        pr[...] = pt[...]

    @pl.when(x != z)
    def _():
        for q in (2, 0, 1):
            p_out[q].start()

    q_copy = [send(xq, xqr.at[c], q_s.at[q], q_r.at[q], r, peer) for q, peer in enumerate(col_peers)]

    def hole_x():
        load_vo.wait()
        send(tcol.at[r_k], tcol.at[r_k], col_s.at[2], col_r.at[2], r_k, c).wait_recv()

        @pl.when(jnp.logical_and(x == z, r != c))
        def _():
            send(tcol.at[r_x], tcol.at[r_x], f_s.at[0], col_r.at[4], r_k, c).wait_recv()

        @pl.when(r != c)
        def _():
            send(tcol.at[r_d], tcol.at[r_d], col_s.at[3], col_r.at[3], r_k, c).wait_recv()

        xq[...] = lax.dot_general(
            vo[...], tcol[...].reshape(4 * RB, CB), (((1,), (1,)), ((), ())), preferred_element_type=F32
        )
        xqr[c] = xq[...]
        for copy in q_copy:
            copy.start()

    @pl.when(x != z)
    def _():
        with scope("col"):
            for h in range(2):
                piece = tcol.at[r_x, halves[h]]
                send(piece, piece, col_s.at[h], col_r.at[h], r_x, c).wait_recv()
        col_relay.start()
        with scope("hole_x"):
            hole_x()
        p_out[3].start()

    @pl.when(jnp.logical_not(gives))
    def _():
        for h in range(2):
            for slot in (r_x, r_d):
                with scope("lad"):
                    lad_wait(slot, h)

    for h in range(2):
        with scope("lad_k"):
            lad_wait(r_k, h)

    fwd = (
        send(tlad.at[r_d], tcol.at[r_d], f_s.at[0], col_r.at[4], r_k, c),
        send(tlad.at[r_x], tcol.at[r_x], f_s.at[1], col_r.at[3], r_k, c),
    )

    @pl.when(r == c)
    def _():
        for copy in fwd:
            copy.start()
        tcol[r_d] = tlad[r_d]
        tcol[r_x] = tlad[r_x]

    @pl.when(x == z)
    def _():
        with scope("hole_x"):
            hole_x()

        @pl.when(r != c)
        def _():
            p_copy.start()

    def w_copy(rr):
        return send(wt.at[RB * rr : RB * rr + RB], wblk.at[r], w_s.at[rr], w_r.at[r], rr, c)

    def hole_w():
        load_oo.wait()
        for q, peer in enumerate(col_peers):
            send(xq, xqr.at[peer], q_s.at[q], q_r.at[q], r, peer).wait_recv()
        x_sum = (xqr[0] + xqr[1]) + (xqr[2] + xqr[3])
        w_hole = oo[...].astype(F32) + 0.5 * x_sum
        wt[...] = w_hole.T.astype(BF16)
        wblk[r] = wt[pl.ds(pl.multiple_of(r * RB, RB), RB), :]
        for rr in range(4):

            @pl.when(r != rr)
            def _():
                w_copy(rr).start()

    def d2_copy(n):
        return send(acc.at[n, 1 - k], d2r.at[n], dd_s.at[n], dd_r.at[n], r_k, c)

    def xx_copy(n):
        return send(xsb.at[n], xrb.at[n], xx_s.at[n], xx_r.at[n], r_x, c)

    d2_tail = send(acct.at[1 - k], d2t, dd_s.at[NCH], dd_r.at[NCH], r_k, c)
    xx_tail = send(xst, xrt, xx_s.at[NCH], xx_r.at[NCH], r_x, c)

    def gather_w():
        with scope("w_in"):
            for rr in range(4):

                @pl.when(r != rr)
                def _():
                    send(wt.at[0:RB], wblk.at[rr], w_s.at[rr], w_r.at[rr], rr, c).wait_recv()

        wf[...] = jnp.concatenate([wblk[rr].astype(F32) for rr in range(4)], axis=1).astype(BF16)

    def close(lo, hi, landed):
        hole = jnp.dot(wf[...], tcol[:, :, lo:hi].reshape(4 * RB, hi - lo), preferred_element_type=F32)
        r1[:, lo:hi] = r1[:, lo:hi] + landed + hole + vo[:, lo:hi].astype(F32)

    def stripe_rows(m):
        return 32 if m < 4 else 16

    def l_copy(m, q):
        there = pl.ds(V * m, stripe_rows(m) * 9 // 2)
        peer = col_peers[q]
        return send(lsnd.at[peer, there], lrcv.at[c, there], l_s.at[m, q], l_r.at[m, q], r, peer)

    def stripe_out(m):
        for n in ((0, 1, 2), (3, 4), (5, 6), (7, 8), (9,))[m]:
            with scope("sum"):
                xx_copy(n).wait_recv()
            close(CW * n, CW * n + CW, xrb[n])
        if m == 4:
            xx_tail.wait_recv()
            close(NCH * CW, CB, xrt[...])
        split_cols(lambda lo, hi: r1[:, lo:hi], planes, m)
        rows = stripe_rows(m)
        for cc in range(4):
            parts = []
            for j in range(4):
                parts += take_j(planes, 4 * cc + j, RB * 8 * m, rows)

            def put_l(at, count, lanes, value):
                lsnd[cc, V * m + at : V * m + at + count, lanes] = value

            pack(put_l, rows, jnp.concatenate(parts, axis=1))
        there = slice(V * m, V * m + rows * 9 // 2)
        lrcv[c, there, :] = lsnd[c, there, :]
        for q in range(3):
            l_copy(m, q).start()

    load_tail.wait()
    part = jnp.dot(tlad[...].reshape(4 * RB, CB), vtail[...], preferred_element_type=F32)
    for rr in range(4):
        acct[rr % 2, rr // 2] = part[RB * rr : RB * rr + RB]
    d2_tail.start()

    def second(n):
        with scope("pair"):
            d2_copy(n).wait_recv()
        xsb[n] = acc[n, k, 1 - x] + d2r[n, 1 - x]
        at = pl.multiple_of(n * CW, CW)
        r1[:, pl.ds(at, CW)] = acc[n, k, x] + d2r[n, x]
        xx_copy(n).start()

    def relay(*quarters):
        for q in quarters:
            with scope("relay"):
                p_out[q].wait_recv()
            p_on[q].start()

    def ladder_step(n, carry):
        slot = n % 2
        with scope("wait_v"):
            load_v(n, slot).wait()
        with scope("dot"):
            for h in range(2):
                part = jnp.dot(
                    tlad[...].reshape(4 * RB, CB), vbuf[slot, :, 256 * h : 256 * h + 256], preferred_element_type=F32
                )
                for rr in range(4):
                    acc[n, rr % 2, rr // 2, :, 256 * h : 256 * h + 256] = part[RB * rr : RB * rr + RB]
        d2_copy(n).start()

        @pl.when(n + 2 < NCH)
        def _():
            load_v(n + 2, slot).start()

        @pl.when(n == 0)
        def _():
            d2_tail.wait_recv()
            xst[...] = acct[k, 1 - x] + d2t[1 - x]
            r1[:, NCH * CW : CB] = acct[k, x] + d2t[x]
            xx_tail.start()

        @pl.when(n > 0)
        def _():
            second(n - 1)

        @pl.when(jnp.logical_and(n == 1, x != z))
        def _():
            d_copy[0].start()
            d_copy[2].start()

        @pl.when(jnp.logical_and(n == 3, x == z))
        def _():
            relay(0)

        @pl.when(jnp.logical_and(n == 5, x == z))
        def _():
            relay(1)

        @pl.when(n == jnp.where(x == z, 4, 2))
        def _():
            with scope("hole_w"):
                hole_w()

        @pl.when(jnp.logical_and(n == 9, x != z))
        def _():
            gather_w()
            stripe_out(0)
            stripe_out(1)

        return carry

    lax.fori_loop(0, NCH, ladder_step, 0)
    second(NCH - 1)

    @pl.when(x == z)
    def _():
        relay(2, 3)
        gather_w()
        stripe_out(0)
        stripe_out(1)

    for m in range(2, 5):
        stripe_out(m)

    with scope("mirror"):

        @pl.when(jnp.logical_and(x == z, r != c))
        def _():
            p_copy.wait_recv()

        @pl.when(x != z)
        def _():
            for copy in p_on:
                copy.wait_recv()

    for b in range(4):
        pp[:, 128 * b : 128 * b + 128] += pr[PB * b : PB * b + PB, :]
    pp[0 : PB // 2, 512:576] += pr[4 * PB :, 0:64]
    pp[PB // 2 :, 512:576] += pr[4 * PB :, 64:128]
    for q, peer in enumerate(col_peers):
        with scope("denom"):
            send(dsnd.at[peer], drcv.at[peer], d_s.at[q], d_r.at[q], r, peer).wait_recv()
    for cc in range(4):
        for i in range(4):
            first = V * i + AB * cc
            for b in range(4):
                r3[first : first + AB, 128 * b : 128 * b + 128] = drcv[cc, pl.ds(V * b + i, AB, stride=4), :]
            ends = drcv[cc, pl.ds(4 * V + i, AB // 2, stride=4), :]
            r3[first : first + AB // 2, 512:576] = ends[:, 0:64]
            r3[first + AB // 2 : first + AB, 512:576] = ends[:, 64:128]

    for m in range(5):
        rows = stripe_rows(m)
        for q, peer in enumerate(col_peers):
            there = pl.ds(V * m, rows * 9 // 2)
            with scope("regroup"):
                send(
                    lsnd.at[peer, there], lrcv.at[peer, there], l_s.at[m, q], l_r.at[m, q], r, peer
                ).wait_recv()
        for cc in range(4):
            for i in range(4):
                first = V * i + AB * cc + 8 * m
                n = rows // 4

                def finish(at, count, lanes, value):
                    there = slice(at, at + count)
                    out_ref[there, lanes] = (value + pp[there, lanes]) / r3[there, lanes]

                for b in range(4):
                    part = lrcv[cc, pl.ds(V * m + rows * b + i, n, stride=4), :]
                    finish(first, n, slice(128 * b, 128 * b + 128), part)
                ends = lrcv[cc, pl.ds(V * m + 4 * rows + i, n // 2, stride=4), :]
                finish(first, n // 2, slice(512, 576), ends[:, 0:64])
                finish(first + n // 2, n // 2, slice(512, 576), ends[:, 64:128])

    for copy in (col_pair, *q_copy, *d_copy, d2_tail, xx_tail):
        copy.wait_send()
    for m in range(5):
        for q in range(3):
            l_copy(m, q).wait_send()
    for way in range(3):
        for h in range(2):
            row_copy(way, h).wait_send()

    @pl.when(x == z)
    def _():
        for h in range(2):
            col_piece(h).wait_send()
        for copy in p_on:
            copy.wait_send()

    @pl.when(jnp.logical_and(x == z, r != c))
    def _():
        p_copy.wait_send()

    @pl.when(x != z)
    def _():
        col_relay.wait_send()
        for copy in p_out:
            copy.wait_send()

    @pl.when(r == c)
    def _():
        for copy in fwd:
            copy.wait_send()

    @pl.when(gives)
    def _():
        for h in range(2):
            for slot in (r_x, r_d):
                lad_forward(slot, h).wait_send()

    for slot in range(4):

        @pl.when(slot != r)
        def _():
            w_copy(slot).wait_send()

        @pl.when(jnp.logical_and(slot != r, jnp.logical_or(slot != c_d, x != z)))
        def _():
            for h in range(2):
                lad_copy(slot, h).wait_send()

    def drain(n, carry):
        d2_copy(n).wait_send()
        xx_copy(n).wait_send()
        return carry

    lax.fori_loop(0, NCH, drain, 0)


def solution(mesh):
    vm = pltpu.VMEM
    dma = pltpu.SemaphoreType.DMA
    scratch = [
        vm((RB, CB), F32), vm((RB, CB), F32), vm((RB, CB), BF16), vm((PB, O * V), BF16),
        vm((4, RB, CB), BF16), vm((4, RB, CB), BF16), vm((4, RB, CB), BF16),
        vm((2, AB * RB, 128), F32), vm((V, O * V), BF16),
        vm((PB, PB), F32), vm((PB, PB), F32), vm((4 * PQ, 128), F32), vm((4 * PQ, 128), F32),
        vm((4, PQ, 128), F32), vm((4, PQ, 128), F32), vm((4, PQ, 128), F32), vm((4, PQ, 128), F32),
        vm((5, PB, 128), F32), vm((4, PQ, 128), F32),
        vm((RB, O * O), F32), vm((4, RB, O * O), F32), vm((O * O, RB), BF16), vm((RB, O * O), BF16), vm((4, RB, RB), BF16), vm((RB, O * O), BF16),
        vm((2, CB, CW), BF16), vm((CB, TW), BF16),
        vm((NCH, 2, 2, RB, CW), F32), vm((NCH, 2, RB, CW), F32), vm((NCH, RB, CW), F32), vm((NCH, RB, CW), F32),
        vm((2, 2, RB, TW), F32), vm((2, RB, TW), F32), vm((RB, TW), F32), vm((RB, TW), F32),
        vm((RB, CB), F32),
        dma((6,)), dma((2,)), dma((3, 2)), dma((3, 2)), dma((5,)), dma((5,)), dma((4, 2)), dma((4, 2)),
        dma((3,)), dma((3,)), dma((3,)), dma((3,)), dma((5, 3)), dma((5, 3)), dma((9,)), dma((9,)), dma((4, 2)),
        dma((NCH + 1,)), dma((NCH + 1,)), dma((NCH + 1,)), dma((NCH + 1,)), dma((4,)), dma((4,)), dma((2,)),
    ]
    hbm = pl.BlockSpec(memory_space=pl.ANY)
    vmem = pl.BlockSpec(memory_space=pltpu.VMEM)
    call = pl.pallas_call(
        kernel,
        out_shape=jax.ShapeDtypeStruct((PB, PB), F32),
        in_specs=[hbm] * 6,
        out_specs=vmem,
        scratch_shapes=scratch,
        compiler_params=pltpu.CompilerParams(
            collective_id=0, has_side_effects=True, vmem_limit_bytes=67_000_000
        ),
        name="sweep",
    )
    def local_sweep(t_blk, d_blk, voovv_blk, vvvvv_blk, oooo, w_blk):
        return call(t_blk, d_blk, voovv_blk, vvvvv_blk, oooo, w_blk.T)

    return jax.shard_map(
        local_sweep,
        mesh=mesh,
        in_specs=(P("row", "col"), P("row", "col"), P("row", "col"), P("row", "col"), P(None, None), P(None, "col")),
        out_specs=P("row", "col"),
        check_vma=False,
    )
```

```python
import functools

import jax
import jax.numpy as jnp
from jax import lax
from jax.experimental import pallas as pl
from jax.experimental.pallas import tpu as pltpu
from jax.sharding import PartitionSpec as P

MESH = pl.DeviceIdType.MESH
scope = jax.named_scope
F32 = jnp.float32
BF16 = jnp.bfloat16

O = 16
V = 144
RB = 64
CB = 5184
AB = 36
PQ = 648
PB = 576
CW = 512
NCH = CB // CW
TW = CB - NCH * CW


def stripe(load, m, q):
    first = 1152 * m + V * q
    low = first // 128 * 128
    high = min(-(-(first + V) // 128) * 128, CB)
    return load(low, high)[:, first - low : first - low + V]


def split_cols(load, planes, m):
    for q in range(8 if m < 4 else 4):
        piece = stripe(load, m, q)
        base = RB * (8 * m + q)
        planes[0, base : base + RB, :] = piece[:, 0:128]
        planes[1, base : base + RB, 0:16] = piece[:, 128:144]


def take_j(planes, j, base, rows):
    wide = planes[0, pl.ds(base + j, rows, stride=16), :]
    rest = planes[1, pl.ds(base + j, rows, stride=16), :]
    return [wide, rest[:, 0:16]]


def pack(put, rows, wide):
    for b in range(4):
        put(rows * b, rows, slice(0, 128), wide[:, 128 * b : 128 * b + 128])
    put(4 * rows, rows // 2, slice(0, 64), wide[: rows // 2, 512:576])
    put(4 * rows, rows // 2, slice(64, 128), wide[rows // 2 :, 512:576])


def kernel(
    t_hbm, d_hbm, vo_hbm, vv_hbm, oo_hbm, w_hbm, out_ref,
    t32, d32, vo, wv, trow, tcol, tlad, planes, tm, r3, pp, pt, pr,
    dsnd, drcv, lsnd, lrcv, prel, xq, xqr, wt, oo, wblk, wf, vbuf, vtail,
    acc, d2r, xsb, xrb, acct, d2t, xst, xrt, r1,
    in_sem, v_sem, row_s, row_r, col_s, col_r, lad_s, lad_r, q_s, q_r,
    d_s, d_r, l_s, l_r, p_s, p_r, fw_s, dd_s, dd_r, xx_s, xx_r, w_s, w_r, f_s,
):
    r = lax.axis_index("row")
    c = lax.axis_index("col")
    x, k = r // 2, r % 2
    z, y = c // 2, c % 2
    r_k, r_x = 2 * x + 1 - k, 2 * (1 - x) + k
    r_d = 2 * (1 - x) + 1 - k
    c_y, c_z = 2 * z + 1 - y, 2 * (1 - z) + y
    c_d = 2 * (1 - z) + 1 - y
    col_peers = (c_y, c_z, c_d)

    def send(src, dst, ss, rs, row, col):
        return pltpu.make_async_remote_copy(
            src_ref=src, dst_ref=dst, send_sem=ss, recv_sem=rs,
            device_id={"row": row, "col": col}, device_id_type=MESH,
        )

    def load_v(n, slot):
        at = pl.multiple_of(n * CW, CW)
        return pltpu.make_async_copy(vv_hbm.at[:, pl.ds(at, CW)], vbuf.at[slot], v_sem.at[slot])

    load_t = pltpu.make_async_copy(t_hbm, t32, in_sem.at[0])
    load_d = pltpu.make_async_copy(d_hbm, d32, in_sem.at[1])
    load_vo = pltpu.make_async_copy(vo_hbm, vo, in_sem.at[2])
    load_w = pltpu.make_async_copy(w_hbm, wv, in_sem.at[3])
    load_tail = pltpu.make_async_copy(vv_hbm.at[:, pl.ds(NCH * CW, TW)], vtail, in_sem.at[4])
    load_oo = pltpu.make_async_copy(oo_hbm.at[pl.ds(pl.multiple_of(r * RB, RB), RB)], oo, in_sem.at[5])
    load_t.start()
    load_w.start()
    load_d.start()
    load_vo.start()
    load_tail.start()
    load_oo.start()
    load_v(0, 0).start()
    load_v(1, 1).start()

    barrier = pltpu.get_barrier_semaphore()
    for rr in range(4):
        for cc in range(4):
            pl.semaphore_signal(barrier, inc=1, device_id={"row": rr, "col": cc}, device_id_type=MESH)

    with scope("wait_t"):
        load_t.wait()
    for m in range(9):
        piece = t32[:, PB * m : PB * m + PB].astype(BF16)
        trow[c, :, PB * m : PB * m + PB] = piece
        tcol[r, :, PB * m : PB * m + PB] = piece
    with scope("barrier"):
        pl.semaphore_wait(barrier, 16)

    half = RB // 2
    halves = (slice(0, half), slice(half, RB))

    def row_copy(way, h):
        block, peer = ((c, c_y), (c, c_z), ((c_z, c_y), (c_y, c_z))[h])[way]
        piece = trow.at[block, halves[h]]
        return send(piece, piece, row_s.at[way, h], row_r.at[way, h], r, peer)

    def row_wait(way, h):
        piece = trow.at[(c_y, c_z, c_d)[way], halves[h]]
        send(piece, piece, row_s.at[way, h], row_r.at[way, h], r, c_y).wait_recv()

    def col_piece(h):
        piece = tcol.at[r, halves[h]]
        return send(piece, piece, col_s.at[h], col_r.at[h], r_x, c)

    col_pair = send(tcol.at[r], tcol.at[r], col_s.at[2], col_r.at[2], r_k, c)
    col_relay = send(tcol.at[r_x], tcol.at[r_x], col_s.at[3], col_r.at[3], r_k, c)

    def lad_copy(slot, h):
        return send(trow.at[slot, halves[h]], tlad.at[r, halves[h]], lad_s.at[slot, h], lad_r.at[r, h], slot, c)

    def dispatch(slot, h):
        @pl.when(slot != r)
        def _():
            lad_copy(slot, h).start()

        @pl.when(slot == r)
        def _():
            tlad[r, halves[h]] = trow[slot, halves[h]]

    def lad_wait(slot, h):
        send(trow.at[0, halves[h]], tlad.at[slot, halves[h]], lad_s.at[slot, h], lad_r.at[slot, h], r, c).wait_recv()

    def lad_forward(slot, h):
        piece = tlad.at[slot, halves[h]]
        return send(piece, piece, fw_s.at[slot, h], lad_r.at[slot, h], r, c_y)

    gives = jnp.logical_and(x != z, k == y)

    def forward(h):
        @pl.when(gives)
        def _():
            for slot in (r_x, r_d):
                with scope("lad_f"):
                    lad_wait(slot, h)
                lad_forward(slot, h).start()

    @pl.when(x == z)
    def _():
        col_piece(0).start()

    for h in range(2):
        row_copy(0, h).start()
        row_copy(1, h).start()
        dispatch(c, h)
    col_pair.start()

    with scope("wait_w"):
        load_w.wait()

    def mixed(slot):
        for m in range(5):
            split_cols(lambda lo, hi: trow[slot, :, lo:hi].astype(F32), planes, m)
        for h in range(2):
            parts = []
            for j in range(8):
                parts += take_j(planes, 8 * h + j, 0, 4 * AB)
            tm[:, 1152 * h : 1152 * h + 1152] = jnp.concatenate(parts, axis=1).astype(BF16)
        block = lax.dot_general(tm[...], wv[...], (((1,), (1,)), ((), ())), preferred_element_type=F32)

        def put(at, rows, lanes, value):
            pt[slot, at : at + rows, lanes] = value

        pack(put, V, block)

    p_copy = send(pt, pr, p_s.at[0], p_r.at[0], c, r)
    p_out, p_on = [], []
    for q, slot in enumerate((c_y, c_d, c, c_z)):
        via, to, src = ((r_x, c), (c, r_x), slot) if q < 2 else ((r, c_z), (c_z, r), (c_z, c)[q - 2])
        p_out.append(send(pt.at[slot], prel.at[q], p_s.at[1 + q], p_r.at[1 + q], *via))
        p_on.append(send(prel.at[q], pr.at[src], p_s.at[5 + q], p_r.at[5 + q], *to))

    def p_start(q):
        @pl.when(x != z)
        def _():
            p_out[q].start()

    def relay(*quarters):
        for q in quarters:
            with scope("relay"):
                p_out[q].wait_recv()
            p_on[q].start()

    with scope("mixed_c"):
        mixed(c)

    with scope("row10"):
        row_wait(1, 0)
    row_copy(2, 0).start()
    dispatch(c_z, 0)
    with scope("row00"):
        row_wait(0, 0)
    dispatch(c_y, 0)

    load_d.wait()
    for m in range(5):
        split_cols(lambda lo, hi: d32[:, lo:hi], planes, m)
    for cc in range(4):
        parts = []
        for j in range(4):
            parts += take_j(planes, 4 * cc + j, 0, 4 * AB)
        def put_d(at, rows, lanes, value):
            dsnd[cc, at : at + rows, lanes] = value

        pack(put_d, V, jnp.concatenate(parts, axis=1))
    drcv[c] = dsnd[c]

    with scope("row11"):
        row_wait(1, 1)
    dispatch(c_z, 1)
    with scope("row01"):
        row_wait(0, 1)
    row_copy(2, 1).start()
    dispatch(c_y, 1)
    d_copy = [
        send(dsnd.at[peer], drcv.at[c], d_s.at[q], d_r.at[q], r, peer) for q, peer in enumerate(col_peers)
    ]

    @pl.when(x == z)
    def _():
        col_piece(1).start()
        for q in (1, 0, 2):
            d_copy[q].start()

    p_start(2)
    forward(0)
    with scope("mixed_c_z"):
        mixed(c_z)
    p_start(3)
    with scope("row20"):
        row_wait(2, 0)
    with scope("row21"):
        row_wait(2, 1)

    @pl.when(x != z)
    def _():
        dispatch(c_d, 0)
        dispatch(c_d, 1)

    forward(1)
    with scope("mixed_c_y"):
        mixed(c_y)
    p_start(0)
    with scope("mixed_c_d"):
        mixed(c_d)
    p_start(1)

    q_copy = [send(xq, xqr.at[c], q_s.at[q], q_r.at[q], r, peer) for q, peer in enumerate(col_peers)]

    def hole_x():
        load_vo.wait()
        send(tcol.at[r_k], tcol.at[r_k], col_s.at[2], col_r.at[2], r_k, c).wait_recv()

        @pl.when(jnp.logical_and(x == z, r != c))
        def _():
            send(tcol.at[r_x], tcol.at[r_x], f_s.at[0], col_r.at[4], r_k, c).wait_recv()

        @pl.when(r != c)
        def _():
            send(tcol.at[r_d], tcol.at[r_d], col_s.at[3], col_r.at[3], r_k, c).wait_recv()

        xq[...] = lax.dot_general(
            vo[...], tcol[...].reshape(4 * RB, CB), (((1,), (1,)), ((), ())), preferred_element_type=F32
        )
        xqr[c] = xq[...]
        for copy in q_copy:
            copy.start()

    @pl.when(x != z)
    def _():
        with scope("col"):
            for h in range(2):
                piece = tcol.at[r_x, halves[h]]
                send(piece, piece, col_s.at[h], col_r.at[h], r_x, c).wait_recv()
        col_relay.start()
        with scope("hole_x"):
            hole_x()

    @pl.when(jnp.logical_not(gives))
    def _():
        for h in range(2):
            for slot in (r_x, r_d):
                with scope("lad"):
                    lad_wait(slot, h)

    for h in range(2):
        with scope("lad_k"):
            lad_wait(r_k, h)

    fwd = (
        send(tlad.at[r_d], tcol.at[r_d], f_s.at[0], col_r.at[4], r_k, c),
        send(tlad.at[r_x], tcol.at[r_x], f_s.at[1], col_r.at[3], r_k, c),
    )

    @pl.when(r == c)
    def _():
        for copy in fwd:
            copy.start()
        tcol[r_d] = tlad[r_d]
        tcol[r_x] = tlad[r_x]

    @pl.when(x == z)
    def _():
        relay(2)
        with scope("hole_x"):
            hole_x()

        @pl.when(r != c)
        def _():
            p_copy.start()

        @pl.when(r == c)
        def _():
            pr[...] = pt[...]

    def w_copy(rr):
        return send(wt.at[RB * rr : RB * rr + RB], wblk.at[r], w_s.at[rr], w_r.at[r], rr, c)

    def hole_w():
        load_oo.wait()
        for q, peer in enumerate(col_peers):
            send(xq, xqr.at[peer], q_s.at[q], q_r.at[q], r, peer).wait_recv()
        x_sum = (xqr[0] + xqr[1]) + (xqr[2] + xqr[3])
        w_hole = oo[...].astype(F32) + 0.5 * x_sum
        wt[...] = w_hole.T.astype(BF16)
        wblk[r] = wt[pl.ds(pl.multiple_of(r * RB, RB), RB), :]
        for rr in range(4):

            @pl.when(r != rr)
            def _():
                w_copy(rr).start()

    def d2_copy(n):
        return send(acc.at[n, 1 - k], d2r.at[n], dd_s.at[n], dd_r.at[n], r_k, c)

    def xx_copy(n):
        return send(xsb.at[n], xrb.at[n], xx_s.at[n], xx_r.at[n], r_x, c)

    d2_tail = send(acct.at[1 - k], d2t, dd_s.at[NCH], dd_r.at[NCH], r_k, c)
    xx_tail = send(xst, xrt, xx_s.at[NCH], xx_r.at[NCH], r_x, c)

    def gather_w():
        with scope("w_in"):
            for rr in range(4):

                @pl.when(r != rr)
                def _():
                    send(wt.at[0:RB], wblk.at[rr], w_s.at[rr], w_r.at[rr], rr, c).wait_recv()

        wf[...] = jnp.concatenate([wblk[rr].astype(F32) for rr in range(4)], axis=1).astype(BF16)

    def close(lo, hi, landed):
        hole = jnp.dot(wf[...], tcol[:, :, lo:hi].reshape(4 * RB, hi - lo), preferred_element_type=F32)
        r1[:, lo:hi] = r1[:, lo:hi] + landed + hole + vo[:, lo:hi].astype(F32)

    def stripe_rows(m):
        return 32 if m < 4 else 16

    def l_copy(m, q):
        there = pl.ds(V * m, stripe_rows(m) * 9 // 2)
        peer = col_peers[q]
        return send(lsnd.at[peer, there], lrcv.at[c, there], l_s.at[m, q], l_r.at[m, q], r, peer)

    def stripe_out(m):
        for n in ((0, 1, 2), (3, 4), (5, 6), (7, 8), (9,))[m]:
            with scope("sum"):
                xx_copy(n).wait_recv()
            close(CW * n, CW * n + CW, xrb[n])
        if m == 4:
            xx_tail.wait_recv()
            close(NCH * CW, CB, xrt[...])
        split_cols(lambda lo, hi: r1[:, lo:hi], planes, m)
        rows = stripe_rows(m)
        for cc in range(4):
            parts = []
            for j in range(4):
                parts += take_j(planes, 4 * cc + j, RB * 8 * m, rows)

            def put_l(at, count, lanes, value):
                lsnd[cc, V * m + at : V * m + at + count, lanes] = value

            pack(put_l, rows, jnp.concatenate(parts, axis=1))
        there = slice(V * m, V * m + rows * 9 // 2)
        lrcv[c, there, :] = lsnd[c, there, :]
        for q in range(3):
            l_copy(m, q).start()

    load_tail.wait()
    part = jnp.dot(tlad[...].reshape(4 * RB, CB), vtail[...], preferred_element_type=F32)
    for rr in range(4):
        acct[rr % 2, rr // 2] = part[RB * rr : RB * rr + RB]
    d2_tail.start()

    def second(n):
        with scope("pair"):
            d2_copy(n).wait_recv()
        xsb[n] = acc[n, k, 1 - x] + d2r[n, 1 - x]
        at = pl.multiple_of(n * CW, CW)
        r1[:, pl.ds(at, CW)] = acc[n, k, x] + d2r[n, x]
        xx_copy(n).start()

    def ladder_step(n, carry):
        slot = n % 2
        with scope("wait_v"):
            load_v(n, slot).wait()
        with scope("dot"):
            for h in range(2):
                part = jnp.dot(
                    tlad[...].reshape(4 * RB, CB), vbuf[slot, :, 256 * h : 256 * h + 256], preferred_element_type=F32
                )
                for rr in range(4):
                    acc[n, rr % 2, rr // 2, :, 256 * h : 256 * h + 256] = part[RB * rr : RB * rr + RB]
        d2_copy(n).start()

        @pl.when(n + 2 < NCH)
        def _():
            load_v(n + 2, slot).start()

        @pl.when(n == 0)
        def _():
            d2_tail.wait_recv()
            xst[...] = acct[k, 1 - x] + d2t[1 - x]
            r1[:, NCH * CW : CB] = acct[k, x] + d2t[x]
            xx_tail.start()

        @pl.when(n > 0)
        def _():
            second(n - 1)

        @pl.when(jnp.logical_and(n == 1, x != z))
        def _():
            for copy in d_copy:
                copy.start()

        @pl.when(jnp.logical_and(n == 1, x == z))
        def _():
            relay(3)

        @pl.when(jnp.logical_and(n == 3, x == z))
        def _():
            relay(0)

        @pl.when(jnp.logical_and(n == 5, x == z))
        def _():
            relay(1)

        @pl.when(n == jnp.where(x == z, 4, 2))
        def _():
            with scope("hole_w"):
                hole_w()

        @pl.when(jnp.logical_and(n == 9, x != z))
        def _():
            gather_w()
            stripe_out(0)
            stripe_out(1)

        return carry

    lax.fori_loop(0, NCH, ladder_step, 0)
    second(NCH - 1)

    @pl.when(x == z)
    def _():
        gather_w()
        stripe_out(0)
        stripe_out(1)

    for m in range(2, 5):
        stripe_out(m)

    def order_rows(src, dst):
        for cc in range(4):
            for i in range(4):
                first = V * i + AB * cc
                for b in range(4):
                    dst[first : first + AB, 128 * b : 128 * b + 128] = src[cc, pl.ds(V * b + i, AB, stride=4), :]
                ends = src[cc, pl.ds(4 * V + i, AB // 2, stride=4), :]
                dst[first : first + AB // 2, 512:576] = ends[:, 0:64]
                dst[first + AB // 2 : first + AB, 512:576] = ends[:, 64:128]

    order_rows(pt, pp)
    with scope("mirror"):

        @pl.when(jnp.logical_and(x == z, r != c))
        def _():
            p_copy.wait_recv()

        @pl.when(x != z)
        def _():
            for copy in p_on:
                copy.wait_recv()

    order_rows(pr, r3)
    pp[...] = pp[...] + r3[...].T
    for q, peer in enumerate(col_peers):
        with scope("denom"):
            send(dsnd.at[peer], drcv.at[peer], d_s.at[q], d_r.at[q], r, peer).wait_recv()
    order_rows(drcv, r3)
    for m in range(5):
        rows = stripe_rows(m)
        for q, peer in enumerate(col_peers):
            there = pl.ds(V * m, rows * 9 // 2)
            with scope("regroup"):
                send(
                    lsnd.at[peer, there], lrcv.at[peer, there], l_s.at[m, q], l_r.at[m, q], r, peer
                ).wait_recv()
        for cc in range(4):
            for i in range(4):
                first = V * i + AB * cc + 8 * m
                n = rows // 4

                def finish(at, count, lanes, value):
                    there = slice(at, at + count)
                    out_ref[there, lanes] = (value + pp[there, lanes]) / r3[there, lanes]

                for b in range(4):
                    part = lrcv[cc, pl.ds(V * m + rows * b + i, n, stride=4), :]
                    finish(first, n, slice(128 * b, 128 * b + 128), part)
                ends = lrcv[cc, pl.ds(V * m + 4 * rows + i, n // 2, stride=4), :]
                finish(first, n // 2, slice(512, 576), ends[:, 0:64])
                finish(first + n // 2, n // 2, slice(512, 576), ends[:, 64:128])

    for copy in (col_pair, *q_copy, *d_copy, d2_tail, xx_tail):
        copy.wait_send()
    for m in range(5):
        for q in range(3):
            l_copy(m, q).wait_send()
    for way in range(3):
        for h in range(2):
            row_copy(way, h).wait_send()

    @pl.when(x == z)
    def _():
        for h in range(2):
            col_piece(h).wait_send()
        for copy in p_on:
            copy.wait_send()

    @pl.when(jnp.logical_and(x == z, r != c))
    def _():
        p_copy.wait_send()

    @pl.when(x != z)
    def _():
        col_relay.wait_send()
        for copy in p_out:
            copy.wait_send()

    @pl.when(r == c)
    def _():
        for copy in fwd:
            copy.wait_send()

    @pl.when(gives)
    def _():
        for h in range(2):
            for slot in (r_x, r_d):
                lad_forward(slot, h).wait_send()

    for slot in range(4):

        @pl.when(slot != r)
        def _():
            w_copy(slot).wait_send()

        @pl.when(jnp.logical_and(slot != r, jnp.logical_or(slot != c_d, x != z)))
        def _():
            for h in range(2):
                lad_copy(slot, h).wait_send()

    def drain(n, carry):
        d2_copy(n).wait_send()
        xx_copy(n).wait_send()
        return carry

    lax.fori_loop(0, NCH, drain, 0)


def solution(mesh):
    vm = pltpu.VMEM
    dma = pltpu.SemaphoreType.DMA
    scratch = [
        vm((RB, CB), F32), vm((RB, CB), F32), vm((RB, CB), BF16), vm((PB, O * V), BF16),
        vm((4, RB, CB), BF16), vm((4, RB, CB), BF16), vm((4, RB, CB), BF16),
        vm((2, AB * RB, 128), F32), vm((V, O * V), BF16),
        vm((PB, PB), F32), vm((PB, PB), F32), vm((4, PQ, 128), F32), vm((4, PQ, 128), F32),
        vm((4, PQ, 128), F32), vm((4, PQ, 128), F32), vm((4, PQ, 128), F32), vm((4, PQ, 128), F32),
        vm((4, PQ, 128), F32),
        vm((RB, O * O), F32), vm((4, RB, O * O), F32), vm((O * O, RB), BF16), vm((RB, O * O), BF16), vm((4, RB, RB), BF16), vm((RB, O * O), BF16),
        vm((2, CB, CW), BF16), vm((CB, TW), BF16),
        vm((NCH, 2, 2, RB, CW), F32), vm((NCH, 2, RB, CW), F32), vm((NCH, RB, CW), F32), vm((NCH, RB, CW), F32),
        vm((2, 2, RB, TW), F32), vm((2, RB, TW), F32), vm((RB, TW), F32), vm((RB, TW), F32),
        vm((RB, CB), F32),
        dma((6,)), dma((2,)), dma((3, 2)), dma((3, 2)), dma((5,)), dma((5,)), dma((4, 2)), dma((4, 2)),
        dma((3,)), dma((3,)), dma((3,)), dma((3,)), dma((5, 3)), dma((5, 3)), dma((9,)), dma((9,)), dma((4, 2)),
        dma((NCH + 1,)), dma((NCH + 1,)), dma((NCH + 1,)), dma((NCH + 1,)), dma((4,)), dma((4,)), dma((2,)),
    ]
    hbm = pl.BlockSpec(memory_space=pl.ANY)
    vmem = pl.BlockSpec(memory_space=pltpu.VMEM)
    call = pl.pallas_call(
        kernel,
        out_shape=jax.ShapeDtypeStruct((PB, PB), F32),
        in_specs=[hbm] * 6,
        out_specs=vmem,
        scratch_shapes=scratch,
        compiler_params=pltpu.CompilerParams(
            collective_id=0, has_side_effects=True, vmem_limit_bytes=67_000_000
        ),
        name="sweep",
    )
    def local_sweep(t_blk, d_blk, voovv_blk, vvvvv_blk, oooo, w_blk):
        return call(t_blk, d_blk, voovv_blk, vvvvv_blk, oooo, w_blk.T)

    return jax.shard_map(
        local_sweep,
        mesh=mesh,
        in_specs=(P("row", "col"), P("row", "col"), P("row", "col"), P("row", "col"), P(None, None), P(None, "col")),
        out_specs=P("row", "col"),
        check_vma=False,
    )
```

```python
import functools

import jax
import jax.numpy as jnp
from jax import lax
from jax.experimental import pallas as pl
from jax.experimental.pallas import tpu as pltpu
from jax.sharding import PartitionSpec as P

MESH = pl.DeviceIdType.MESH
scope = jax.named_scope
F32 = jnp.float32
BF16 = jnp.bfloat16

O = 16
V = 144
RB = 64
CB = 5184
AB = 36
PQ = 648
PB = 576
CW = 512
NCH = CB // CW
TW = CB - NCH * CW


def stripe(load, m, q):
    first = 1152 * m + V * q
    low = first // 128 * 128
    high = min(-(-(first + V) // 128) * 128, CB)
    return load(low, high)[:, first - low : first - low + V]


def split_cols(load, planes, m):
    for q in range(8 if m < 4 else 4):
        piece = stripe(load, m, q)
        base = RB * (8 * m + q)
        planes[0, base : base + RB, :] = piece[:, 0:128]
        planes[1, base : base + RB, 0:16] = piece[:, 128:144]


def take_j(planes, j, base, rows):
    wide = planes[0, pl.ds(base + j, rows, stride=16), :]
    rest = planes[1, pl.ds(base + j, rows, stride=16), :]
    return [wide, rest[:, 0:16]]


def pack(put, rows, wide):
    for b in range(4):
        put(rows * b, rows, slice(0, 128), wide[:, 128 * b : 128 * b + 128])
    put(4 * rows, rows // 2, slice(0, 64), wide[: rows // 2, 512:576])
    put(4 * rows, rows // 2, slice(64, 128), wide[rows // 2 :, 512:576])


def kernel(
    t_hbm, d_hbm, vo_hbm, vv_hbm, oo_hbm, w_hbm, out_ref,
    t32, d32, vo, wv, trow, tcol, tlad, planes, tm, r3, pp, pt, pr,
    dsnd, drcv, lsnd, lrcv, prel, xq, xqr, wt, oo, wblk, wf, vbuf, vtail,
    acc, d2r, xsb, xrb, acct, d2t, xst, xrt, r1,
    in_sem, v_sem, row_s, row_r, col_s, col_r, lad_s, lad_r, q_s, q_r,
    d_s, d_r, l_s, l_r, p_s, p_r, fw_s, dd_s, dd_r, xx_s, xx_r, w_s, w_r, f_s,
):
    r = lax.axis_index("row")
    c = lax.axis_index("col")
    x, k = r // 2, r % 2
    z, y = c // 2, c % 2
    r_k, r_x = 2 * x + 1 - k, 2 * (1 - x) + k
    r_d = 2 * (1 - x) + 1 - k
    c_y, c_z = 2 * z + 1 - y, 2 * (1 - z) + y
    c_d = 2 * (1 - z) + 1 - y
    col_peers = (c_y, c_z, c_d)

    def send(src, dst, ss, rs, row, col):
        return pltpu.make_async_remote_copy(
            src_ref=src, dst_ref=dst, send_sem=ss, recv_sem=rs,
            device_id={"row": row, "col": col}, device_id_type=MESH,
        )

    def load_v(n, slot):
        at = pl.multiple_of(n * CW, CW)
        return pltpu.make_async_copy(vv_hbm.at[:, pl.ds(at, CW)], vbuf.at[slot], v_sem.at[slot])

    load_t = pltpu.make_async_copy(t_hbm, t32, in_sem.at[0])
    load_d = pltpu.make_async_copy(d_hbm, d32, in_sem.at[1])
    load_vo = pltpu.make_async_copy(vo_hbm, vo, in_sem.at[2])
    load_w = pltpu.make_async_copy(w_hbm, wv, in_sem.at[3])
    load_tail = pltpu.make_async_copy(vv_hbm.at[:, pl.ds(NCH * CW, TW)], vtail, in_sem.at[4])
    load_oo = pltpu.make_async_copy(oo_hbm.at[pl.ds(pl.multiple_of(r * RB, RB), RB)], oo, in_sem.at[5])
    load_t.start()
    load_w.start()
    load_d.start()
    load_vo.start()
    load_tail.start()
    load_oo.start()
    load_v(0, 0).start()
    load_v(1, 1).start()

    barrier = pltpu.get_barrier_semaphore()
    for rr in range(4):
        for cc in range(4):
            pl.semaphore_signal(barrier, inc=1, device_id={"row": rr, "col": cc}, device_id_type=MESH)

    with scope("wait_t"):
        load_t.wait()
    for m in range(9):
        piece = t32[:, PB * m : PB * m + PB].astype(BF16)
        trow[c, :, PB * m : PB * m + PB] = piece
        tcol[r, :, PB * m : PB * m + PB] = piece
    with scope("barrier"):
        pl.semaphore_wait(barrier, 16)

    half = RB // 2
    halves = (slice(0, half), slice(half, RB))

    def row_copy(way, h):
        block, peer = ((c, c_y), (c, c_z), ((c_z, c_y), (c_y, c_z))[h])[way]
        piece = trow.at[block, halves[h]]
        return send(piece, piece, row_s.at[way, h], row_r.at[way, h], r, peer)

    def row_wait(way, h):
        piece = trow.at[(c_y, c_z, c_d)[way], halves[h]]
        send(piece, piece, row_s.at[way, h], row_r.at[way, h], r, c_y).wait_recv()

    def col_piece(h):
        piece = tcol.at[r, halves[h]]
        return send(piece, piece, col_s.at[h], col_r.at[h], r_x, c)

    col_pair = send(tcol.at[r], tcol.at[r], col_s.at[2], col_r.at[2], r_k, c)
    col_relay = send(tcol.at[r_x], tcol.at[r_x], col_s.at[3], col_r.at[3], r_k, c)

    def lad_copy(slot, h):
        return send(trow.at[slot, halves[h]], tlad.at[r, halves[h]], lad_s.at[slot, h], lad_r.at[r, h], slot, c)

    def dispatch(slot, h):
        @pl.when(slot != r)
        def _():
            lad_copy(slot, h).start()

        @pl.when(slot == r)
        def _():
            tlad[r, halves[h]] = trow[slot, halves[h]]

    def lad_wait(slot, h):
        send(trow.at[0, halves[h]], tlad.at[slot, halves[h]], lad_s.at[slot, h], lad_r.at[slot, h], r, c).wait_recv()

    def lad_forward(slot, h):
        piece = tlad.at[slot, halves[h]]
        return send(piece, piece, fw_s.at[slot, h], lad_r.at[slot, h], r, c_y)

    gives = jnp.logical_and(x != z, k == y)

    def forward(h):
        @pl.when(gives)
        def _():
            for slot in (r_x, r_d):
                with scope("lad_f"):
                    lad_wait(slot, h)
                lad_forward(slot, h).start()

    @pl.when(x == z)
    def _():
        col_piece(0).start()

    for h in range(2):
        row_copy(0, h).start()
        row_copy(1, h).start()
        dispatch(c, h)
    col_pair.start()

    with scope("wait_w"):
        load_w.wait()

    def mixed(slot):
        for m in range(5):
            split_cols(lambda lo, hi: trow[slot, :, lo:hi].astype(F32), planes, m)
        for h in range(2):
            parts = []
            for j in range(8):
                parts += take_j(planes, 8 * h + j, 0, 4 * AB)
            tm[:, 1152 * h : 1152 * h + 1152] = jnp.concatenate(parts, axis=1).astype(BF16)
        block = lax.dot_general(tm[...], wv[...], (((1,), (1,)), ((), ())), preferred_element_type=F32)

        def put(at, rows, lanes, value):
            pt[slot, at : at + rows, lanes] = value

        pack(put, V, block)

    p_copy = send(pt, pr, p_s.at[0], p_r.at[0], c, r)
    p_out, p_on = [], []
    for q, slot in enumerate((c_y, c_d, c, c_z)):
        via, to, src = ((r_x, c), (c, r_x), slot) if q < 2 else ((r, c_z), (c_z, r), (c_z, c)[q - 2])
        p_out.append(send(pt.at[slot], prel.at[q], p_s.at[1 + q], p_r.at[1 + q], *via))
        p_on.append(send(prel.at[q], pr.at[src], p_s.at[5 + q], p_r.at[5 + q], *to))

    def p_start(q):
        @pl.when(x != z)
        def _():
            p_out[q].start()

    def relay(*quarters):
        for q in quarters:
            with scope("relay"):
                p_out[q].wait_recv()
            p_on[q].start()

    with scope("mixed_c"):
        mixed(c)

    with scope("row10"):
        row_wait(1, 0)
    row_copy(2, 0).start()
    dispatch(c_z, 0)
    with scope("row00"):
        row_wait(0, 0)
    dispatch(c_y, 0)

    load_d.wait()
    for m in range(5):
        split_cols(lambda lo, hi: d32[:, lo:hi], planes, m)
    for cc in range(4):
        parts = []
        for j in range(4):
            parts += take_j(planes, 4 * cc + j, 0, 4 * AB)
        def put_d(at, rows, lanes, value):
            dsnd[cc, at : at + rows, lanes] = value

        pack(put_d, V, jnp.concatenate(parts, axis=1))
    drcv[c] = dsnd[c]

    with scope("row11"):
        row_wait(1, 1)
    dispatch(c_z, 1)
    with scope("row01"):
        row_wait(0, 1)
    row_copy(2, 1).start()
    dispatch(c_y, 1)
    d_copy = [
        send(dsnd.at[peer], drcv.at[c], d_s.at[q], d_r.at[q], r, peer) for q, peer in enumerate(col_peers)
    ]

    @pl.when(x == z)
    def _():
        col_piece(1).start()
        d_copy[1].start()
        d_copy[0].start()

    p_start(2)
    forward(0)
    with scope("mixed_c_z"):
        mixed(c_z)
    p_start(3)
    with scope("row20"):
        row_wait(2, 0)
    forward(1)
    with scope("row21"):
        row_wait(2, 1)

    @pl.when(x != z)
    def _():
        dispatch(c_d, 0)
        dispatch(c_d, 1)

    with scope("mixed_c_y"):
        mixed(c_y)
    p_start(0)
    with scope("mixed_c_d"):
        mixed(c_d)
    p_start(1)

    q_copy = [send(xq, xqr.at[c], q_s.at[q], q_r.at[q], r, peer) for q, peer in enumerate(col_peers)]

    def hole_x():
        load_vo.wait()
        send(tcol.at[r_k], tcol.at[r_k], col_s.at[2], col_r.at[2], r_k, c).wait_recv()

        @pl.when(jnp.logical_and(x == z, r != c))
        def _():
            send(tcol.at[r_x], tcol.at[r_x], f_s.at[0], col_r.at[4], r_k, c).wait_recv()

        @pl.when(r != c)
        def _():
            send(tcol.at[r_d], tcol.at[r_d], col_s.at[3], col_r.at[3], r_k, c).wait_recv()

        xq[...] = lax.dot_general(
            vo[...], tcol[...].reshape(4 * RB, CB), (((1,), (1,)), ((), ())), preferred_element_type=F32
        )
        xqr[c] = xq[...]
        for copy in q_copy:
            copy.start()

    @pl.when(x != z)
    def _():
        with scope("col"):
            for h in range(2):
                piece = tcol.at[r_x, halves[h]]
                send(piece, piece, col_s.at[h], col_r.at[h], r_x, c).wait_recv()
        col_relay.start()
        with scope("hole_x"):
            hole_x()

    @pl.when(jnp.logical_not(gives))
    def _():
        for h in range(2):
            for slot in (r_x, r_d):
                with scope("lad"):
                    lad_wait(slot, h)

    for h in range(2):
        with scope("lad_k"):
            lad_wait(r_k, h)

    fwd = (
        send(tlad.at[r_d], tcol.at[r_d], f_s.at[0], col_r.at[4], r_k, c),
        send(tlad.at[r_x], tcol.at[r_x], f_s.at[1], col_r.at[3], r_k, c),
    )

    @pl.when(r == c)
    def _():
        for copy in fwd:
            copy.start()
        tcol[r_d] = tlad[r_d]
        tcol[r_x] = tlad[r_x]

    @pl.when(x == z)
    def _():
        relay(2)
        with scope("hole_x"):
            hole_x()

        @pl.when(r != c)
        def _():
            p_copy.start()

        @pl.when(r == c)
        def _():
            pr[...] = pt[...]

    def w_copy(rr):
        return send(wt.at[RB * rr : RB * rr + RB], wblk.at[r], w_s.at[rr], w_r.at[r], rr, c)

    def hole_w():
        load_oo.wait()
        for q, peer in enumerate(col_peers):
            send(xq, xqr.at[peer], q_s.at[q], q_r.at[q], r, peer).wait_recv()
        x_sum = (xqr[0] + xqr[1]) + (xqr[2] + xqr[3])
        w_hole = oo[...].astype(F32) + 0.5 * x_sum
        wt[...] = w_hole.T.astype(BF16)
        wblk[r] = wt[pl.ds(pl.multiple_of(r * RB, RB), RB), :]
        for rr in range(4):

            @pl.when(r != rr)
            def _():
                w_copy(rr).start()

    def d2_copy(n):
        return send(acc.at[n, 1 - k], d2r.at[n], dd_s.at[n], dd_r.at[n], r_k, c)

    def xx_copy(n):
        return send(xsb.at[n], xrb.at[n], xx_s.at[n], xx_r.at[n], r_x, c)

    d2_tail = send(acct.at[1 - k], d2t, dd_s.at[NCH], dd_r.at[NCH], r_k, c)
    xx_tail = send(xst, xrt, xx_s.at[NCH], xx_r.at[NCH], r_x, c)

    def gather_w():
        with scope("w_in"):
            for rr in range(4):

                @pl.when(r != rr)
                def _():
                    send(wt.at[0:RB], wblk.at[rr], w_s.at[rr], w_r.at[rr], rr, c).wait_recv()

        wf[...] = jnp.concatenate([wblk[rr].astype(F32) for rr in range(4)], axis=1).astype(BF16)

    def close(lo, hi, landed):
        hole = jnp.dot(wf[...], tcol[:, :, lo:hi].reshape(4 * RB, hi - lo), preferred_element_type=F32)
        r1[:, lo:hi] = r1[:, lo:hi] + landed + hole + vo[:, lo:hi].astype(F32)

    def stripe_rows(m):
        return 32 if m < 4 else 16

    def l_copy(m, q):
        there = pl.ds(V * m, stripe_rows(m) * 9 // 2)
        peer = col_peers[q]
        return send(lsnd.at[peer, there], lrcv.at[c, there], l_s.at[m, q], l_r.at[m, q], r, peer)

    def stripe_out(m):
        for n in ((0, 1, 2), (3, 4), (5, 6), (7, 8), (9,))[m]:
            with scope("sum"):
                xx_copy(n).wait_recv()
            close(CW * n, CW * n + CW, xrb[n])
        if m == 4:
            xx_tail.wait_recv()
            close(NCH * CW, CB, xrt[...])
        split_cols(lambda lo, hi: r1[:, lo:hi], planes, m)
        rows = stripe_rows(m)
        for cc in range(4):
            parts = []
            for j in range(4):
                parts += take_j(planes, 4 * cc + j, RB * 8 * m, rows)

            def put_l(at, count, lanes, value):
                lsnd[cc, V * m + at : V * m + at + count, lanes] = value

            pack(put_l, rows, jnp.concatenate(parts, axis=1))
        there = slice(V * m, V * m + rows * 9 // 2)
        lrcv[c, there, :] = lsnd[c, there, :]
        for q in range(3):
            l_copy(m, q).start()

    load_tail.wait()
    part = jnp.dot(tlad[...].reshape(4 * RB, CB), vtail[...], preferred_element_type=F32)
    for rr in range(4):
        acct[rr % 2, rr // 2] = part[RB * rr : RB * rr + RB]
    d2_tail.start()

    def second(n):
        with scope("pair"):
            d2_copy(n).wait_recv()
        xsb[n] = acc[n, k, 1 - x] + d2r[n, 1 - x]
        at = pl.multiple_of(n * CW, CW)
        r1[:, pl.ds(at, CW)] = acc[n, k, x] + d2r[n, x]
        xx_copy(n).start()

    def ladder_step(n, carry):
        slot = n % 2
        with scope("wait_v"):
            load_v(n, slot).wait()
        with scope("dot"):
            for h in range(2):
                part = jnp.dot(
                    tlad[...].reshape(4 * RB, CB), vbuf[slot, :, 256 * h : 256 * h + 256], preferred_element_type=F32
                )
                for rr in range(4):
                    acc[n, rr % 2, rr // 2, :, 256 * h : 256 * h + 256] = part[RB * rr : RB * rr + RB]
        d2_copy(n).start()

        @pl.when(n + 2 < NCH)
        def _():
            load_v(n + 2, slot).start()

        @pl.when(n == 0)
        def _():
            d2_tail.wait_recv()
            xst[...] = acct[k, 1 - x] + d2t[1 - x]
            r1[:, NCH * CW : CB] = acct[k, x] + d2t[x]
            xx_tail.start()

        @pl.when(n > 0)
        def _():
            second(n - 1)

        @pl.when(jnp.logical_and(n == 1, x != z))
        def _():
            for copy in d_copy:
                copy.start()

        @pl.when(jnp.logical_and(n == 1, x == z))
        def _():
            relay(3)

        @pl.when(jnp.logical_and(n == 2, x == z))
        def _():
            d_copy[2].start()

        @pl.when(jnp.logical_and(n == 3, x == z))
        def _():
            relay(0)

        @pl.when(jnp.logical_and(n == 5, x == z))
        def _():
            relay(1)

        @pl.when(n == jnp.where(x == z, 4, 2))
        def _():
            with scope("hole_w"):
                hole_w()

        @pl.when(jnp.logical_and(n == 9, x != z))
        def _():
            gather_w()
            stripe_out(0)
            stripe_out(1)

        return carry

    lax.fori_loop(0, NCH, ladder_step, 0)
    second(NCH - 1)

    @pl.when(x == z)
    def _():
        gather_w()
        stripe_out(0)
        stripe_out(1)

    def order_rows(src, dst):
        for cc in range(4):
            for i in range(4):
                first = V * i + AB * cc
                for b in range(4):
                    dst[first : first + AB, 128 * b : 128 * b + 128] = src[cc, pl.ds(V * b + i, AB, stride=4), :]
                ends = src[cc, pl.ds(4 * V + i, AB // 2, stride=4), :]
                dst[first : first + AB // 2, 512:576] = ends[:, 0:64]
                dst[first + AB // 2 : first + AB, 512:576] = ends[:, 64:128]

    for m in range(2, 4):
        stripe_out(m)
    order_rows(pt, pp)
    with scope("mirror"):

        @pl.when(jnp.logical_and(x == z, r != c))
        def _():
            p_copy.wait_recv()

        @pl.when(x != z)
        def _():
            for copy in p_on:
                copy.wait_recv()

    order_rows(pr, r3)
    pp[...] = pp[...] + r3[...].T
    for q, peer in enumerate(col_peers):
        with scope("denom"):
            send(dsnd.at[peer], drcv.at[peer], d_s.at[q], d_r.at[q], r, peer).wait_recv()
    order_rows(drcv, r3)
    stripe_out(4)

    for m in range(5):
        rows = stripe_rows(m)
        for q, peer in enumerate(col_peers):
            there = pl.ds(V * m, rows * 9 // 2)
            with scope("regroup"):
                send(
                    lsnd.at[peer, there], lrcv.at[peer, there], l_s.at[m, q], l_r.at[m, q], r, peer
                ).wait_recv()
        for cc in range(4):
            for i in range(4):
                first = V * i + AB * cc + 8 * m
                n = rows // 4

                def finish(at, count, lanes, value):
                    there = slice(at, at + count)
                    out_ref[there, lanes] = (value + pp[there, lanes]) / r3[there, lanes]

                for b in range(4):
                    part = lrcv[cc, pl.ds(V * m + rows * b + i, n, stride=4), :]
                    finish(first, n, slice(128 * b, 128 * b + 128), part)
                ends = lrcv[cc, pl.ds(V * m + 4 * rows + i, n // 2, stride=4), :]
                finish(first, n // 2, slice(512, 576), ends[:, 0:64])
                finish(first + n // 2, n // 2, slice(512, 576), ends[:, 64:128])

    for copy in (col_pair, *q_copy, *d_copy, d2_tail, xx_tail):
        copy.wait_send()
    for m in range(5):
        for q in range(3):
            l_copy(m, q).wait_send()
    for way in range(3):
        for h in range(2):
            row_copy(way, h).wait_send()

    @pl.when(x == z)
    def _():
        for h in range(2):
            col_piece(h).wait_send()
        for copy in p_on:
            copy.wait_send()

    @pl.when(jnp.logical_and(x == z, r != c))
    def _():
        p_copy.wait_send()

    @pl.when(x != z)
    def _():
        col_relay.wait_send()
        for copy in p_out:
            copy.wait_send()

    @pl.when(r == c)
    def _():
        for copy in fwd:
            copy.wait_send()

    @pl.when(gives)
    def _():
        for h in range(2):
            for slot in (r_x, r_d):
                lad_forward(slot, h).wait_send()

    for slot in range(4):

        @pl.when(slot != r)
        def _():
            w_copy(slot).wait_send()

        @pl.when(jnp.logical_and(slot != r, jnp.logical_or(slot != c_d, x != z)))
        def _():
            for h in range(2):
                lad_copy(slot, h).wait_send()

    def drain(n, carry):
        d2_copy(n).wait_send()
        xx_copy(n).wait_send()
        return carry

    lax.fori_loop(0, NCH, drain, 0)


def solution(mesh):
    vm = pltpu.VMEM
    dma = pltpu.SemaphoreType.DMA
    scratch = [
        vm((RB, CB), F32), vm((RB, CB), F32), vm((RB, CB), BF16), vm((PB, O * V), BF16),
        vm((4, RB, CB), BF16), vm((4, RB, CB), BF16), vm((4, RB, CB), BF16),
        vm((2, AB * RB, 128), F32), vm((V, O * V), BF16),
        vm((PB, PB), F32), vm((PB, PB), F32), vm((4, PQ, 128), F32), vm((4, PQ, 128), F32),
        vm((4, PQ, 128), F32), vm((4, PQ, 128), F32), vm((4, PQ, 128), F32), vm((4, PQ, 128), F32),
        vm((4, PQ, 128), F32),
        vm((RB, O * O), F32), vm((4, RB, O * O), F32), vm((O * O, RB), BF16), vm((RB, O * O), BF16), vm((4, RB, RB), BF16), vm((RB, O * O), BF16),
        vm((2, CB, CW), BF16), vm((CB, TW), BF16),
        vm((NCH, 2, 2, RB, CW), F32), vm((NCH, 2, RB, CW), F32), vm((NCH, RB, CW), F32), vm((NCH, RB, CW), F32),
        vm((2, 2, RB, TW), F32), vm((2, RB, TW), F32), vm((RB, TW), F32), vm((RB, TW), F32),
        vm((RB, CB), F32),
        dma((6,)), dma((2,)), dma((3, 2)), dma((3, 2)), dma((5,)), dma((5,)), dma((4, 2)), dma((4, 2)),
        dma((3,)), dma((3,)), dma((3,)), dma((3,)), dma((5, 3)), dma((5, 3)), dma((9,)), dma((9,)), dma((4, 2)),
        dma((NCH + 1,)), dma((NCH + 1,)), dma((NCH + 1,)), dma((NCH + 1,)), dma((4,)), dma((4,)), dma((2,)),
    ]
    hbm = pl.BlockSpec(memory_space=pl.ANY)
    vmem = pl.BlockSpec(memory_space=pltpu.VMEM)
    call = pl.pallas_call(
        kernel,
        out_shape=jax.ShapeDtypeStruct((PB, PB), F32),
        in_specs=[hbm] * 6,
        out_specs=vmem,
        scratch_shapes=scratch,
        compiler_params=pltpu.CompilerParams(
            collective_id=0, has_side_effects=True, vmem_limit_bytes=67_000_000
        ),
        name="sweep",
    )
    def local_sweep(t_blk, d_blk, voovv_blk, vvvvv_blk, oooo, w_blk):
        return call(t_blk, d_blk, voovv_blk, vvvvv_blk, oooo, w_blk.T)

    return jax.shard_map(
        local_sweep,
        mesh=mesh,
        in_specs=(P("row", "col"), P("row", "col"), P("row", "col"), P("row", "col"), P(None, None), P(None, "col")),
        out_specs=P("row", "col"),
        check_vma=False,
    )
```

```python
import functools

import jax
import jax.numpy as jnp
from jax import lax
from jax.experimental import pallas as pl
from jax.experimental.pallas import tpu as pltpu
from jax.sharding import PartitionSpec as P

MESH = pl.DeviceIdType.MESH
scope = jax.named_scope
F32 = jnp.float32
BF16 = jnp.bfloat16

O = 16
V = 144
RB = 64
CB = 5184
AB = 36
PQ = 648
PB = 576
CW = 512
NCH = CB // CW
TW = CB - NCH * CW


def stripe(load, m, q):
    first = 1152 * m + V * q
    low = first // 128 * 128
    high = min(-(-(first + V) // 128) * 128, CB)
    return load(low, high)[:, first - low : first - low + V]


def split_cols(load, planes, m):
    for q in range(8 if m < 4 else 4):
        piece = stripe(load, m, q)
        base = RB * (8 * m + q)
        planes[0, base : base + RB, :] = piece[:, 0:128]
        planes[1, base : base + RB, 0:16] = piece[:, 128:144]


def take_j(planes, j, base, rows):
    wide = planes[0, pl.ds(base + j, rows, stride=16), :]
    rest = planes[1, pl.ds(base + j, rows, stride=16), :]
    return [wide, rest[:, 0:16]]


def pack(put, rows, wide):
    for b in range(4):
        put(rows * b, rows, slice(0, 128), wide[:, 128 * b : 128 * b + 128])
    put(4 * rows, rows // 2, slice(0, 64), wide[: rows // 2, 512:576])
    put(4 * rows, rows // 2, slice(64, 128), wide[rows // 2 :, 512:576])


def kernel(
    t_hbm, d_hbm, vo_hbm, vv_hbm, oo_hbm, w_hbm, out_ref,
    t32, d32, vo, wv, trow, tcol, tlad, planes, tm, r3, pp, pt, pr,
    dsnd, drcv, lsnd, lrcv, prel, xq, xqr, wt, oo, wblk, wf, vbuf, vtail,
    acc, d2r, xsb, xrb, acct, d2t, xst, xrt, r1,
    in_sem, v_sem, row_s, row_r, col_s, col_r, lad_s, lad_r, q_s, q_r,
    d_s, d_r, l_s, l_r, p_s, p_r, fw_s, dd_s, dd_r, xx_s, xx_r, w_s, w_r, f_s,
):
    r = lax.axis_index("row")
    c = lax.axis_index("col")
    x, k = r // 2, r % 2
    z, y = c // 2, c % 2
    r_k, r_x = 2 * x + 1 - k, 2 * (1 - x) + k
    r_d = 2 * (1 - x) + 1 - k
    c_y, c_z = 2 * z + 1 - y, 2 * (1 - z) + y
    c_d = 2 * (1 - z) + 1 - y
    col_peers = (c_y, c_z, c_d)

    def send(src, dst, ss, rs, row, col):
        return pltpu.make_async_remote_copy(
            src_ref=src, dst_ref=dst, send_sem=ss, recv_sem=rs,
            device_id={"row": row, "col": col}, device_id_type=MESH,
        )

    def load_v(n, slot):
        at = pl.multiple_of(n * CW, CW)
        return pltpu.make_async_copy(vv_hbm.at[:, pl.ds(at, CW)], vbuf.at[slot], v_sem.at[slot])

    load_t = pltpu.make_async_copy(t_hbm, t32, in_sem.at[0])
    load_d = pltpu.make_async_copy(d_hbm, d32, in_sem.at[1])
    load_vo = pltpu.make_async_copy(vo_hbm, vo, in_sem.at[2])
    load_w = pltpu.make_async_copy(w_hbm, wv, in_sem.at[3])
    load_tail = pltpu.make_async_copy(vv_hbm.at[:, pl.ds(NCH * CW, TW)], vtail, in_sem.at[4])
    load_oo = pltpu.make_async_copy(oo_hbm.at[pl.ds(pl.multiple_of(r * RB, RB), RB)], oo, in_sem.at[5])
    load_t.start()
    load_w.start()
    load_d.start()
    load_vo.start()
    load_tail.start()
    load_oo.start()
    load_v(0, 0).start()
    load_v(1, 1).start()

    barrier = pltpu.get_barrier_semaphore()
    for rr in range(4):
        for cc in range(4):
            pl.semaphore_signal(barrier, inc=1, device_id={"row": rr, "col": cc}, device_id_type=MESH)

    with scope("wait_t"):
        load_t.wait()
    for m in range(9):
        piece = t32[:, PB * m : PB * m + PB].astype(BF16)
        trow[c, :, PB * m : PB * m + PB] = piece
        tcol[r, :, PB * m : PB * m + PB] = piece
    with scope("barrier"):
        pl.semaphore_wait(barrier, 16)

    half = RB // 2
    halves = (slice(0, half), slice(half, RB))

    def row_copy(way, h):
        block, peer = ((c, c_y), (c, c_z), ((c_z, c_y), (c_y, c_z))[h])[way]
        piece = trow.at[block, halves[h]]
        return send(piece, piece, row_s.at[way, h], row_r.at[way, h], r, peer)

    row_extra = send(
        trow.at[c_y, halves[0]], trow.at[c_y, halves[0]], row_s.at[3, 0], row_r.at[2, 0], r, c_z
    )

    def row_wait(way, h):
        piece = trow.at[(c_y, c_z, c_d)[way], halves[h]]
        send(piece, piece, row_s.at[way, h], row_r.at[way, h], r, c_y).wait_recv()

    def col_piece(h):
        piece = tcol.at[r, halves[h]]
        return send(piece, piece, col_s.at[h], col_r.at[h], r_x, c)

    col_pair = send(tcol.at[r], tcol.at[r], col_s.at[2], col_r.at[2], r_k, c)
    col_relay = send(tcol.at[r_x], tcol.at[r_x], col_s.at[3], col_r.at[3], r_k, c)

    def lad_copy(slot, h):
        return send(trow.at[slot, halves[h]], tlad.at[r, halves[h]], lad_s.at[slot, h], lad_r.at[r, h], slot, c)

    def dispatch(slot, h):
        @pl.when(slot != r)
        def _():
            lad_copy(slot, h).start()

        @pl.when(slot == r)
        def _():
            tlad[r, halves[h]] = trow[slot, halves[h]]

    def lad_wait(slot, h):
        send(trow.at[0, halves[h]], tlad.at[slot, halves[h]], lad_s.at[slot, h], lad_r.at[slot, h], r, c).wait_recv()

    def lad_forward(slot, h):
        piece = tlad.at[slot, halves[h]]
        return send(piece, piece, fw_s.at[slot, h], lad_r.at[slot, h], r, c_y)

    gives = jnp.logical_and(x != z, k == y)

    def forward(h):
        @pl.when(gives)
        def _():
            for slot in (r_x, r_d):
                with scope("lad_f"):
                    lad_wait(slot, h)
                lad_forward(slot, h).start()

    @pl.when(x == z)
    def _():
        col_piece(0).start()

    for h in range(2):
        row_copy(0, h).start()
        row_copy(1, h).start()
        dispatch(c, h)
    col_pair.start()

    with scope("wait_w"):
        load_w.wait()

    def mixed(slot):
        for m in range(5):
            split_cols(lambda lo, hi: trow[slot, :, lo:hi].astype(F32), planes, m)
        for h in range(2):
            parts = []
            for j in range(8):
                parts += take_j(planes, 8 * h + j, 0, 4 * AB)
            tm[:, 1152 * h : 1152 * h + 1152] = jnp.concatenate(parts, axis=1).astype(BF16)
        block = lax.dot_general(tm[...], wv[...], (((1,), (1,)), ((), ())), preferred_element_type=F32)

        def put(at, rows, lanes, value):
            pt[slot, at : at + rows, lanes] = value

        pack(put, V, block)

    p_copy = send(pt, pr, p_s.at[0], p_r.at[0], c, r)
    p_out, p_on = [], []
    for q, slot in enumerate((c_y, c_d, c, c_z)):
        via, to, src = ((r_x, c), (c, r_x), slot) if q < 2 else ((r, c_z), (c_z, r), (c_z, c)[q - 2])
        p_out.append(send(pt.at[slot], prel.at[q], p_s.at[1 + q], p_r.at[1 + q], *via))
        p_on.append(send(prel.at[q], pr.at[src], p_s.at[5 + q], p_r.at[5 + q], *to))

    def p_start(q):
        @pl.when(x != z)
        def _():
            p_out[q].start()

    def relay(*quarters):
        for q in quarters:
            with scope("relay"):
                p_out[q].wait_recv()
            p_on[q].start()

    with scope("mixed_c"):
        mixed(c)

    with scope("row10"):
        row_wait(1, 0)

    @pl.when(x == z)
    def _():
        row_copy(2, 0).start()

    dispatch(c_z, 0)
    with scope("row00"):
        row_wait(0, 0)

    @pl.when(x == z)
    def _():
        row_extra.start()

    dispatch(c_y, 0)

    load_d.wait()
    for m in range(5):
        split_cols(lambda lo, hi: d32[:, lo:hi], planes, m)
    for cc in range(4):
        parts = []
        for j in range(4):
            parts += take_j(planes, 4 * cc + j, 0, 4 * AB)
        def put_d(at, rows, lanes, value):
            dsnd[cc, at : at + rows, lanes] = value

        pack(put_d, V, jnp.concatenate(parts, axis=1))
    drcv[c] = dsnd[c]

    with scope("row11"):
        row_wait(1, 1)
    dispatch(c_z, 1)
    with scope("row01"):
        row_wait(0, 1)
    row_copy(2, 1).start()
    dispatch(c_y, 1)
    d_copy = [
        send(dsnd.at[peer], drcv.at[c], d_s.at[q], d_r.at[q], r, peer) for q, peer in enumerate(col_peers)
    ]

    @pl.when(x == z)
    def _():
        col_piece(1).start()
        d_copy[0].start()

    p_start(2)
    forward(0)
    with scope("mixed_c_z"):
        mixed(c_z)
    p_start(3)
    with scope("row20"):
        row_wait(2, 0)
    forward(1)
    with scope("row21"):
        row_wait(2, 1)

    @pl.when(x != z)
    def _():
        dispatch(c_d, 0)
        dispatch(c_d, 1)

    with scope("mixed_c_y"):
        mixed(c_y)
    p_start(0)
    with scope("mixed_c_d"):
        mixed(c_d)
    p_start(1)

    q_copy = [send(xq, xqr.at[c], q_s.at[q], q_r.at[q], r, peer) for q, peer in enumerate(col_peers)]

    def hole_x():
        load_vo.wait()
        send(tcol.at[r_k], tcol.at[r_k], col_s.at[2], col_r.at[2], r_k, c).wait_recv()

        @pl.when(jnp.logical_and(x == z, r != c))
        def _():
            send(tcol.at[r_x], tcol.at[r_x], f_s.at[0], col_r.at[4], r_k, c).wait_recv()

        @pl.when(r != c)
        def _():
            send(tcol.at[r_d], tcol.at[r_d], col_s.at[3], col_r.at[3], r_k, c).wait_recv()

        xq[...] = lax.dot_general(
            vo[...], tcol[...].reshape(4 * RB, CB), (((1,), (1,)), ((), ())), preferred_element_type=F32
        )
        xqr[c] = xq[...]
        for copy in q_copy:
            copy.start()

    @pl.when(x != z)
    def _():
        with scope("col"):
            for h in range(2):
                piece = tcol.at[r_x, halves[h]]
                send(piece, piece, col_s.at[h], col_r.at[h], r_x, c).wait_recv()
        col_relay.start()
        with scope("hole_x"):
            hole_x()

    @pl.when(jnp.logical_not(gives))
    def _():
        for h in range(2):
            for slot in (r_x, r_d):
                with scope("lad"):
                    lad_wait(slot, h)

    for h in range(2):
        with scope("lad_k"):
            lad_wait(r_k, h)

    fwd = (
        send(tlad.at[r_d], tcol.at[r_d], f_s.at[0], col_r.at[4], r_k, c),
        send(tlad.at[r_x], tcol.at[r_x], f_s.at[1], col_r.at[3], r_k, c),
    )

    @pl.when(r == c)
    def _():
        for copy in fwd:
            copy.start()
        tcol[r_d] = tlad[r_d]
        tcol[r_x] = tlad[r_x]

    @pl.when(x == z)
    def _():
        relay(2)
        with scope("hole_x"):
            hole_x()

        d_copy[1].start()

        @pl.when(r != c)
        def _():
            p_copy.start()

        @pl.when(r == c)
        def _():
            pr[...] = pt[...]

    def w_copy(rr):
        return send(wt.at[RB * rr : RB * rr + RB], wblk.at[r], w_s.at[rr], w_r.at[r], rr, c)

    def hole_w():
        load_oo.wait()
        for q, peer in enumerate(col_peers):
            send(xq, xqr.at[peer], q_s.at[q], q_r.at[q], r, peer).wait_recv()
        x_sum = (xqr[0] + xqr[1]) + (xqr[2] + xqr[3])
        w_hole = oo[...].astype(F32) + 0.5 * x_sum
        wt[...] = w_hole.T.astype(BF16)
        wblk[r] = wt[pl.ds(pl.multiple_of(r * RB, RB), RB), :]
        for rr in range(4):

            @pl.when(r != rr)
            def _():
                w_copy(rr).start()

    def d2_copy(n):
        return send(acc.at[n, 1 - k], d2r.at[n], dd_s.at[n], dd_r.at[n], r_k, c)

    def xx_copy(n):
        return send(xsb.at[n], xrb.at[n], xx_s.at[n], xx_r.at[n], r_x, c)

    d2_tail = send(acct.at[1 - k], d2t, dd_s.at[NCH], dd_r.at[NCH], r_k, c)
    xx_tail = send(xst, xrt, xx_s.at[NCH], xx_r.at[NCH], r_x, c)

    def gather_w():
        with scope("w_in"):
            for rr in range(4):

                @pl.when(r != rr)
                def _():
                    send(wt.at[0:RB], wblk.at[rr], w_s.at[rr], w_r.at[rr], rr, c).wait_recv()

        wf[...] = jnp.concatenate([wblk[rr].astype(F32) for rr in range(4)], axis=1).astype(BF16)

    def close(lo, hi, landed):
        hole = jnp.dot(wf[...], tcol[:, :, lo:hi].reshape(4 * RB, hi - lo), preferred_element_type=F32)
        r1[:, lo:hi] = r1[:, lo:hi] + landed + hole + vo[:, lo:hi].astype(F32)

    def stripe_rows(m):
        return 32 if m < 4 else 16

    def l_copy(m, q):
        there = pl.ds(V * m, stripe_rows(m) * 9 // 2)
        peer = col_peers[q]
        return send(lsnd.at[peer, there], lrcv.at[c, there], l_s.at[m, q], l_r.at[m, q], r, peer)

    def stripe_out(m):
        for n in ((0, 1, 2), (3, 4), (5, 6), (7, 8), (9,))[m]:
            with scope("sum"):
                xx_copy(n).wait_recv()
            close(CW * n, CW * n + CW, xrb[n])
        if m == 4:
            xx_tail.wait_recv()
            close(NCH * CW, CB, xrt[...])
        split_cols(lambda lo, hi: r1[:, lo:hi], planes, m)
        rows = stripe_rows(m)
        for cc in range(4):
            parts = []
            for j in range(4):
                parts += take_j(planes, 4 * cc + j, RB * 8 * m, rows)

            def put_l(at, count, lanes, value):
                lsnd[cc, V * m + at : V * m + at + count, lanes] = value

            pack(put_l, rows, jnp.concatenate(parts, axis=1))
        there = slice(V * m, V * m + rows * 9 // 2)
        lrcv[c, there, :] = lsnd[c, there, :]
        for q in range(3):
            l_copy(m, q).start()

    load_tail.wait()
    part = jnp.dot(tlad[...].reshape(4 * RB, CB), vtail[...], preferred_element_type=F32)
    for rr in range(4):
        acct[rr % 2, rr // 2] = part[RB * rr : RB * rr + RB]
    d2_tail.start()

    def second(n):
        with scope("pair"):
            d2_copy(n).wait_recv()
        xsb[n] = acc[n, k, 1 - x] + d2r[n, 1 - x]
        at = pl.multiple_of(n * CW, CW)
        r1[:, pl.ds(at, CW)] = acc[n, k, x] + d2r[n, x]
        xx_copy(n).start()

    def ladder_step(n, carry):
        slot = n % 2
        with scope("wait_v"):
            load_v(n, slot).wait()
        with scope("dot"):
            for h in range(2):
                part = jnp.dot(
                    tlad[...].reshape(4 * RB, CB), vbuf[slot, :, 256 * h : 256 * h + 256], preferred_element_type=F32
                )
                for rr in range(4):
                    acc[n, rr % 2, rr // 2, :, 256 * h : 256 * h + 256] = part[RB * rr : RB * rr + RB]
        d2_copy(n).start()

        @pl.when(n + 2 < NCH)
        def _():
            load_v(n + 2, slot).start()

        @pl.when(n == 0)
        def _():
            d2_tail.wait_recv()
            xst[...] = acct[k, 1 - x] + d2t[1 - x]
            r1[:, NCH * CW : CB] = acct[k, x] + d2t[x]
            xx_tail.start()

        @pl.when(n > 0)
        def _():
            second(n - 1)

        @pl.when(jnp.logical_and(n == 1, x != z))
        def _():
            for copy in d_copy:
                copy.start()

        @pl.when(jnp.logical_and(n == 1, x == z))
        def _():
            relay(3)

        @pl.when(jnp.logical_and(n == 2, x == z))
        def _():
            d_copy[2].start()

        @pl.when(jnp.logical_and(n == 3, x == z))
        def _():
            relay(0)

        @pl.when(jnp.logical_and(n == 5, x == z))
        def _():
            relay(1)

        @pl.when(n == jnp.where(x == z, 4, 2))
        def _():
            with scope("hole_w"):
                hole_w()

        @pl.when(jnp.logical_and(n == 9, x != z))
        def _():
            gather_w()
            stripe_out(0)
            stripe_out(1)

        return carry

    lax.fori_loop(0, NCH, ladder_step, 0)
    second(NCH - 1)

    @pl.when(x == z)
    def _():
        gather_w()
        stripe_out(0)
        stripe_out(1)

    def order_rows(src, dst):
        for cc in range(4):
            for i in range(4):
                first = V * i + AB * cc
                for b in range(4):
                    dst[first : first + AB, 128 * b : 128 * b + 128] = src[cc, pl.ds(V * b + i, AB, stride=4), :]
                ends = src[cc, pl.ds(4 * V + i, AB // 2, stride=4), :]
                dst[first : first + AB // 2, 512:576] = ends[:, 0:64]
                dst[first + AB // 2 : first + AB, 512:576] = ends[:, 64:128]

    for m in range(2, 4):
        stripe_out(m)
    order_rows(pt, pp)
    with scope("mirror"):

        @pl.when(jnp.logical_and(x == z, r != c))
        def _():
            p_copy.wait_recv()

        @pl.when(x != z)
        def _():
            for copy in p_on:
                copy.wait_recv()

    order_rows(pr, r3)
    pp[...] = pp[...] + r3[...].T
    for q, peer in enumerate(col_peers):
        with scope("denom"):
            send(dsnd.at[peer], drcv.at[peer], d_s.at[q], d_r.at[q], r, peer).wait_recv()
    order_rows(drcv, r3)
    stripe_out(4)

    for m in range(5):
        rows = stripe_rows(m)
        for q, peer in enumerate(col_peers):
            there = pl.ds(V * m, rows * 9 // 2)
            with scope("regroup"):
                send(
                    lsnd.at[peer, there], lrcv.at[peer, there], l_s.at[m, q], l_r.at[m, q], r, peer
                ).wait_recv()
        for cc in range(4):
            for i in range(4):
                first = V * i + AB * cc + 8 * m
                n = rows // 4

                def finish(at, count, lanes, value):
                    there = slice(at, at + count)
                    out_ref[there, lanes] = (value + pp[there, lanes]) / r3[there, lanes]

                for b in range(4):
                    part = lrcv[cc, pl.ds(V * m + rows * b + i, n, stride=4), :]
                    finish(first, n, slice(128 * b, 128 * b + 128), part)
                ends = lrcv[cc, pl.ds(V * m + 4 * rows + i, n // 2, stride=4), :]
                finish(first, n // 2, slice(512, 576), ends[:, 0:64])
                finish(first + n // 2, n // 2, slice(512, 576), ends[:, 64:128])

    for copy in (col_pair, *q_copy, *d_copy, d2_tail, xx_tail):
        copy.wait_send()
    for m in range(5):
        for q in range(3):
            l_copy(m, q).wait_send()
    for way, h in ((0, 0), (0, 1), (1, 0), (1, 1), (2, 1)):
        row_copy(way, h).wait_send()

    @pl.when(x == z)
    def _():
        row_copy(2, 0).wait_send()
        row_extra.wait_send()
        for h in range(2):
            col_piece(h).wait_send()
        for copy in p_on:
            copy.wait_send()

    @pl.when(jnp.logical_and(x == z, r != c))
    def _():
        p_copy.wait_send()

    @pl.when(x != z)
    def _():
        col_relay.wait_send()
        for copy in p_out:
            copy.wait_send()

    @pl.when(r == c)
    def _():
        for copy in fwd:
            copy.wait_send()

    @pl.when(gives)
    def _():
        for h in range(2):
            for slot in (r_x, r_d):
                lad_forward(slot, h).wait_send()

    for slot in range(4):

        @pl.when(slot != r)
        def _():
            w_copy(slot).wait_send()

        @pl.when(jnp.logical_and(slot != r, jnp.logical_or(slot != c_d, x != z)))
        def _():
            for h in range(2):
                lad_copy(slot, h).wait_send()

    def drain(n, carry):
        d2_copy(n).wait_send()
        xx_copy(n).wait_send()
        return carry

    lax.fori_loop(0, NCH, drain, 0)


def solution(mesh):
    vm = pltpu.VMEM
    dma = pltpu.SemaphoreType.DMA
    scratch = [
        vm((RB, CB), F32), vm((RB, CB), F32), vm((RB, CB), BF16), vm((PB, O * V), BF16),
        vm((4, RB, CB), BF16), vm((4, RB, CB), BF16), vm((4, RB, CB), BF16),
        vm((2, AB * RB, 128), F32), vm((V, O * V), BF16),
        vm((PB, PB), F32), vm((PB, PB), F32), vm((4, PQ, 128), F32), vm((4, PQ, 128), F32),
        vm((4, PQ, 128), F32), vm((4, PQ, 128), F32), vm((4, PQ, 128), F32), vm((4, PQ, 128), F32),
        vm((4, PQ, 128), F32),
        vm((RB, O * O), F32), vm((4, RB, O * O), F32), vm((O * O, RB), BF16), vm((RB, O * O), BF16), vm((4, RB, RB), BF16), vm((RB, O * O), BF16),
        vm((2, CB, CW), BF16), vm((CB, TW), BF16),
        vm((NCH, 2, 2, RB, CW), F32), vm((NCH, 2, RB, CW), F32), vm((NCH, RB, CW), F32), vm((NCH, RB, CW), F32),
        vm((2, 2, RB, TW), F32), vm((2, RB, TW), F32), vm((RB, TW), F32), vm((RB, TW), F32),
        vm((RB, CB), F32),
        dma((6,)), dma((2,)), dma((4, 2)), dma((4, 2)), dma((5,)), dma((5,)), dma((4, 2)), dma((4, 2)),
        dma((3,)), dma((3,)), dma((3,)), dma((3,)), dma((5, 3)), dma((5, 3)), dma((9,)), dma((9,)), dma((4, 2)),
        dma((NCH + 1,)), dma((NCH + 1,)), dma((NCH + 1,)), dma((NCH + 1,)), dma((4,)), dma((4,)), dma((2,)),
    ]
    hbm = pl.BlockSpec(memory_space=pl.ANY)
    vmem = pl.BlockSpec(memory_space=pltpu.VMEM)
    call = pl.pallas_call(
        kernel,
        out_shape=jax.ShapeDtypeStruct((PB, PB), F32),
        in_specs=[hbm] * 6,
        out_specs=vmem,
        scratch_shapes=scratch,
        compiler_params=pltpu.CompilerParams(
            collective_id=0, has_side_effects=True, vmem_limit_bytes=67_000_000
        ),
        name="sweep",
    )
    def local_sweep(t_blk, d_blk, voovv_blk, vvvvv_blk, oooo, w_blk):
        return call(t_blk, d_blk, voovv_blk, vvvvv_blk, oooo, w_blk.T)

    return jax.shard_map(
        local_sweep,
        mesh=mesh,
        in_specs=(P("row", "col"), P("row", "col"), P("row", "col"), P("row", "col"), P(None, None), P(None, "col")),
        out_specs=P("row", "col"),
        check_vma=False,
    )
```

```python
import functools

import jax
import jax.numpy as jnp
from jax import lax
from jax.experimental import pallas as pl
from jax.experimental.pallas import tpu as pltpu
from jax.sharding import PartitionSpec as P

MESH = pl.DeviceIdType.MESH
scope = jax.named_scope
F32 = jnp.float32
BF16 = jnp.bfloat16

O = 16
V = 144
RB = 64
CB = 5184
AB = 36
PQ = 648
PB = 576
CW = 512
NCH = CB // CW
TW = CB - NCH * CW


def stripe(load, m, q):
    first = 1152 * m + V * q
    low = first // 128 * 128
    high = min(-(-(first + V) // 128) * 128, CB)
    return load(low, high)[:, first - low : first - low + V]


def split_cols(load, planes, m):
    for q in range(8 if m < 4 else 4):
        piece = stripe(load, m, q)
        base = RB * (8 * m + q)
        planes[0, base : base + RB, :] = piece[:, 0:128]
        planes[1, base : base + RB, 0:16] = piece[:, 128:144]


def take_j(planes, j, base, rows):
    wide = planes[0, pl.ds(base + j, rows, stride=16), :]
    rest = planes[1, pl.ds(base + j, rows, stride=16), :]
    return [wide, rest[:, 0:16]]


def pack(put, rows, wide):
    for b in range(4):
        put(rows * b, rows, slice(0, 128), wide[:, 128 * b : 128 * b + 128])
    put(4 * rows, rows // 2, slice(0, 64), wide[: rows // 2, 512:576])
    put(4 * rows, rows // 2, slice(64, 128), wide[rows // 2 :, 512:576])


def kernel(
    t_hbm, d_hbm, vo_hbm, vv_hbm, oo_hbm, w_hbm, out_ref,
    t32, d32, vo, wv, trow, tcol, tlad, planes, tm, r3, pp, pt, pr,
    dsnd, drcv, lsnd, lrcv, prel, xq, xqr, wt, oo, wblk, wf, vbuf, vtail,
    acc, d2r, xsb, xrb, acct, d2t, xst, xrt, r1,
    in_sem, v_sem, row_s, row_r, col_s, col_r, lad_s, lad_r, q_s, q_r,
    d_s, d_r, l_s, l_r, p_s, p_r, fw_s, dd_s, dd_r, xx_s, xx_r, w_s, w_r, f_s,
):
    r = lax.axis_index("row")
    c = lax.axis_index("col")
    x, k = r // 2, r % 2
    z, y = c // 2, c % 2
    r_k, r_x = 2 * x + 1 - k, 2 * (1 - x) + k
    r_d = 2 * (1 - x) + 1 - k
    c_y, c_z = 2 * z + 1 - y, 2 * (1 - z) + y
    c_d = 2 * (1 - z) + 1 - y
    col_peers = (c_y, c_z, c_d)

    def send(src, dst, ss, rs, row, col):
        return pltpu.make_async_remote_copy(
            src_ref=src, dst_ref=dst, send_sem=ss, recv_sem=rs,
            device_id={"row": row, "col": col}, device_id_type=MESH,
        )

    def load_v(n, slot):
        at = pl.multiple_of(n * CW, CW)
        return pltpu.make_async_copy(vv_hbm.at[:, pl.ds(at, CW)], vbuf.at[slot], v_sem.at[slot])

    load_t = pltpu.make_async_copy(t_hbm, t32, in_sem.at[0])
    load_d = pltpu.make_async_copy(d_hbm, d32, in_sem.at[1])
    load_vo = pltpu.make_async_copy(vo_hbm, vo, in_sem.at[2])
    load_w = pltpu.make_async_copy(w_hbm, wv, in_sem.at[3])
    load_tail = pltpu.make_async_copy(vv_hbm.at[:, pl.ds(NCH * CW, TW)], vtail, in_sem.at[4])
    load_oo = pltpu.make_async_copy(oo_hbm.at[pl.ds(pl.multiple_of(r * RB, RB), RB)], oo, in_sem.at[5])
    load_t.start()
    load_w.start()
    load_d.start()
    load_vo.start()
    load_tail.start()
    load_oo.start()
    load_v(0, 0).start()
    load_v(1, 1).start()

    barrier = pltpu.get_barrier_semaphore()
    for rr in range(4):
        for cc in range(4):
            pl.semaphore_signal(barrier, inc=1, device_id={"row": rr, "col": cc}, device_id_type=MESH)

    with scope("wait_t"):
        load_t.wait()
    for m in range(9):
        piece = t32[:, PB * m : PB * m + PB].astype(BF16)
        trow[c, :, PB * m : PB * m + PB] = piece
        tcol[r, :, PB * m : PB * m + PB] = piece
    with scope("barrier"):
        pl.semaphore_wait(barrier, 16)

    half = RB // 2
    halves = (slice(0, half), slice(half, RB))

    def row_copy(way, h):
        block, peer = ((c, c_y), (c, c_z), ((c_z, c_y), (c_y, c_z))[h])[way]
        piece = trow.at[block, halves[h]]
        return send(piece, piece, row_s.at[way, h], row_r.at[way, h], r, peer)

    row_extra = send(
        trow.at[c_y, halves[0]], trow.at[c_y, halves[0]], row_s.at[3, 0], row_r.at[2, 0], r, c_z
    )

    def row_wait(way, h):
        piece = trow.at[(c_y, c_z, c_d)[way], halves[h]]
        send(piece, piece, row_s.at[way, h], row_r.at[way, h], r, c_y).wait_recv()

    def col_piece(h):
        piece = tcol.at[r, halves[h]]
        return send(piece, piece, col_s.at[h], col_r.at[h], r_x, c)

    col_pair = send(tcol.at[r], tcol.at[r], col_s.at[2], col_r.at[2], r_k, c)
    col_relay = send(tcol.at[r_x], tcol.at[r_x], col_s.at[3], col_r.at[3], r_k, c)

    def lad_copy(slot, h):
        return send(trow.at[slot, halves[h]], tlad.at[r, halves[h]], lad_s.at[slot, h], lad_r.at[r, h], slot, c)

    def dispatch(slot, h):
        @pl.when(slot != r)
        def _():
            lad_copy(slot, h).start()

        @pl.when(slot == r)
        def _():
            tlad[r, halves[h]] = trow[slot, halves[h]]

    def lad_wait(slot, h):
        send(trow.at[0, halves[h]], tlad.at[slot, halves[h]], lad_s.at[slot, h], lad_r.at[slot, h], r, c).wait_recv()

    def lad_forward(slot, h):
        piece = tlad.at[slot, halves[h]]
        return send(piece, piece, fw_s.at[slot, h], lad_r.at[slot, h], r, c_y)

    gives = jnp.logical_and(x != z, k == y)

    def forward(h):
        @pl.when(gives)
        def _():
            for slot in (r_x, r_d):
                with scope("lad_f"):
                    lad_wait(slot, h)
                lad_forward(slot, h).start()

    @pl.when(x == z)
    def _():
        col_piece(0).start()

    for h in range(2):
        row_copy(0, h).start()
        row_copy(1, h).start()
        dispatch(c, h)
    col_pair.start()

    with scope("wait_w"):
        load_w.wait()

    def mixed(slot):
        for m in range(5):
            split_cols(lambda lo, hi: trow[slot, :, lo:hi].astype(F32), planes, m)
        for h in range(2):
            parts = []
            for j in range(8):
                parts += take_j(planes, 8 * h + j, 0, 4 * AB)
            tm[:, 1152 * h : 1152 * h + 1152] = jnp.concatenate(parts, axis=1).astype(BF16)
        block = lax.dot_general(tm[...], wv[...], (((1,), (1,)), ((), ())), preferred_element_type=F32)

        def put(at, rows, lanes, value):
            pt[slot, at : at + rows, lanes] = value

        pack(put, V, block)

    p_copy = send(pt, pr, p_s.at[0], p_r.at[0], c, r)
    p_out, p_on = [], []
    for q, slot in enumerate((c_y, c_d, c, c_z)):
        via, to, src = ((r_x, c), (c, r_x), slot) if q < 2 else ((r, c_z), (c_z, r), (c_z, c)[q - 2])
        p_out.append(send(pt.at[slot], prel.at[q], p_s.at[1 + q], p_r.at[1 + q], *via))
        p_on.append(send(prel.at[q], pr.at[src], p_s.at[5 + q], p_r.at[5 + q], *to))

    def p_start(q):
        @pl.when(x != z)
        def _():
            p_out[q].start()

    def relay(*quarters):
        for q in quarters:
            with scope("relay"):
                p_out[q].wait_recv()
            p_on[q].start()

    with scope("mixed_c"):
        mixed(c)

    with scope("row10"):
        row_wait(1, 0)

    @pl.when(x == z)
    def _():
        row_copy(2, 0).start()

    dispatch(c_z, 0)
    with scope("row00"):
        row_wait(0, 0)

    @pl.when(x == z)
    def _():
        row_extra.start()

    dispatch(c_y, 0)

    load_d.wait()
    for m in range(5):
        split_cols(lambda lo, hi: d32[:, lo:hi], planes, m)
    for cc in range(4):
        parts = []
        for j in range(4):
            parts += take_j(planes, 4 * cc + j, 0, 4 * AB)
        def put_d(at, rows, lanes, value):
            dsnd[cc, at : at + rows, lanes] = value

        pack(put_d, V, jnp.concatenate(parts, axis=1))
    drcv[c] = dsnd[c]

    with scope("row11"):
        row_wait(1, 1)
    dispatch(c_z, 1)
    with scope("row01"):
        row_wait(0, 1)
    row_copy(2, 1).start()
    dispatch(c_y, 1)
    d_copy = [
        send(dsnd.at[peer], drcv.at[c], d_s.at[q], d_r.at[q], r, peer) for q, peer in enumerate(col_peers)
    ]

    @pl.when(x == z)
    def _():
        col_piece(1).start()
        d_copy[0].start()

    p_start(2)
    forward(0)
    with scope("mixed_c_z"):
        mixed(c_z)
    p_start(3)
    with scope("row20"):
        row_wait(2, 0)
    forward(1)
    with scope("row21"):
        row_wait(2, 1)

    @pl.when(x != z)
    def _():
        dispatch(c_d, 0)
        dispatch(c_d, 1)

    with scope("mixed_c_y"):
        mixed(c_y)
    p_start(0)
    with scope("mixed_c_d"):
        mixed(c_d)
    p_start(1)

    q_copy = [send(xq, xqr.at[c], q_s.at[q], q_r.at[q], r, peer) for q, peer in enumerate(col_peers)]

    def hole_x():
        load_vo.wait()
        send(tcol.at[r_k], tcol.at[r_k], col_s.at[2], col_r.at[2], r_k, c).wait_recv()

        @pl.when(jnp.logical_and(x == z, r != c))
        def _():
            send(tcol.at[r_x], tcol.at[r_x], f_s.at[0], col_r.at[4], r_k, c).wait_recv()

        @pl.when(r != c)
        def _():
            send(tcol.at[r_d], tcol.at[r_d], col_s.at[3], col_r.at[3], r_k, c).wait_recv()

        xq[...] = lax.dot_general(
            vo[...], tcol[...].reshape(4 * RB, CB), (((1,), (1,)), ((), ())), preferred_element_type=F32
        )
        xqr[c] = xq[...]
        for copy in q_copy:
            copy.start()

    @pl.when(x != z)
    def _():
        with scope("col"):
            for h in range(2):
                piece = tcol.at[r_x, halves[h]]
                send(piece, piece, col_s.at[h], col_r.at[h], r_x, c).wait_recv()
        col_relay.start()
        with scope("hole_x"):
            hole_x()

    @pl.when(jnp.logical_not(gives))
    def _():
        for h in range(2):
            for slot in (r_x, r_d):
                with scope("lad"):
                    lad_wait(slot, h)

    for h in range(2):
        with scope("lad_k"):
            lad_wait(r_k, h)

    fwd = (
        send(tlad.at[r_d], tcol.at[r_d], f_s.at[0], col_r.at[4], r_k, c),
        send(tlad.at[r_x], tcol.at[r_x], f_s.at[1], col_r.at[3], r_k, c),
    )

    @pl.when(r == c)
    def _():
        for copy in fwd:
            copy.start()
        tcol[r_d] = tlad[r_d]
        tcol[r_x] = tlad[r_x]

    @pl.when(x == z)
    def _():
        with scope("hole_x"):
            hole_x()

        d_copy[1].start()

        @pl.when(r != c)
        def _():
            p_copy.start()

        @pl.when(r == c)
        def _():
            pr[...] = pt[...]

    def w_copy(rr):
        return send(wt.at[RB * rr : RB * rr + RB], wblk.at[r], w_s.at[rr], w_r.at[r], rr, c)

    def hole_w():
        load_oo.wait()
        for q, peer in enumerate(col_peers):
            send(xq, xqr.at[peer], q_s.at[q], q_r.at[q], r, peer).wait_recv()
        x_sum = (xqr[0] + xqr[1]) + (xqr[2] + xqr[3])
        w_hole = oo[...].astype(F32) + 0.5 * x_sum
        wt[...] = w_hole.T.astype(BF16)
        wblk[r] = wt[pl.ds(pl.multiple_of(r * RB, RB), RB), :]
        for rr in range(4):

            @pl.when(r != rr)
            def _():
                w_copy(rr).start()

    def d2_copy(n):
        return send(acc.at[n, 1 - k], d2r.at[n], dd_s.at[n], dd_r.at[n], r_k, c)

    def xx_copy(n):
        return send(xsb.at[n], xrb.at[n], xx_s.at[n], xx_r.at[n], r_x, c)

    d2_tail = send(acct.at[1 - k], d2t, dd_s.at[NCH], dd_r.at[NCH], r_k, c)
    xx_tail = send(xst, xrt, xx_s.at[NCH], xx_r.at[NCH], r_x, c)

    def gather_w():
        with scope("w_in"):
            for rr in range(4):

                @pl.when(r != rr)
                def _():
                    send(wt.at[0:RB], wblk.at[rr], w_s.at[rr], w_r.at[rr], rr, c).wait_recv()

        wf[...] = jnp.concatenate([wblk[rr].astype(F32) for rr in range(4)], axis=1).astype(BF16)

    def close(lo, hi, landed):
        hole = jnp.dot(wf[...], tcol[:, :, lo:hi].reshape(4 * RB, hi - lo), preferred_element_type=F32)
        r1[:, lo:hi] = r1[:, lo:hi] + landed + hole + vo[:, lo:hi].astype(F32)

    def stripe_rows(m):
        return 32 if m < 4 else 16

    def l_copy(m, q):
        there = pl.ds(V * m, stripe_rows(m) * 9 // 2)
        peer = col_peers[q]
        return send(lsnd.at[peer, there], lrcv.at[c, there], l_s.at[m, q], l_r.at[m, q], r, peer)

    def stripe_out(m):
        for n in ((0, 1, 2), (3, 4), (5, 6), (7, 8), (9,))[m]:
            with scope("sum"):
                xx_copy(n).wait_recv()
            close(CW * n, CW * n + CW, xrb[n])
        if m == 4:
            xx_tail.wait_recv()
            close(NCH * CW, CB, xrt[...])
        split_cols(lambda lo, hi: r1[:, lo:hi], planes, m)
        rows = stripe_rows(m)
        for cc in range(4):
            parts = []
            for j in range(4):
                parts += take_j(planes, 4 * cc + j, RB * 8 * m, rows)

            def put_l(at, count, lanes, value):
                lsnd[cc, V * m + at : V * m + at + count, lanes] = value

            pack(put_l, rows, jnp.concatenate(parts, axis=1))
        there = slice(V * m, V * m + rows * 9 // 2)
        lrcv[c, there, :] = lsnd[c, there, :]
        for q in range(3):
            l_copy(m, q).start()

    load_tail.wait()
    part = jnp.dot(tlad[...].reshape(4 * RB, CB), vtail[...], preferred_element_type=F32)
    for rr in range(4):
        acct[rr % 2, rr // 2] = part[RB * rr : RB * rr + RB]
    d2_tail.start()

    def second(n):
        with scope("pair"):
            d2_copy(n).wait_recv()
        xsb[n] = acc[n, k, 1 - x] + d2r[n, 1 - x]
        at = pl.multiple_of(n * CW, CW)
        r1[:, pl.ds(at, CW)] = acc[n, k, x] + d2r[n, x]
        xx_copy(n).start()

    def ladder_step(n, carry):
        slot = n % 2
        with scope("wait_v"):
            load_v(n, slot).wait()
        with scope("dot"):
            for h in range(2):
                part = jnp.dot(
                    tlad[...].reshape(4 * RB, CB), vbuf[slot, :, 256 * h : 256 * h + 256], preferred_element_type=F32
                )
                for rr in range(4):
                    acc[n, rr % 2, rr // 2, :, 256 * h : 256 * h + 256] = part[RB * rr : RB * rr + RB]
        d2_copy(n).start()

        @pl.when(n + 2 < NCH)
        def _():
            load_v(n + 2, slot).start()

        @pl.when(n == 0)
        def _():
            d2_tail.wait_recv()
            xst[...] = acct[k, 1 - x] + d2t[1 - x]
            r1[:, NCH * CW : CB] = acct[k, x] + d2t[x]
            xx_tail.start()

        @pl.when(n > 0)
        def _():
            second(n - 1)

        @pl.when(jnp.logical_and(n == 1, x != z))
        def _():
            for copy in d_copy:
                copy.start()

        @pl.when(jnp.logical_and(n == 1, x == z))
        def _():
            relay(2)

        @pl.when(jnp.logical_and(n == 2, x == z))
        def _():
            d_copy[2].start()

        @pl.when(jnp.logical_and(n == 3, x == z))
        def _():
            relay(0)

        @pl.when(jnp.logical_and(n == 5, x == z))
        def _():
            relay(1)

        @pl.when(n == jnp.where(x == z, 4, 2))
        def _():
            with scope("hole_w"):
                hole_w()

        @pl.when(jnp.logical_and(n == 9, x != z))
        def _():
            gather_w()
            stripe_out(0)
            stripe_out(1)

        return carry

    lax.fori_loop(0, NCH, ladder_step, 0)
    second(NCH - 1)

    @pl.when(x == z)
    def _():
        relay(3)
        gather_w()
        stripe_out(0)
        stripe_out(1)

    def order_rows(src, dst):
        for cc in range(4):
            for i in range(4):
                first = V * i + AB * cc
                for b in range(4):
                    dst[first : first + AB, 128 * b : 128 * b + 128] = src[cc, pl.ds(V * b + i, AB, stride=4), :]
                ends = src[cc, pl.ds(4 * V + i, AB // 2, stride=4), :]
                dst[first : first + AB // 2, 512:576] = ends[:, 0:64]
                dst[first + AB // 2 : first + AB, 512:576] = ends[:, 64:128]

    for m in range(2, 4):
        stripe_out(m)
    order_rows(pt, pp)
    with scope("mirror"):

        @pl.when(jnp.logical_and(x == z, r != c))
        def _():
            p_copy.wait_recv()

        @pl.when(x != z)
        def _():
            for copy in p_on:
                copy.wait_recv()

    order_rows(pr, r3)
    pp[...] = pp[...] + r3[...].T
    for q, peer in enumerate(col_peers):
        with scope("denom"):
            send(dsnd.at[peer], drcv.at[peer], d_s.at[q], d_r.at[q], r, peer).wait_recv()
    order_rows(drcv, r3)
    stripe_out(4)

    for m in range(5):
        rows = stripe_rows(m)
        for q, peer in enumerate(col_peers):
            there = pl.ds(V * m, rows * 9 // 2)
            with scope("regroup"):
                send(
                    lsnd.at[peer, there], lrcv.at[peer, there], l_s.at[m, q], l_r.at[m, q], r, peer
                ).wait_recv()
        for cc in range(4):
            for i in range(4):
                first = V * i + AB * cc + 8 * m
                n = rows // 4

                def finish(at, count, lanes, value):
                    there = slice(at, at + count)
                    out_ref[there, lanes] = (value + pp[there, lanes]) / r3[there, lanes]

                for b in range(4):
                    part = lrcv[cc, pl.ds(V * m + rows * b + i, n, stride=4), :]
                    finish(first, n, slice(128 * b, 128 * b + 128), part)
                ends = lrcv[cc, pl.ds(V * m + 4 * rows + i, n // 2, stride=4), :]
                finish(first, n // 2, slice(512, 576), ends[:, 0:64])
                finish(first + n // 2, n // 2, slice(512, 576), ends[:, 64:128])

    for copy in (col_pair, *q_copy, *d_copy, d2_tail, xx_tail):
        copy.wait_send()
    for m in range(5):
        for q in range(3):
            l_copy(m, q).wait_send()
    for way, h in ((0, 0), (0, 1), (1, 0), (1, 1), (2, 1)):
        row_copy(way, h).wait_send()

    @pl.when(x == z)
    def _():
        row_copy(2, 0).wait_send()
        row_extra.wait_send()
        for h in range(2):
            col_piece(h).wait_send()
        for copy in p_on:
            copy.wait_send()

    @pl.when(jnp.logical_and(x == z, r != c))
    def _():
        p_copy.wait_send()

    @pl.when(x != z)
    def _():
        col_relay.wait_send()
        for copy in p_out:
            copy.wait_send()

    @pl.when(r == c)
    def _():
        for copy in fwd:
            copy.wait_send()

    @pl.when(gives)
    def _():
        for h in range(2):
            for slot in (r_x, r_d):
                lad_forward(slot, h).wait_send()

    for slot in range(4):

        @pl.when(slot != r)
        def _():
            w_copy(slot).wait_send()

        @pl.when(jnp.logical_and(slot != r, jnp.logical_or(slot != c_d, x != z)))
        def _():
            for h in range(2):
                lad_copy(slot, h).wait_send()

    def drain(n, carry):
        d2_copy(n).wait_send()
        xx_copy(n).wait_send()
        return carry

    lax.fori_loop(0, NCH, drain, 0)


def solution(mesh):
    vm = pltpu.VMEM
    dma = pltpu.SemaphoreType.DMA
    scratch = [
        vm((RB, CB), F32), vm((RB, CB), F32), vm((RB, CB), BF16), vm((PB, O * V), BF16),
        vm((4, RB, CB), BF16), vm((4, RB, CB), BF16), vm((4, RB, CB), BF16),
        vm((2, AB * RB, 128), F32), vm((V, O * V), BF16),
        vm((PB, PB), F32), vm((PB, PB), F32), vm((4, PQ, 128), F32), vm((4, PQ, 128), F32),
        vm((4, PQ, 128), F32), vm((4, PQ, 128), F32), vm((4, PQ, 128), F32), vm((4, PQ, 128), F32),
        vm((4, PQ, 128), F32),
        vm((RB, O * O), F32), vm((4, RB, O * O), F32), vm((O * O, RB), BF16), vm((RB, O * O), BF16), vm((4, RB, RB), BF16), vm((RB, O * O), BF16),
        vm((2, CB, CW), BF16), vm((CB, TW), BF16),
        vm((NCH, 2, 2, RB, CW), F32), vm((NCH, 2, RB, CW), F32), vm((NCH, RB, CW), F32), vm((NCH, RB, CW), F32),
        vm((2, 2, RB, TW), F32), vm((2, RB, TW), F32), vm((RB, TW), F32), vm((RB, TW), F32),
        vm((RB, CB), F32),
        dma((6,)), dma((2,)), dma((4, 2)), dma((4, 2)), dma((5,)), dma((5,)), dma((4, 2)), dma((4, 2)),
        dma((3,)), dma((3,)), dma((3,)), dma((3,)), dma((5, 3)), dma((5, 3)), dma((9,)), dma((9,)), dma((4, 2)),
        dma((NCH + 1,)), dma((NCH + 1,)), dma((NCH + 1,)), dma((NCH + 1,)), dma((4,)), dma((4,)), dma((2,)),
    ]
    hbm = pl.BlockSpec(memory_space=pl.ANY)
    vmem = pl.BlockSpec(memory_space=pltpu.VMEM)
    call = pl.pallas_call(
        kernel,
        out_shape=jax.ShapeDtypeStruct((PB, PB), F32),
        in_specs=[hbm] * 6,
        out_specs=vmem,
        scratch_shapes=scratch,
        compiler_params=pltpu.CompilerParams(
            collective_id=0, has_side_effects=True, vmem_limit_bytes=67_000_000
        ),
        name="sweep",
    )
    def local_sweep(t_blk, d_blk, voovv_blk, vvvvv_blk, oooo, w_blk):
        return call(t_blk, d_blk, voovv_blk, vvvvv_blk, oooo, w_blk.T)

    return jax.shard_map(
        local_sweep,
        mesh=mesh,
        in_specs=(P("row", "col"), P("row", "col"), P("row", "col"), P("row", "col"), P(None, None), P(None, "col")),
        out_specs=P("row", "col"),
        check_vma=False,
    )
```

```python
import functools

import jax
import jax.numpy as jnp
from jax import lax
from jax.experimental import pallas as pl
from jax.experimental.pallas import tpu as pltpu
from jax.sharding import PartitionSpec as P

MESH = pl.DeviceIdType.MESH
scope = jax.named_scope
F32 = jnp.float32
BF16 = jnp.bfloat16

O = 16
V = 144
RB = 64
CB = 5184
AB = 36
PQ = 648
PB = 576
CW = 512
NCH = CB // CW
TW = CB - NCH * CW


def stripe(load, m, q):
    first = 1152 * m + V * q
    low = first // 128 * 128
    high = min(-(-(first + V) // 128) * 128, CB)
    return load(low, high)[:, first - low : first - low + V]


def split_cols(load, planes, m):
    for q in range(8 if m < 4 else 4):
        piece = stripe(load, m, q)
        base = RB * (8 * m + q)
        planes[0, base : base + RB, :] = piece[:, 0:128]
        planes[1, base : base + RB, 0:16] = piece[:, 128:144]


def take_j(planes, j, base, rows):
    wide = planes[0, pl.ds(base + j, rows, stride=16), :]
    rest = planes[1, pl.ds(base + j, rows, stride=16), :]
    return [wide, rest[:, 0:16]]


def pack(put, rows, wide):
    for b in range(4):
        put(rows * b, rows, slice(0, 128), wide[:, 128 * b : 128 * b + 128])
    put(4 * rows, rows // 2, slice(0, 64), wide[: rows // 2, 512:576])
    put(4 * rows, rows // 2, slice(64, 128), wide[rows // 2 :, 512:576])


def kernel(
    t_hbm, d_hbm, vo_hbm, vv_hbm, oo_hbm, w_hbm, out_ref,
    t32, d32, vo, wv, trow, tcol, tlad, planes, tm, r3, pp, pt, pr,
    dsnd, drcv, lsnd, lrcv, prel, xq, xqr, wt, oo, wblk, wf, vbuf, vtail,
    acc, d2r, xsb, xrb, acct, d2t, xst, xrt, r1,
    in_sem, v_sem, row_s, row_r, col_s, col_r, lad_s, lad_r, q_s, q_r,
    d_s, d_r, l_s, l_r, p_s, p_r, fw_s, dd_s, dd_r, xx_s, xx_r, w_s, w_r, f_s,
):
    r = lax.axis_index("row")
    c = lax.axis_index("col")
    x, k = r // 2, r % 2
    z, y = c // 2, c % 2
    r_k, r_x = 2 * x + 1 - k, 2 * (1 - x) + k
    r_d = 2 * (1 - x) + 1 - k
    c_y, c_z = 2 * z + 1 - y, 2 * (1 - z) + y
    c_d = 2 * (1 - z) + 1 - y
    col_peers = (c_y, c_z, c_d)

    def send(src, dst, ss, rs, row, col):
        return pltpu.make_async_remote_copy(
            src_ref=src, dst_ref=dst, send_sem=ss, recv_sem=rs,
            device_id={"row": row, "col": col}, device_id_type=MESH,
        )

    def load_v(n, slot):
        at = pl.multiple_of(n * CW, CW)
        return pltpu.make_async_copy(vv_hbm.at[:, pl.ds(at, CW)], vbuf.at[slot], v_sem.at[slot])

    load_t = pltpu.make_async_copy(t_hbm, t32, in_sem.at[0])
    load_d = pltpu.make_async_copy(d_hbm, d32, in_sem.at[1])
    load_vo = pltpu.make_async_copy(vo_hbm, vo, in_sem.at[2])
    load_w = pltpu.make_async_copy(w_hbm, wv, in_sem.at[3])
    load_tail = pltpu.make_async_copy(vv_hbm.at[:, pl.ds(NCH * CW, TW)], vtail, in_sem.at[4])
    load_oo = pltpu.make_async_copy(oo_hbm.at[pl.ds(pl.multiple_of(r * RB, RB), RB)], oo, in_sem.at[5])
    load_t.start()
    load_w.start()
    load_d.start()
    load_vo.start()
    load_tail.start()
    load_oo.start()
    load_v(0, 0).start()
    load_v(1, 1).start()

    barrier = pltpu.get_barrier_semaphore()
    for rr in range(4):
        for cc in range(4):
            pl.semaphore_signal(barrier, inc=1, device_id={"row": rr, "col": cc}, device_id_type=MESH)

    with scope("wait_t"):
        load_t.wait()
    for m in range(9):
        piece = t32[:, PB * m : PB * m + PB].astype(BF16)
        trow[c, :, PB * m : PB * m + PB] = piece
        tcol[r, :, PB * m : PB * m + PB] = piece
    with scope("barrier"):
        pl.semaphore_wait(barrier, 16)

    half = RB // 2
    halves = (slice(0, half), slice(half, RB))

    def row_copy(way, h):
        block, peer = ((c, c_y), (c, c_z), ((c_z, c_y), (c_y, c_z))[h])[way]
        piece = trow.at[block, halves[h]]
        return send(piece, piece, row_s.at[way, h], row_r.at[way, h], r, peer)

    row_extra = send(
        trow.at[c_y, halves[0]], trow.at[c_y, halves[0]], row_s.at[3, 0], row_r.at[2, 0], r, c_z
    )

    def row_wait(way, h):
        piece = trow.at[(c_y, c_z, c_d)[way], halves[h]]
        send(piece, piece, row_s.at[way, h], row_r.at[way, h], r, c_y).wait_recv()

    def col_piece(h):
        piece = tcol.at[r, halves[h]]
        return send(piece, piece, col_s.at[h], col_r.at[h], r_x, c)

    col_pair = send(tcol.at[r], tcol.at[r], col_s.at[2], col_r.at[2], r_k, c)
    col_relay = send(tcol.at[r_x], tcol.at[r_x], col_s.at[3], col_r.at[3], r_k, c)

    def lad_copy(slot, h):
        return send(trow.at[slot, halves[h]], tlad.at[r, halves[h]], lad_s.at[slot, h], lad_r.at[r, h], slot, c)

    def dispatch(slot, h):
        @pl.when(slot != r)
        def _():
            lad_copy(slot, h).start()

        @pl.when(slot == r)
        def _():
            tlad[r, halves[h]] = trow[slot, halves[h]]

    def lad_wait(slot, h):
        send(trow.at[0, halves[h]], tlad.at[slot, halves[h]], lad_s.at[slot, h], lad_r.at[slot, h], r, c).wait_recv()

    def lad_forward(slot, h):
        piece = tlad.at[slot, halves[h]]
        return send(piece, piece, fw_s.at[slot, h], lad_r.at[slot, h], r, c_y)

    gives = jnp.logical_and(x != z, k == y)

    def forward(h):
        @pl.when(gives)
        def _():
            for slot in (r_x, r_d):
                with scope("lad_f"):
                    lad_wait(slot, h)
                lad_forward(slot, h).start()

    @pl.when(x == z)
    def _():
        col_piece(0).start()

    for h in range(2):
        row_copy(0, h).start()
        row_copy(1, h).start()
        dispatch(c, h)
    col_pair.start()

    with scope("wait_w"):
        load_w.wait()

    def mixed(slot):
        for m in range(5):
            split_cols(lambda lo, hi: trow[slot, :, lo:hi].astype(F32), planes, m)
        for h in range(2):
            parts = []
            for j in range(8):
                parts += take_j(planes, 8 * h + j, 0, 4 * AB)
            tm[:, 1152 * h : 1152 * h + 1152] = jnp.concatenate(parts, axis=1).astype(BF16)
        block = lax.dot_general(tm[...], wv[...], (((1,), (1,)), ((), ())), preferred_element_type=F32)

        def put(at, rows, lanes, value):
            pt[slot, at : at + rows, lanes] = value

        pack(put, V, block)

    p_copy = send(pt, pr, p_s.at[0], p_r.at[0], c, r)
    p_out, p_on = [], []
    for q, slot in enumerate((c_y, c_d, c, c_z)):
        via, to, src = ((r_x, c), (c, r_x), slot) if q < 2 else ((r, c_z), (c_z, r), (c_z, c)[q - 2])
        p_out.append(send(pt.at[slot], prel.at[q], p_s.at[1 + q], p_r.at[1 + q], *via))
        p_on.append(send(prel.at[q], pr.at[src], p_s.at[5 + q], p_r.at[5 + q], *to))

    def p_start(q):
        @pl.when(x != z)
        def _():
            p_out[q].start()

    def relay(*quarters):
        for q in quarters:
            with scope("relay"):
                p_out[q].wait_recv()
            p_on[q].start()

    with scope("mixed_c"):
        mixed(c)

    with scope("row10"):
        row_wait(1, 0)

    @pl.when(x == z)
    def _():
        row_copy(2, 0).start()

    dispatch(c_z, 0)
    with scope("row00"):
        row_wait(0, 0)

    @pl.when(x == z)
    def _():
        row_extra.start()

    dispatch(c_y, 0)

    load_d.wait()
    for m in range(5):
        split_cols(lambda lo, hi: d32[:, lo:hi], planes, m)
    for cc in range(4):
        parts = []
        for j in range(4):
            parts += take_j(planes, 4 * cc + j, 0, 4 * AB)
        def put_d(at, rows, lanes, value):
            dsnd[cc, at : at + rows, lanes] = value

        pack(put_d, V, jnp.concatenate(parts, axis=1))
    drcv[c] = dsnd[c]

    with scope("row11"):
        row_wait(1, 1)
    dispatch(c_z, 1)
    with scope("row01"):
        row_wait(0, 1)
    row_copy(2, 1).start()
    dispatch(c_y, 1)
    d_copy = [
        send(dsnd.at[peer], drcv.at[c], d_s.at[q], d_r.at[q], r, peer) for q, peer in enumerate(col_peers)
    ]

    @pl.when(x == z)
    def _():
        col_piece(1).start()
        d_copy[0].start()

    p_start(2)
    forward(0)
    with scope("mixed_c_z"):
        mixed(c_z)
    p_start(3)
    with scope("mixed_c_y"):
        mixed(c_y)
    with scope("row20"):
        row_wait(2, 0)
    forward(1)
    p_start(0)
    with scope("row21"):
        row_wait(2, 1)

    @pl.when(x != z)
    def _():
        dispatch(c_d, 0)
        dispatch(c_d, 1)

    with scope("mixed_c_d"):
        mixed(c_d)
    p_start(1)

    q_copy = [send(xq, xqr.at[c], q_s.at[q], q_r.at[q], r, peer) for q, peer in enumerate(col_peers)]

    def hole_x():
        load_vo.wait()
        send(tcol.at[r_k], tcol.at[r_k], col_s.at[2], col_r.at[2], r_k, c).wait_recv()

        @pl.when(jnp.logical_and(x == z, r != c))
        def _():
            send(tcol.at[r_x], tcol.at[r_x], f_s.at[0], col_r.at[4], r_k, c).wait_recv()

        @pl.when(r != c)
        def _():
            send(tcol.at[r_d], tcol.at[r_d], col_s.at[3], col_r.at[3], r_k, c).wait_recv()

        xq[...] = lax.dot_general(
            vo[...], tcol[...].reshape(4 * RB, CB), (((1,), (1,)), ((), ())), preferred_element_type=F32
        )
        xqr[c] = xq[...]
        for copy in q_copy:
            copy.start()

    @pl.when(x != z)
    def _():
        with scope("col"):
            for h in range(2):
                piece = tcol.at[r_x, halves[h]]
                send(piece, piece, col_s.at[h], col_r.at[h], r_x, c).wait_recv()
        col_relay.start()
        with scope("hole_x"):
            hole_x()

    @pl.when(jnp.logical_not(gives))
    def _():
        for h in range(2):
            for slot in (r_x, r_d):
                with scope("lad"):
                    lad_wait(slot, h)

    for h in range(2):
        with scope("lad_k"):
            lad_wait(r_k, h)

    fwd = (
        send(tlad.at[r_d], tcol.at[r_d], f_s.at[0], col_r.at[4], r_k, c),
        send(tlad.at[r_x], tcol.at[r_x], f_s.at[1], col_r.at[3], r_k, c),
    )

    @pl.when(r == c)
    def _():
        for copy in fwd:
            copy.start()
        tcol[r_d] = tlad[r_d]
        tcol[r_x] = tlad[r_x]

    @pl.when(x == z)
    def _():
        with scope("hole_x"):
            hole_x()

        d_copy[1].start()

        @pl.when(r != c)
        def _():
            p_copy.start()

        @pl.when(r == c)
        def _():
            pr[...] = pt[...]

    def w_copy(rr):
        return send(wt.at[RB * rr : RB * rr + RB], wblk.at[r], w_s.at[rr], w_r.at[r], rr, c)

    def hole_w():
        load_oo.wait()
        for q, peer in enumerate(col_peers):
            send(xq, xqr.at[peer], q_s.at[q], q_r.at[q], r, peer).wait_recv()
        x_sum = (xqr[0] + xqr[1]) + (xqr[2] + xqr[3])
        w_hole = oo[...].astype(F32) + 0.5 * x_sum
        wt[...] = w_hole.T.astype(BF16)
        wblk[r] = wt[pl.ds(pl.multiple_of(r * RB, RB), RB), :]
        for rr in range(4):

            @pl.when(r != rr)
            def _():
                w_copy(rr).start()

    def d2_copy(n):
        return send(acc.at[n, 1 - k], d2r.at[n], dd_s.at[n], dd_r.at[n], r_k, c)

    def xx_copy(n):
        return send(xsb.at[n], xrb.at[n], xx_s.at[n], xx_r.at[n], r_x, c)

    d2_tail = send(acct.at[1 - k], d2t, dd_s.at[NCH], dd_r.at[NCH], r_k, c)
    xx_tail = send(xst, xrt, xx_s.at[NCH], xx_r.at[NCH], r_x, c)

    def gather_w():
        with scope("w_in"):
            for rr in range(4):

                @pl.when(r != rr)
                def _():
                    send(wt.at[0:RB], wblk.at[rr], w_s.at[rr], w_r.at[rr], rr, c).wait_recv()

        wf[...] = jnp.concatenate([wblk[rr].astype(F32) for rr in range(4)], axis=1).astype(BF16)

    def close(lo, hi, landed):
        hole = jnp.dot(wf[...], tcol[:, :, lo:hi].reshape(4 * RB, hi - lo), preferred_element_type=F32)
        r1[:, lo:hi] = r1[:, lo:hi] + landed + hole + vo[:, lo:hi].astype(F32)

    def stripe_rows(m):
        return 32 if m < 4 else 16

    def l_copy(m, q):
        there = pl.ds(V * m, stripe_rows(m) * 9 // 2)
        peer = col_peers[q]
        return send(lsnd.at[peer, there], lrcv.at[c, there], l_s.at[m, q], l_r.at[m, q], r, peer)

    def stripe_out(m):
        for n in ((0, 1, 2), (3, 4), (5, 6), (7, 8), (9,))[m]:
            with scope("sum"):
                xx_copy(n).wait_recv()
            close(CW * n, CW * n + CW, xrb[n])
        if m == 4:
            xx_tail.wait_recv()
            close(NCH * CW, CB, xrt[...])
        split_cols(lambda lo, hi: r1[:, lo:hi], planes, m)
        rows = stripe_rows(m)
        for cc in range(4):
            parts = []
            for j in range(4):
                parts += take_j(planes, 4 * cc + j, RB * 8 * m, rows)

            def put_l(at, count, lanes, value):
                lsnd[cc, V * m + at : V * m + at + count, lanes] = value

            pack(put_l, rows, jnp.concatenate(parts, axis=1))
        there = slice(V * m, V * m + rows * 9 // 2)
        lrcv[c, there, :] = lsnd[c, there, :]
        for q in range(3):
            l_copy(m, q).start()

    load_tail.wait()
    part = jnp.dot(tlad[...].reshape(4 * RB, CB), vtail[...], preferred_element_type=F32)
    for rr in range(4):
        acct[rr % 2, rr // 2] = part[RB * rr : RB * rr + RB]
    d2_tail.start()

    def second(n):
        with scope("pair"):
            d2_copy(n).wait_recv()
        xsb[n] = acc[n, k, 1 - x] + d2r[n, 1 - x]
        at = pl.multiple_of(n * CW, CW)
        r1[:, pl.ds(at, CW)] = acc[n, k, x] + d2r[n, x]
        xx_copy(n).start()

    def ladder_step(n, carry):
        slot = n % 2
        with scope("wait_v"):
            load_v(n, slot).wait()
        with scope("dot"):
            for h in range(2):
                part = jnp.dot(
                    tlad[...].reshape(4 * RB, CB), vbuf[slot, :, 256 * h : 256 * h + 256], preferred_element_type=F32
                )
                for rr in range(4):
                    acc[n, rr % 2, rr // 2, :, 256 * h : 256 * h + 256] = part[RB * rr : RB * rr + RB]
        d2_copy(n).start()

        @pl.when(n + 2 < NCH)
        def _():
            load_v(n + 2, slot).start()

        @pl.when(n == 0)
        def _():
            d2_tail.wait_recv()
            xst[...] = acct[k, 1 - x] + d2t[1 - x]
            r1[:, NCH * CW : CB] = acct[k, x] + d2t[x]
            xx_tail.start()

        @pl.when(n > 0)
        def _():
            second(n - 1)

        @pl.when(jnp.logical_and(n == 1, x != z))
        def _():
            for copy in d_copy:
                copy.start()

        @pl.when(jnp.logical_and(n == 1, x == z))
        def _():
            relay(2)

        @pl.when(jnp.logical_and(n == 2, x == z))
        def _():
            relay(3)
            d_copy[2].start()

        @pl.when(jnp.logical_and(n == 3, x == z))
        def _():
            relay(0)

        @pl.when(jnp.logical_and(n == 5, x == z))
        def _():
            relay(1)

        @pl.when(n == jnp.where(x == z, 4, 2))
        def _():
            with scope("hole_w"):
                hole_w()

        @pl.when(jnp.logical_and(n == 9, x != z))
        def _():
            gather_w()
            stripe_out(0)
            stripe_out(1)

        return carry

    lax.fori_loop(0, NCH, ladder_step, 0)
    second(NCH - 1)

    @pl.when(x == z)
    def _():
        gather_w()
        stripe_out(0)
        stripe_out(1)

    def order_rows(src, dst):
        for cc in range(4):
            for i in range(4):
                first = V * i + AB * cc
                for b in range(4):
                    dst[first : first + AB, 128 * b : 128 * b + 128] = src[cc, pl.ds(V * b + i, AB, stride=4), :]
                ends = src[cc, pl.ds(4 * V + i, AB // 2, stride=4), :]
                dst[first : first + AB // 2, 512:576] = ends[:, 0:64]
                dst[first + AB // 2 : first + AB, 512:576] = ends[:, 64:128]

    for m in range(2, 4):
        stripe_out(m)
    order_rows(pt, pp)
    with scope("mirror"):

        @pl.when(jnp.logical_and(x == z, r != c))
        def _():
            p_copy.wait_recv()

        @pl.when(x != z)
        def _():
            for copy in p_on:
                copy.wait_recv()

    order_rows(pr, r3)
    pp[...] = pp[...] + r3[...].T
    for q, peer in enumerate(col_peers):
        with scope("denom"):
            send(dsnd.at[peer], drcv.at[peer], d_s.at[q], d_r.at[q], r, peer).wait_recv()
    order_rows(drcv, r3)
    stripe_out(4)

    for m in range(5):
        rows = stripe_rows(m)
        for q, peer in enumerate(col_peers):
            there = pl.ds(V * m, rows * 9 // 2)
            with scope("regroup"):
                send(
                    lsnd.at[peer, there], lrcv.at[peer, there], l_s.at[m, q], l_r.at[m, q], r, peer
                ).wait_recv()
        for cc in range(4):
            for i in range(4):
                first = V * i + AB * cc + 8 * m
                n = rows // 4

                def finish(at, count, lanes, value):
                    there = slice(at, at + count)
                    out_ref[there, lanes] = (value + pp[there, lanes]) / r3[there, lanes]

                for b in range(4):
                    part = lrcv[cc, pl.ds(V * m + rows * b + i, n, stride=4), :]
                    finish(first, n, slice(128 * b, 128 * b + 128), part)
                ends = lrcv[cc, pl.ds(V * m + 4 * rows + i, n // 2, stride=4), :]
                finish(first, n // 2, slice(512, 576), ends[:, 0:64])
                finish(first + n // 2, n // 2, slice(512, 576), ends[:, 64:128])

    for copy in (col_pair, *q_copy, *d_copy, d2_tail, xx_tail):
        copy.wait_send()
    for m in range(5):
        for q in range(3):
            l_copy(m, q).wait_send()
    for way, h in ((0, 0), (0, 1), (1, 0), (1, 1), (2, 1)):
        row_copy(way, h).wait_send()

    @pl.when(x == z)
    def _():
        row_copy(2, 0).wait_send()
        row_extra.wait_send()
        for h in range(2):
            col_piece(h).wait_send()
        for copy in p_on:
            copy.wait_send()

    @pl.when(jnp.logical_and(x == z, r != c))
    def _():
        p_copy.wait_send()

    @pl.when(x != z)
    def _():
        col_relay.wait_send()
        for copy in p_out:
            copy.wait_send()

    @pl.when(r == c)
    def _():
        for copy in fwd:
            copy.wait_send()

    @pl.when(gives)
    def _():
        for h in range(2):
            for slot in (r_x, r_d):
                lad_forward(slot, h).wait_send()

    for slot in range(4):

        @pl.when(slot != r)
        def _():
            w_copy(slot).wait_send()

        @pl.when(jnp.logical_and(slot != r, jnp.logical_or(slot != c_d, x != z)))
        def _():
            for h in range(2):
                lad_copy(slot, h).wait_send()

    def drain(n, carry):
        d2_copy(n).wait_send()
        xx_copy(n).wait_send()
        return carry

    lax.fori_loop(0, NCH, drain, 0)


def solution(mesh):
    vm = pltpu.VMEM
    dma = pltpu.SemaphoreType.DMA
    scratch = [
        vm((RB, CB), F32), vm((RB, CB), F32), vm((RB, CB), BF16), vm((PB, O * V), BF16),
        vm((4, RB, CB), BF16), vm((4, RB, CB), BF16), vm((4, RB, CB), BF16),
        vm((2, AB * RB, 128), F32), vm((V, O * V), BF16),
        vm((PB, PB), F32), vm((PB, PB), F32), vm((4, PQ, 128), F32), vm((4, PQ, 128), F32),
        vm((4, PQ, 128), F32), vm((4, PQ, 128), F32), vm((4, PQ, 128), F32), vm((4, PQ, 128), F32),
        vm((4, PQ, 128), F32),
        vm((RB, O * O), F32), vm((4, RB, O * O), F32), vm((O * O, RB), BF16), vm((RB, O * O), BF16), vm((4, RB, RB), BF16), vm((RB, O * O), BF16),
        vm((2, CB, CW), BF16), vm((CB, TW), BF16),
        vm((NCH, 2, 2, RB, CW), F32), vm((NCH, 2, RB, CW), F32), vm((NCH, RB, CW), F32), vm((NCH, RB, CW), F32),
        vm((2, 2, RB, TW), F32), vm((2, RB, TW), F32), vm((RB, TW), F32), vm((RB, TW), F32),
        vm((RB, CB), F32),
        dma((6,)), dma((2,)), dma((4, 2)), dma((4, 2)), dma((5,)), dma((5,)), dma((4, 2)), dma((4, 2)),
        dma((3,)), dma((3,)), dma((3,)), dma((3,)), dma((5, 3)), dma((5, 3)), dma((9,)), dma((9,)), dma((4, 2)),
        dma((NCH + 1,)), dma((NCH + 1,)), dma((NCH + 1,)), dma((NCH + 1,)), dma((4,)), dma((4,)), dma((2,)),
    ]
    hbm = pl.BlockSpec(memory_space=pl.ANY)
    vmem = pl.BlockSpec(memory_space=pltpu.VMEM)
    call = pl.pallas_call(
        kernel,
        out_shape=jax.ShapeDtypeStruct((PB, PB), F32),
        in_specs=[hbm] * 6,
        out_specs=vmem,
        scratch_shapes=scratch,
        compiler_params=pltpu.CompilerParams(
            collective_id=0, has_side_effects=True, vmem_limit_bytes=67_000_000
        ),
        name="sweep",
    )
    def local_sweep(t_blk, d_blk, voovv_blk, vvvvv_blk, oooo, w_blk):
        return call(t_blk, d_blk, voovv_blk, vvvvv_blk, oooo, w_blk.T)

    return jax.shard_map(
        local_sweep,
        mesh=mesh,
        in_specs=(P("row", "col"), P("row", "col"), P("row", "col"), P("row", "col"), P(None, None), P(None, "col")),
        out_specs=P("row", "col"),
        check_vma=False,
    )
```

```python
import functools

import jax
import jax.numpy as jnp
from jax import lax
from jax.experimental import pallas as pl
from jax.experimental.pallas import tpu as pltpu
from jax.sharding import PartitionSpec as P

MESH = pl.DeviceIdType.MESH
scope = jax.named_scope
F32 = jnp.float32
BF16 = jnp.bfloat16

O = 16
V = 144
RB = 64
CB = 5184
AB = 36
PQ = 648
PB = 576
CW = 512
NCH = CB // CW
TW = CB - NCH * CW


def stripe(load, m, q):
    first = 1152 * m + V * q
    low = first // 128 * 128
    high = min(-(-(first + V) // 128) * 128, CB)
    return load(low, high)[:, first - low : first - low + V]


def split_cols(load, planes, m):
    for q in range(8 if m < 4 else 4):
        piece = stripe(load, m, q)
        base = RB * (8 * m + q)
        planes[0, base : base + RB, :] = piece[:, 0:128]
        planes[1, base : base + RB, 0:16] = piece[:, 128:144]


def take_j(planes, j, base, rows):
    wide = planes[0, pl.ds(base + j, rows, stride=16), :]
    rest = planes[1, pl.ds(base + j, rows, stride=16), :]
    return [wide, rest[:, 0:16]]


def pack(put, rows, wide):
    for b in range(4):
        put(rows * b, rows, slice(0, 128), wide[:, 128 * b : 128 * b + 128])
    put(4 * rows, rows // 2, slice(0, 64), wide[: rows // 2, 512:576])
    put(4 * rows, rows // 2, slice(64, 128), wide[rows // 2 :, 512:576])


def kernel(
    t_hbm, d_hbm, vo_hbm, vv_hbm, oo_hbm, w_hbm, out_ref,
    t32, d32, vo, wv, trow, tcol, tlad, planes, tm, r3, pp, pt, pr,
    dsnd, drcv, lsnd, lrcv, prel, xq, xqr, wt, oo, wblk, wf, vbuf, vtail,
    acc, d2r, xsb, xrb, acct, d2t, xst, xrt, r1,
    in_sem, v_sem, row_s, row_r, col_s, col_r, lad_s, lad_r, q_s, q_r,
    d_s, d_r, l_s, l_r, p_s, p_r, fw_s, dd_s, dd_r, xx_s, xx_r, w_s, w_r, f_s,
):
    r = lax.axis_index("row")
    c = lax.axis_index("col")
    x, k = r // 2, r % 2
    z, y = c // 2, c % 2
    r_k, r_x = 2 * x + 1 - k, 2 * (1 - x) + k
    r_d = 2 * (1 - x) + 1 - k
    c_y, c_z = 2 * z + 1 - y, 2 * (1 - z) + y
    c_d = 2 * (1 - z) + 1 - y
    col_peers = (c_y, c_z, c_d)

    def send(src, dst, ss, rs, row, col):
        return pltpu.make_async_remote_copy(
            src_ref=src, dst_ref=dst, send_sem=ss, recv_sem=rs,
            device_id={"row": row, "col": col}, device_id_type=MESH,
        )

    def load_v(n, slot):
        at = pl.multiple_of(n * CW, CW)
        return pltpu.make_async_copy(vv_hbm.at[:, pl.ds(at, CW)], vbuf.at[slot], v_sem.at[slot])

    load_t = pltpu.make_async_copy(t_hbm, t32, in_sem.at[0])
    load_d = pltpu.make_async_copy(d_hbm, d32, in_sem.at[1])
    load_vo = pltpu.make_async_copy(vo_hbm, vo, in_sem.at[2])
    load_w = pltpu.make_async_copy(w_hbm, wv, in_sem.at[3])
    load_tail = pltpu.make_async_copy(vv_hbm.at[:, pl.ds(NCH * CW, TW)], vtail, in_sem.at[4])
    load_oo = pltpu.make_async_copy(oo_hbm.at[pl.ds(pl.multiple_of(r * RB, RB), RB)], oo, in_sem.at[5])
    load_t.start()
    load_w.start()
    load_d.start()
    load_vo.start()
    load_tail.start()
    load_oo.start()
    load_v(0, 0).start()
    load_v(1, 1).start()

    barrier = pltpu.get_barrier_semaphore()
    for rr in range(4):
        for cc in range(4):
            pl.semaphore_signal(barrier, inc=1, device_id={"row": rr, "col": cc}, device_id_type=MESH)

    with scope("wait_t"):
        load_t.wait()
    for m in range(9):
        piece = t32[:, PB * m : PB * m + PB].astype(BF16)
        trow[c, :, PB * m : PB * m + PB] = piece
        tcol[r, :, PB * m : PB * m + PB] = piece
    with scope("barrier"):
        pl.semaphore_wait(barrier, 16)

    half = RB // 2
    halves = (slice(0, half), slice(half, RB))

    def row_copy(way, h):
        block, peer = ((c, c_y), (c, c_z), ((c_z, c_y), (c_y, c_z))[h])[way]
        piece = trow.at[block, halves[h]]
        return send(piece, piece, row_s.at[way, h], row_r.at[way, h], r, peer)

    row_extra = send(
        trow.at[c_y, halves[0]], trow.at[c_y, halves[0]], row_s.at[3, 0], row_r.at[2, 0], r, c_z
    )

    def row_wait(way, h):
        piece = trow.at[(c_y, c_z, c_d)[way], halves[h]]
        send(piece, piece, row_s.at[way, h], row_r.at[way, h], r, c_y).wait_recv()

    def col_piece(h):
        piece = tcol.at[r, halves[h]]
        return send(piece, piece, col_s.at[h], col_r.at[h], r_x, c)

    col_pair = send(tcol.at[r], tcol.at[r], col_s.at[2], col_r.at[2], r_k, c)
    col_relay = send(tcol.at[r_x], tcol.at[r_x], col_s.at[3], col_r.at[3], r_k, c)

    def lad_copy(slot, h):
        return send(trow.at[slot, halves[h]], tlad.at[r, halves[h]], lad_s.at[slot, h], lad_r.at[r, h], slot, c)

    def dispatch(slot, h):
        @pl.when(slot != r)
        def _():
            lad_copy(slot, h).start()

        @pl.when(slot == r)
        def _():
            tlad[r, halves[h]] = trow[slot, halves[h]]

    def lad_wait(slot, h):
        send(trow.at[0, halves[h]], tlad.at[slot, halves[h]], lad_s.at[slot, h], lad_r.at[slot, h], r, c).wait_recv()

    def lad_forward(slot, h):
        piece = tlad.at[slot, halves[h]]
        return send(piece, piece, fw_s.at[slot, h], lad_r.at[slot, h], r, c_y)

    gives = jnp.logical_and(x != z, k == y)

    def forward(h):
        @pl.when(gives)
        def _():
            for slot in (r_x, r_d):
                with scope("lad_f"):
                    lad_wait(slot, h)
                lad_forward(slot, h).start()

    @pl.when(x == z)
    def _():
        col_piece(0).start()

    for h in range(2):
        row_copy(0, h).start()
        row_copy(1, h).start()
        dispatch(c, h)
    col_pair.start()

    with scope("wait_w"):
        load_w.wait()

    def mixed(slot):
        for m in range(5):
            split_cols(lambda lo, hi: trow[slot, :, lo:hi].astype(F32), planes, m)
        for h in range(2):
            parts = []
            for j in range(8):
                parts += take_j(planes, 8 * h + j, 0, 4 * AB)
            tm[:, 1152 * h : 1152 * h + 1152] = jnp.concatenate(parts, axis=1).astype(BF16)
        block = lax.dot_general(tm[...], wv[...], (((1,), (1,)), ((), ())), preferred_element_type=F32)

        def put(at, rows, lanes, value):
            pt[slot, at : at + rows, lanes] = value

        pack(put, V, block)

    p_copy = send(pt, pr, p_s.at[0], p_r.at[0], c, r)
    p_out, p_on = [], []
    for q, slot in enumerate((c_y, c_d, c, c_z)):
        via, to, src = ((r_x, c), (c, r_x), slot) if q < 2 else ((r, c_z), (c_z, r), (c_z, c)[q - 2])
        p_out.append(send(pt.at[slot], prel.at[q], p_s.at[1 + q], p_r.at[1 + q], *via))
        p_on.append(send(prel.at[q], pr.at[src], p_s.at[5 + q], p_r.at[5 + q], *to))

    def p_start(q):
        @pl.when(x != z)
        def _():
            p_out[q].start()

    def relay(*quarters):
        for q in quarters:
            with scope("relay"):
                p_out[q].wait_recv()
            p_on[q].start()

    with scope("mixed_c"):
        mixed(c)

    with scope("row10"):
        row_wait(1, 0)

    @pl.when(x == z)
    def _():
        row_copy(2, 0).start()

    dispatch(c_z, 0)
    with scope("row00"):
        row_wait(0, 0)

    @pl.when(x == z)
    def _():
        row_extra.start()

    dispatch(c_y, 0)

    load_d.wait()
    for m in range(5):
        split_cols(lambda lo, hi: d32[:, lo:hi], planes, m)
    for cc in range(4):
        parts = []
        for j in range(4):
            parts += take_j(planes, 4 * cc + j, 0, 4 * AB)
        def put_d(at, rows, lanes, value):
            dsnd[cc, at : at + rows, lanes] = value

        pack(put_d, V, jnp.concatenate(parts, axis=1))
    drcv[c] = dsnd[c]

    with scope("row11"):
        row_wait(1, 1)
    dispatch(c_z, 1)
    with scope("row01"):
        row_wait(0, 1)
    row_copy(2, 1).start()
    dispatch(c_y, 1)
    d_copy = [
        send(dsnd.at[peer], drcv.at[c], d_s.at[q], d_r.at[q], r, peer) for q, peer in enumerate(col_peers)
    ]

    @pl.when(x == z)
    def _():
        col_piece(1).start()
        d_copy[0].start()

    p_start(2)
    forward(0)
    with scope("mixed_c_z"):
        mixed(c_z)
    p_start(3)
    with scope("mixed_c_y"):
        mixed(c_y)
    with scope("row20"):
        row_wait(2, 0)
    forward(1)
    p_start(0)
    with scope("row21"):
        row_wait(2, 1)

    @pl.when(x != z)
    def _():
        dispatch(c_d, 0)
        dispatch(c_d, 1)

    with scope("mixed_c_d"):
        mixed(c_d)
    p_start(1)

    q_copy = [send(xq, xqr.at[c], q_s.at[q], q_r.at[q], r, peer) for q, peer in enumerate(col_peers)]

    def hole_x():
        load_vo.wait()
        send(tcol.at[r_k], tcol.at[r_k], col_s.at[2], col_r.at[2], r_k, c).wait_recv()

        @pl.when(jnp.logical_and(x == z, r != c))
        def _():
            send(tcol.at[r_x], tcol.at[r_x], f_s.at[0], col_r.at[4], r_k, c).wait_recv()

        @pl.when(r != c)
        def _():
            send(tcol.at[r_d], tcol.at[r_d], col_s.at[3], col_r.at[3], r_k, c).wait_recv()

        xq[...] = lax.dot_general(
            vo[...], tcol[...].reshape(4 * RB, CB), (((1,), (1,)), ((), ())), preferred_element_type=F32
        )
        xqr[c] = xq[...]
        for copy in q_copy:
            copy.start()

    @pl.when(x != z)
    def _():
        with scope("col"):
            for h in range(2):
                piece = tcol.at[r_x, halves[h]]
                send(piece, piece, col_s.at[h], col_r.at[h], r_x, c).wait_recv()
        col_relay.start()
        with scope("hole_x"):
            hole_x()

    @pl.when(jnp.logical_not(gives))
    def _():
        for h in range(2):
            for slot in (r_x, r_d):
                with scope("lad"):
                    lad_wait(slot, h)

    for h in range(2):
        with scope("lad_k"):
            lad_wait(r_k, h)

    fwd = (
        send(tlad.at[r_d], tcol.at[r_d], f_s.at[0], col_r.at[4], r_k, c),
        send(tlad.at[r_x], tcol.at[r_x], f_s.at[1], col_r.at[3], r_k, c),
    )

    @pl.when(r == c)
    def _():
        for copy in fwd:
            copy.start()
        tcol[r_d] = tlad[r_d]
        tcol[r_x] = tlad[r_x]

    @pl.when(x == z)
    def _():
        relay(2)
        with scope("hole_x"):
            hole_x()

        d_copy[1].start()

        @pl.when(r != c)
        def _():
            p_copy.start()

        @pl.when(r == c)
        def _():
            pr[...] = pt[...]

    def w_copy(rr):
        return send(wt.at[RB * rr : RB * rr + RB], wblk.at[r], w_s.at[rr], w_r.at[r], rr, c)

    def hole_w():
        load_oo.wait()
        for q, peer in enumerate(col_peers):
            send(xq, xqr.at[peer], q_s.at[q], q_r.at[q], r, peer).wait_recv()
        x_sum = (xqr[0] + xqr[1]) + (xqr[2] + xqr[3])
        w_hole = oo[...].astype(F32) + 0.5 * x_sum
        wt[...] = w_hole.T.astype(BF16)
        wblk[r] = wt[pl.ds(pl.multiple_of(r * RB, RB), RB), :]
        for rr in range(4):

            @pl.when(r != rr)
            def _():
                w_copy(rr).start()

    def d2_copy(n):
        return send(acc.at[n, 1 - k], d2r.at[n], dd_s.at[n], dd_r.at[n], r_k, c)

    def xx_copy(n):
        return send(xsb.at[n], xrb.at[n], xx_s.at[n], xx_r.at[n], r_x, c)

    d2_tail = send(acct.at[1 - k], d2t, dd_s.at[NCH], dd_r.at[NCH], r_k, c)
    xx_tail = send(xst, xrt, xx_s.at[NCH], xx_r.at[NCH], r_x, c)

    def gather_w():
        with scope("w_in"):
            for rr in range(4):

                @pl.when(r != rr)
                def _():
                    send(wt.at[0:RB], wblk.at[rr], w_s.at[rr], w_r.at[rr], rr, c).wait_recv()

        wf[...] = jnp.concatenate([wblk[rr].astype(F32) for rr in range(4)], axis=1).astype(BF16)

    def close(lo, hi, landed):
        hole = jnp.dot(wf[...], tcol[:, :, lo:hi].reshape(4 * RB, hi - lo), preferred_element_type=F32)
        r1[:, lo:hi] = r1[:, lo:hi] + landed + hole + vo[:, lo:hi].astype(F32)

    def stripe_rows(m):
        return 32 if m < 4 else 16

    def l_copy(m, q):
        there = pl.ds(V * m, stripe_rows(m) * 9 // 2)
        peer = col_peers[q]
        return send(lsnd.at[peer, there], lrcv.at[c, there], l_s.at[m, q], l_r.at[m, q], r, peer)

    def stripe_out(m):
        for n in ((0, 1, 2), (3, 4), (5, 6), (7, 8), (9,))[m]:
            with scope("sum"):
                xx_copy(n).wait_recv()
            close(CW * n, CW * n + CW, xrb[n])
        if m == 4:
            xx_tail.wait_recv()
            close(NCH * CW, CB, xrt[...])
        split_cols(lambda lo, hi: r1[:, lo:hi], planes, m)
        rows = stripe_rows(m)
        for cc in range(4):
            parts = []
            for j in range(4):
                parts += take_j(planes, 4 * cc + j, RB * 8 * m, rows)

            def put_l(at, count, lanes, value):
                lsnd[cc, V * m + at : V * m + at + count, lanes] = value

            pack(put_l, rows, jnp.concatenate(parts, axis=1))
        there = slice(V * m, V * m + rows * 9 // 2)
        lrcv[c, there, :] = lsnd[c, there, :]
        for q in range(3):
            l_copy(m, q).start()

    load_tail.wait()
    part = jnp.dot(tlad[...].reshape(4 * RB, CB), vtail[...], preferred_element_type=F32)
    for rr in range(4):
        acct[rr % 2, rr // 2] = part[RB * rr : RB * rr + RB]
    d2_tail.start()

    def second(n):
        with scope("pair"):
            d2_copy(n).wait_recv()
        xsb[n] = acc[n, k, 1 - x] + d2r[n, 1 - x]
        at = pl.multiple_of(n * CW, CW)
        r1[:, pl.ds(at, CW)] = acc[n, k, x] + d2r[n, x]
        xx_copy(n).start()

    def ladder_step(n, carry):
        slot = n % 2
        with scope("wait_v"):
            load_v(n, slot).wait()
        with scope("dot"):
            for h in range(2):
                part = jnp.dot(
                    tlad[...].reshape(4 * RB, CB), vbuf[slot, :, 256 * h : 256 * h + 256], preferred_element_type=F32
                )
                for rr in range(4):
                    acc[n, rr % 2, rr // 2, :, 256 * h : 256 * h + 256] = part[RB * rr : RB * rr + RB]
        d2_copy(n).start()

        @pl.when(n + 2 < NCH)
        def _():
            load_v(n + 2, slot).start()

        @pl.when(n == 0)
        def _():
            d2_tail.wait_recv()
            xst[...] = acct[k, 1 - x] + d2t[1 - x]
            r1[:, NCH * CW : CB] = acct[k, x] + d2t[x]
            xx_tail.start()

        @pl.when(n > 0)
        def _():
            second(n - 1)

        @pl.when(jnp.logical_and(n == 1, x != z))
        def _():
            for copy in d_copy:
                copy.start()

        @pl.when(jnp.logical_and(n == 1, x == z))
        def _():
            relay(3)

        @pl.when(jnp.logical_and(n == 2, x == z))
        def _():
            d_copy[2].start()

        @pl.when(jnp.logical_and(n == 3, x == z))
        def _():
            relay(0)

        @pl.when(jnp.logical_and(n == 5, x == z))
        def _():
            relay(1)

        @pl.when(n == jnp.where(x == z, 4, 2))
        def _():
            with scope("hole_w"):
                hole_w()

        @pl.when(jnp.logical_and(n == 9, x != z))
        def _():
            gather_w()
            stripe_out(0)
            stripe_out(1)

        return carry

    lax.fori_loop(0, NCH, ladder_step, 0)
    second(NCH - 1)

    @pl.when(x == z)
    def _():
        gather_w()
        stripe_out(0)
        stripe_out(1)

    def order_rows(src, dst):
        for cc in range(4):
            for i in range(4):
                first = V * i + AB * cc
                for b in range(4):
                    dst[first : first + AB, 128 * b : 128 * b + 128] = src[cc, pl.ds(V * b + i, AB, stride=4), :]
                ends = src[cc, pl.ds(4 * V + i, AB // 2, stride=4), :]
                dst[first : first + AB // 2, 512:576] = ends[:, 0:64]
                dst[first + AB // 2 : first + AB, 512:576] = ends[:, 64:128]

    for m in range(2, 4):
        stripe_out(m)
    order_rows(pt, pp)
    stripe_out(4)
    with scope("mirror"):

        @pl.when(jnp.logical_and(x == z, r != c))
        def _():
            p_copy.wait_recv()

        @pl.when(x != z)
        def _():
            for copy in p_on:
                copy.wait_recv()

    order_rows(pr, r3)
    pp[...] = pp[...] + r3[...].T
    for q, peer in enumerate(col_peers):
        with scope("denom"):
            send(dsnd.at[peer], drcv.at[peer], d_s.at[q], d_r.at[q], r, peer).wait_recv()
    order_rows(drcv, r3)

    for m in range(5):
        rows = stripe_rows(m)
        for q, peer in enumerate(col_peers):
            there = pl.ds(V * m, rows * 9 // 2)
            with scope("regroup"):
                send(
                    lsnd.at[peer, there], lrcv.at[peer, there], l_s.at[m, q], l_r.at[m, q], r, peer
                ).wait_recv()
        for cc in range(4):
            for i in range(4):
                first = V * i + AB * cc + 8 * m
                n = rows // 4

                def finish(at, count, lanes, value):
                    there = slice(at, at + count)
                    out_ref[there, lanes] = (value + pp[there, lanes]) / r3[there, lanes]

                for b in range(4):
                    part = lrcv[cc, pl.ds(V * m + rows * b + i, n, stride=4), :]
                    finish(first, n, slice(128 * b, 128 * b + 128), part)
                ends = lrcv[cc, pl.ds(V * m + 4 * rows + i, n // 2, stride=4), :]
                finish(first, n // 2, slice(512, 576), ends[:, 0:64])
                finish(first + n // 2, n // 2, slice(512, 576), ends[:, 64:128])

    for copy in (col_pair, *q_copy, *d_copy, d2_tail, xx_tail):
        copy.wait_send()
    for m in range(5):
        for q in range(3):
            l_copy(m, q).wait_send()
    for way, h in ((0, 0), (0, 1), (1, 0), (1, 1), (2, 1)):
        row_copy(way, h).wait_send()

    @pl.when(x == z)
    def _():
        row_copy(2, 0).wait_send()
        row_extra.wait_send()
        for h in range(2):
            col_piece(h).wait_send()
        for copy in p_on:
            copy.wait_send()

    @pl.when(jnp.logical_and(x == z, r != c))
    def _():
        p_copy.wait_send()

    @pl.when(x != z)
    def _():
        col_relay.wait_send()
        for copy in p_out:
            copy.wait_send()

    @pl.when(r == c)
    def _():
        for copy in fwd:
            copy.wait_send()

    @pl.when(gives)
    def _():
        for h in range(2):
            for slot in (r_x, r_d):
                lad_forward(slot, h).wait_send()

    for slot in range(4):

        @pl.when(slot != r)
        def _():
            w_copy(slot).wait_send()

        @pl.when(jnp.logical_and(slot != r, jnp.logical_or(slot != c_d, x != z)))
        def _():
            for h in range(2):
                lad_copy(slot, h).wait_send()

    def drain(n, carry):
        d2_copy(n).wait_send()
        xx_copy(n).wait_send()
        return carry

    lax.fori_loop(0, NCH, drain, 0)


def solution(mesh):
    vm = pltpu.VMEM
    dma = pltpu.SemaphoreType.DMA
    scratch = [
        vm((RB, CB), F32), vm((RB, CB), F32), vm((RB, CB), BF16), vm((PB, O * V), BF16),
        vm((4, RB, CB), BF16), vm((4, RB, CB), BF16), vm((4, RB, CB), BF16),
        vm((2, AB * RB, 128), F32), vm((V, O * V), BF16),
        vm((PB, PB), F32), vm((PB, PB), F32), vm((4, PQ, 128), F32), vm((4, PQ, 128), F32),
        vm((4, PQ, 128), F32), vm((4, PQ, 128), F32), vm((4, PQ, 128), F32), vm((4, PQ, 128), F32),
        vm((4, PQ, 128), F32),
        vm((RB, O * O), F32), vm((4, RB, O * O), F32), vm((O * O, RB), BF16), vm((RB, O * O), BF16), vm((4, RB, RB), BF16), vm((RB, O * O), BF16),
        vm((2, CB, CW), BF16), vm((CB, TW), BF16),
        vm((NCH, 2, 2, RB, CW), F32), vm((NCH, 2, RB, CW), F32), vm((NCH, RB, CW), F32), vm((NCH, RB, CW), F32),
        vm((2, 2, RB, TW), F32), vm((2, RB, TW), F32), vm((RB, TW), F32), vm((RB, TW), F32),
        vm((RB, CB), F32),
        dma((6,)), dma((2,)), dma((4, 2)), dma((4, 2)), dma((5,)), dma((5,)), dma((4, 2)), dma((4, 2)),
        dma((3,)), dma((3,)), dma((3,)), dma((3,)), dma((5, 3)), dma((5, 3)), dma((9,)), dma((9,)), dma((4, 2)),
        dma((NCH + 1,)), dma((NCH + 1,)), dma((NCH + 1,)), dma((NCH + 1,)), dma((4,)), dma((4,)), dma((2,)),
    ]
    hbm = pl.BlockSpec(memory_space=pl.ANY)
    vmem = pl.BlockSpec(memory_space=pltpu.VMEM)
    call = pl.pallas_call(
        kernel,
        out_shape=jax.ShapeDtypeStruct((PB, PB), F32),
        in_specs=[hbm] * 6,
        out_specs=vmem,
        scratch_shapes=scratch,
        compiler_params=pltpu.CompilerParams(
            collective_id=0, has_side_effects=True, vmem_limit_bytes=67_000_000
        ),
        name="sweep",
    )
    def local_sweep(t_blk, d_blk, voovv_blk, vvvvv_blk, oooo, w_blk):
        return call(t_blk, d_blk, voovv_blk, vvvvv_blk, oooo, w_blk.T)

    return jax.shard_map(
        local_sweep,
        mesh=mesh,
        in_specs=(P("row", "col"), P("row", "col"), P("row", "col"), P("row", "col"), P(None, None), P(None, "col")),
        out_specs=P("row", "col"),
        check_vma=False,
    )
```
